32 devices in a mesh: dp: 8 (over z, core), seq: 4 (over y, x).
Axes of the slice: x: 2, y: 2, z: 4, core: 2. Of those that a mesh axis runs over, the one named last changes fastest.
Arguments:
- tokens: bfloat16 [2, 8, 512, 768], P(None, 'dp', 'seq'), may hold values from -6 to 6
- piece_starts: int32 [2, 8, 2], P(None, 'dp'), may hold values from 0 to 256, as said below
- qkv_weight: bfloat16 [768, 2304], P(('dp', 'seq')), may hold values from -0.21875 to 0.21875
- qv_bias: bfloat16 [1536], P(('dp', 'seq')), may hold values from -1.796875 to 1.796875
- out_weight: bfloat16 [768, 768], P(('dp', 'seq')), may hold values from -1.25 to 1.25
- out_bias: bfloat16 [768], P(('dp', 'seq')), may hold values from -1.796875 to 1.796875
- norm1_gain: bfloat16 [768], P(('dp', 'seq')), may hold values from 0.5 to 1.5
- norm1_bias: bfloat16 [768], P(('dp', 'seq')), may hold values from -1.796875 to 1.796875
- up_weight: bfloat16 [768, 3072], P(('dp', 'seq')), may hold values from -0.21875 to 0.21875
- up_bias: bfloat16 [3072], P(('dp', 'seq')), may hold values from -1.796875 to 1.796875
- down_weight: bfloat16 [3072, 768], P(('dp', 'seq')), may hold values from -0.109375 to 0.109375
- down_bias: bfloat16 [768], P(('dp', 'seq')), may hold values from -1.796875 to 1.796875
- norm2_gain: bfloat16 [768], P(('dp', 'seq')), may hold values from 0.5 to 1.5
- norm2_bias: bfloat16 [768], P(('dp', 'seq')), may hold values from -1.796875 to 1.796875
- grad_out: bfloat16 [2, 8, 512, 768], P(None, 'dp', 'seq'), may hold values from -6 to 6
Outputs:
- layer_out: bfloat16 [2, 8, 512, 768], P(None, 'dp', 'seq')
- tokens_grad: float32 [2, 8, 512, 768], P(None, 'dp', 'seq')
- qkv_weight_grad: float32 [768, 2304], P(('dp', 'seq'))
- qv_bias_grad: float32 [1536], P(('dp', 'seq'))
- out_weight_grad: float32 [768, 768], P(('dp', 'seq'))
- out_bias_grad: float32 [768], P(('dp', 'seq'))
- norm1_gain_grad: float32 [768], P(('dp', 'seq'))
- norm1_bias_grad: float32 [768], P(('dp', 'seq'))
- up_weight_grad: float32 [768, 3072], P(('dp', 'seq'))
- up_bias_grad: float32 [3072], P(('dp', 'seq'))
- down_weight_grad: float32 [3072, 768], P(('dp', 'seq'))
- down_bias_grad: float32 [768], P(('dp', 'seq'))
- norm2_gain_grad: float32 [768], P(('dp', 'seq'))
- norm2_bias_grad: float32 [768], P(('dp', 'seq'))
The draws below stay inside these ranges and needn't reach their ends.
Inputs may be any that keep to these rules, and one draw needn't show every extreme that they name: `piece_starts`: each sequence's 2 pieces of 256 positions lie inside it, in rising order, without intersection.
All inputs are finite; a program needn't handle non-finite values.
Results may differ from the reference program's by a relative error of at most 0.018.
Values may be sent and summed in bfloat16 or wider, within the bound.
A program may use at most 192 MiB of HBM per device.

```python
import math
import jax
import jax.numpy as jnp
from jax import lax

D = 768
HEADS = 12
FF = 3072
MB = 2
PIC = 256
NPIC = 2
LEN = 512
SEQS = 8


def draw_piece_starts(key, part):
    slot = LEN // NPIC
    room = slot - PIC
    offsets = jax.random.randint(jax.random.fold_in(key, 1), (MB, SEQS, NPIC), 0, room + 1)
    first_pick = jax.random.randint(jax.random.fold_in(key, 2), (), 0, MB * SEQS)
    last_pick = jax.random.randint(jax.random.fold_in(key, 3), (), 0, MB * SEQS)
    index = jnp.arange(MB * SEQS, dtype=jnp.int32).reshape(MB, SEQS)
    piece = jnp.arange(NPIC, dtype=jnp.int32)
    offsets = jnp.where((index == first_pick)[:, :, None] & (piece == 0)[None, None, :], 0, offsets)
    offsets = jnp.where((index == last_pick)[:, :, None] & (piece == NPIC - 1)[None, None, :], room, offsets)
    return (piece * slot + offsets).astype(jnp.int32)


def shard_levels(own_key, extent, split, low, largest):
    def one(position, parts):
        steps = jax.random.uniform(jax.random.fold_in(jax.random.fold_in(own_key, 6), position), (parts,), jnp.float32, low / len(split), largest / len(split))
        return jnp.repeat(jnp.exp(steps), extent[position] // parts).reshape((-1,) + (1,) * (len(extent) - position - 1))

    loudness = one(*split[0])
    for cut in split[1:]:
        loudness = loudness * one(*cut)
    return loudness


def centred(key, extent, scale, most, shards=(), held_as=jnp.bfloat16):
    entries = scale * jax.random.normal(key, extent, jnp.float32)
    if shards:
        entries = entries * shard_levels(key, extent, shards, -0.22, 0.18)
    return jnp.clip(entries, -most, most).astype(held_as)


def setup_inputs(seed: int = 0) -> dict:
    streams_of = jax.random.split(jax.random.key(seed), 16)
    return {
        "tokens": centred(streams_of[0], (MB, SEQS, LEN, D), 1.0, 6.0, ((1, 8), (2, 4))),
        "piece_starts": draw_piece_starts(jax.random.fold_in(streams_of[15], 71), 0),
        "qkv_weight": centred(streams_of[2], (D, 3 * D), D ** -0.5, 0.21875, ((0, 32),)),
        "qv_bias": centred(streams_of[3], (2 * D,), 0.3, 1.796875, ((0, 32),)),
        "out_weight": centred(streams_of[4], (D, D), (D // 32) ** -0.5, 1.25, ((0, 32),)),
        "out_bias": centred(streams_of[5], (D,), 0.3, 1.796875, ((0, 32),)),
        "norm1_gain": jnp.clip(1.0 + 0.1 * jax.random.normal(streams_of[6], (D,), jnp.float32), 0.5, 1.5).astype(jnp.bfloat16),
        "norm1_bias": centred(streams_of[7], (D,), 0.3, 1.796875, ((0, 32),)),
        "up_weight": centred(streams_of[8], (D, FF), D ** -0.5, 0.21875, ((0, 32),)),
        "up_bias": centred(streams_of[9], (FF,), 0.3, 1.796875, ((0, 32),)),
        "down_weight": centred(streams_of[10], (FF, D), FF ** -0.5, 0.109375, ((0, 32),)),
        "down_bias": centred(streams_of[11], (D,), 0.3, 1.796875, ((0, 32),)),
        "norm2_gain": jnp.clip(1.0 + 0.1 * jax.random.normal(streams_of[12], (D,), jnp.float32), 0.5, 1.5).astype(jnp.bfloat16),
        "norm2_bias": centred(streams_of[13], (D,), 0.3, 1.796875, ((0, 32),)),
        "grad_out": centred(streams_of[14], (MB, SEQS, LEN, D), 1.0, 6.0, ((1, 8), (2, 4))),
    }


@jax.custom_vjp
def low(v):
    return lax.optimization_barrier(v.astype(jnp.bfloat16)).astype(jnp.float32)

@jax.custom_vjp
def low_back(v):
    return v

def low_keep(v):
    return (low(v), None)

def low_pass(kept, grad):
    return (grad,)

def back_keep(v):
    return (v, None)

def back_low(kept, grad):
    return (low(grad),)
low.defvjp(low_keep, low_pass)
low_back.defvjp(back_keep, back_low)
HIGH = lax.Precision.HIGHEST
NEG = -1e+30
EPS = 1e-05

def owners(positions, starts):
    inside = (positions[:, None] >= starts[None, :]) & (positions[:, None] < starts[None, :] + PIC)
    return lax.optimization_barrier(jnp.max(jnp.where(inside, starts[None, :], -1), axis=1)).astype(jnp.int32)

def layer_norm(values, gain, shift):
    centre = values - lax.optimization_barrier(jnp.mean(values, axis=-1, keepdims=True))
    spread = lax.optimization_barrier(jnp.mean(centre * centre, axis=-1, keepdims=True))
    return centre * lax.rsqrt(spread + EPS) * gain + shift

def layer(inputs, starts, qkv_weight, qv_bias, out_weight, out_bias, norm1_gain, norm1_bias, up_weight, up_bias, down_weight, down_bias, norm2_gain, norm2_bias):
    length = inputs.shape[0]
    width = inputs.shape[1]
    head_size = width // HEADS
    joined = jnp.dot(inputs, qkv_weight, precision=HIGH)
    queries = low_back(low(joined[:, :width] + qv_bias[:width]))
    keys = low_back(low(joined[:, width:2 * width]))
    values = low_back(low(joined[:, 2 * width:] + qv_bias[width:]))
    positions = jnp.arange(length, dtype=jnp.int32)
    owner = owners(positions, starts)
    key_heads = keys.reshape(length, HEADS, head_size)
    value_heads = values.reshape(length, HEADS, head_size)
    rows = math.gcd(length, 512)
    blocks = length // rows
    scale = 1.0 / math.sqrt(head_size)

    def attend(item):
        query_block, query_pos, query_owner = item
        scores = jnp.einsum('qhd,khd->hqk', query_block, key_heads, precision=HIGH) * scale
        scores = low_back(scores)
        later = positions[None, :] <= query_pos[:, None]
        shared = (owner[None, :] == query_owner[:, None]) & (query_owner[:, None] >= 0)
        scores = jnp.where((later | shared)[None], scores, NEG)
        top = lax.optimization_barrier(jnp.max(scores, axis=-1, keepdims=True))
        expo = jnp.exp(scores - top)
        probs = low(expo / lax.optimization_barrier(jnp.sum(expo, axis=-1, keepdims=True)))
        return jnp.einsum('hqk,khd->qhd', probs, value_heads, precision=HIGH)
    attended = lax.map(jax.checkpoint(attend), (queries.reshape(blocks, rows, HEADS, head_size), positions.reshape(blocks, rows), owner.reshape(blocks, rows)))
    attended = low_back(low(attended.reshape(length, width)))
    branch1 = low_back(jnp.dot(attended, out_weight, precision=HIGH) + out_bias)
    mixed1 = layer_norm(inputs + branch1, norm1_gain, norm1_bias)
    inner = low(mixed1)
    pre = low_back(jnp.dot(inner, up_weight, precision=HIGH) + up_bias)
    act = low(jax.nn.gelu(pre, approximate=False))
    branch2 = low_back(jnp.dot(act, down_weight, precision=HIGH) + down_bias)
    return layer_norm(mixed1 + branch2, norm2_gain, norm2_bias)

def reference(tokens, piece_starts, qkv_weight, qv_bias, out_weight, out_bias, norm1_gain, norm1_bias, up_weight, up_bias, down_weight, down_bias, norm2_gain, norm2_bias, grad_out):
    params = tuple((item.astype(jnp.float32) for item in (qkv_weight, qv_bias, out_weight, out_bias, norm1_gain, norm1_bias, up_weight, up_bias, down_weight, down_bias, norm2_gain, norm2_bias)))
    count = tokens.shape[0] * tokens.shape[1]
    inputs = tokens.astype(jnp.float32).reshape(count, tokens.shape[2], tokens.shape[3])
    cotans = grad_out.astype(jnp.float32).reshape(count, tokens.shape[2], tokens.shape[3])
    starts = piece_starts.reshape(count, piece_starts.shape[2]).astype(jnp.int32)

    def step(totals, item):
        sequence, start_row, cotan = item

        def forward(values, *weights):
            return layer(values, start_row, *weights)
        result, pullback = jax.vjp(forward, sequence, *params)
        grads = pullback(cotan)
        totals = tuple((total + grad for total, grad in zip(totals, grads[1:])))
        return (totals, (result.astype(jnp.bfloat16), grads[0]))
    initial = tuple((jnp.zeros(item.shape, jnp.float32) for item in params))
    totals, (outputs, input_grads) = lax.scan(step, initial, (inputs, starts, cotans))
    return (outputs.reshape(tokens.shape), input_grads.reshape(tokens.shape), totals[0], totals[1], totals[2], totals[3], totals[4], totals[5], totals[6], totals[7], totals[8], totals[9], totals[10], totals[11])
```

```python
import functools
import math

import jax
import jax.numpy as jnp
from jax import lax
from jax.experimental import pallas as pl
from jax.experimental.pallas import tpu as pltpu
from jax.sharding import PartitionSpec as P

HEADS = 12
PIC = 256


NEG = -1e30
EPS = 1e-05


def owners(positions, starts):
    inside = (positions[:, None] >= starts[None, :]) & (positions[:, None] < starts[None, :] + PIC)
    return jnp.max(jnp.where(inside, starts[None, :], -1), axis=1)


def visible_mask(query_pos, query_owner, key_pos, key_owner):
    later = key_pos[None, :] <= query_pos[:, None]
    shared = (key_owner[None, :] == query_owner[:, None]) & (query_owner[:, None] >= 0)
    return later | shared


def normalize(values):
    centre = values - jnp.mean(values, axis=-1, keepdims=True)
    inverse = lax.rsqrt(jnp.mean(centre * centre, axis=-1, keepdims=True) + EPS)
    return (centre * inverse, inverse)


def norm_back(upstream, normed, inverse, gain):
    scaled = upstream * gain
    return inverse * (
        scaled
        - jnp.mean(scaled, axis=-1, keepdims=True)
        - normed * jnp.mean(scaled * normed, axis=-1, keepdims=True)
    )


def matmul(left, right):
    return jnp.dot(left, right, preferred_element_type=jnp.float32)


def left_trans(left, right):
    return lax.dot_general(
        left, right, (((0,), (0,)), ((), ())), preferred_element_type=jnp.float32
    )


def right_trans(left, right):
    return lax.dot_general(
        left, right, (((1,), (1,)), ((), ())), preferred_element_type=jnp.float32
    )


def key_blocks(count):
    size = math.gcd(count, 1024)
    return (size, count // size)


def gather_forward(shards):
    return (
        lax.all_gather(shards[0], ("dp", "seq"), axis=0, tiled=True),
        lax.all_gather(shards[1], ("dp", "seq"), axis=0, tiled=True),
        lax.all_gather(shards[2], ("dp", "seq"), axis=0, tiled=True),
        lax.all_gather(shards[3], ("dp", "seq"), axis=0, tiled=True),
        lax.all_gather(shards[4], ("dp", "seq"), axis=0, tiled=True),
        lax.all_gather(shards[5], ("dp", "seq"), axis=0, tiled=True),
        lax.all_gather(shards[6], ("dp", "seq"), axis=0, tiled=True),
        lax.all_gather(shards[7], ("dp", "seq"), axis=0, tiled=True),
        lax.all_gather(shards[8], ("dp", "seq"), axis=0, tiled=True),
        lax.all_gather(shards[9], ("dp", "seq"), axis=0, tiled=True),
        lax.all_gather(shards[10], ("dp", "seq"), axis=0, tiled=True),
        lax.all_gather(shards[11], ("dp", "seq"), axis=0, tiled=True),
    )


def gather_backward(shards):
    return (
        lax.all_gather(shards[0], ("dp", "seq"), axis=0, tiled=True),
        lax.all_gather(shards[1], ("dp", "seq"), axis=0, tiled=True),
        lax.all_gather(shards[2], ("dp", "seq"), axis=0, tiled=True),
        lax.all_gather(shards[3], ("dp", "seq"), axis=0, tiled=True),
        lax.all_gather(shards[4], ("dp", "seq"), axis=0, tiled=True),
        lax.all_gather(shards[5], ("dp", "seq"), axis=0, tiled=True),
        lax.all_gather(shards[6], ("dp", "seq"), axis=0, tiled=True),
        lax.all_gather(shards[7], ("dp", "seq"), axis=0, tiled=True),
        lax.all_gather(shards[8], ("dp", "seq"), axis=0, tiled=True),
        lax.all_gather(shards[9], ("dp", "seq"), axis=0, tiled=True),
        lax.all_gather(shards[10], ("dp", "seq"), axis=0, tiled=True),
        lax.all_gather(shards[11], ("dp", "seq"), axis=0, tiled=True),
    )


def column_sum(values):
    return jnp.sum(values.astype(jnp.float32), axis=0)


def on_device(
    tokens,
    piece_starts,
    qkv_weight,
    qv_bias,
    out_weight,
    out_bias,
    norm1_gain,
    norm1_bias,
    up_weight,
    up_bias,
    down_weight,
    down_bias,
    norm2_gain,
    norm2_bias,
    grad_out,
):
    shards = (
        qkv_weight,
        qv_bias,
        out_weight,
        out_bias,
        norm1_gain,
        norm1_bias,
        up_weight,
        up_bias,
        down_weight,
        down_bias,
        norm2_gain,
        norm2_bias,
    )
    micro_count = tokens.shape[0]
    rows = tokens.shape[2]
    width = tokens.shape[3]
    head_size = width // HEADS
    scale = 1.0 / math.sqrt(head_size)
    length = rows * lax.axis_size("seq")
    query_pos = lax.axis_index("seq") * rows + jnp.arange(rows, dtype=jnp.int32)
    totals = None
    outputs = []
    input_grads = []
    for micro in range(micro_count):
        params = gather_forward(shards)
        (
            full_qkv,
            full_qvb,
            full_out,
            full_outb,
            full_g1,
            full_b1,
            full_up,
            full_upb,
            full_down,
            full_downb,
            full_g2,
            full_b2,
        ) = params
        starts = piece_starts[micro, 0]
        query_owner = owners(query_pos, starts)
        source = tokens[micro, 0]
        joined = matmul(source, full_qkv)
        queries = (joined[:, :width] + full_qvb[:width].astype(jnp.float32)).astype(jnp.bfloat16)
        keys = joined[:, width : 2 * width].astype(jnp.bfloat16)
        values = (joined[:, 2 * width :] + full_qvb[width:].astype(jnp.float32)).astype(
            jnp.bfloat16
        )
        query_heads = queries.reshape(rows, HEADS, head_size)

        def block_scores(key_block, key_pos):
            scores = (
                jnp.einsum(
                    "qhd,khd->hqk", query_heads, key_block, preferred_element_type=jnp.float32
                )
                * scale
            )
            allowed = visible_mask(query_pos, query_owner, key_pos, owners(key_pos, starts))
            return jnp.where(allowed[None], scores, NEG)

        initial = (
            jnp.full((HEADS, rows), NEG, jnp.float32),
            jnp.zeros((HEADS, rows), jnp.float32),
            jnp.zeros((HEADS, rows, head_size), jnp.float32),
        )
        key_piece = lax.all_gather(keys, "seq", axis=0, tiled=True)
        value_piece = lax.all_gather(values, "seq", axis=0, tiled=True)
        size, count = key_blocks(key_piece.shape[0])

        def one(block, carry):
            run_max, total, accum = carry
            key_block = lax.dynamic_slice_in_dim(key_piece, block * size, size, 0).reshape(
                size, HEADS, head_size
            )
            value_block = lax.dynamic_slice_in_dim(value_piece, block * size, size, 0).reshape(
                size, HEADS, head_size
            )
            key_pos = block * size + jnp.arange(size, dtype=jnp.int32)
            scores = block_scores(key_block, key_pos)
            new_max = jnp.maximum(run_max, jnp.max(scores, axis=-1))
            factor = jnp.exp(run_max - new_max)
            weights = jnp.exp(scores - new_max[:, :, None])
            total = total * factor + jnp.sum(weights, axis=-1)
            accum = accum * factor[:, :, None] + jnp.einsum(
                "hqk,khd->hqd",
                weights.astype(jnp.bfloat16),
                value_block,
                preferred_element_type=jnp.float32,
            )
            return (new_max, total, accum)

        run_max, total, accum = lax.fori_loop(0, count, one, initial)
        lse = run_max + jnp.log(total)
        exact = (accum / total[:, :, None]).transpose(1, 0, 2)
        attended = exact.reshape(rows, width).astype(jnp.bfloat16)
        resid1 = (
            source.astype(jnp.float32) + matmul(attended, full_out) + full_outb.astype(jnp.float32)
        )
        normed1, inverse1 = normalize(resid1)
        gain1 = full_g1.astype(jnp.float32)
        mixed1 = normed1 * gain1 + full_b1.astype(jnp.float32)
        inner = mixed1.astype(jnp.bfloat16)
        pre = matmul(inner, full_up) + full_upb.astype(jnp.float32)
        act = jax.nn.gelu(pre, approximate=False).astype(jnp.bfloat16)
        resid2 = mixed1 + matmul(act, full_down) + full_downb.astype(jnp.float32)
        normed2, inverse2 = normalize(resid2)
        gain2 = full_g2.astype(jnp.float32)
        outputs.append((normed2 * gain2 + full_b2.astype(jnp.float32)).astype(jnp.bfloat16))
        back = gather_backward(shards)
        back_qkv = back[0]
        back_out = back[2]
        back_up = back[6]
        back_down = back[8]
        cotan = grad_out[micro, 0].astype(jnp.float32)
        d_resid2 = norm_back(cotan, normed2, inverse2, gain2)
        grad_g2 = jnp.sum(cotan * normed2, axis=0)
        grad_b2 = jnp.sum(cotan, axis=0)
        d_branch2 = d_resid2.astype(jnp.bfloat16)
        grad_downb = column_sum(d_branch2)
        grad_down = left_trans(act, d_branch2)
        d_act = right_trans(d_branch2, back_down)
        gelu_value, gelu_back = jax.vjp(lambda value: jax.nn.gelu(value, approximate=False), pre)
        d_pre = gelu_back(d_act)[0].astype(jnp.bfloat16)
        grad_upb = column_sum(d_pre)
        grad_up = left_trans(inner, d_pre)
        d_mixed1 = d_resid2 + right_trans(d_pre, back_up)
        d_resid1 = norm_back(d_mixed1, normed1, inverse1, gain1)
        grad_g1 = jnp.sum(d_mixed1 * normed1, axis=0)
        grad_b1 = jnp.sum(d_mixed1, axis=0)
        d_branch1 = d_resid1.astype(jnp.bfloat16)
        grad_outb = column_sum(d_branch1)
        grad_out_w = left_trans(attended, d_branch1)
        d_attended = right_trans(d_branch1, back_out).astype(jnp.bfloat16)
        grad_heads = d_attended.reshape(rows, HEADS, head_size)
        delta = jnp.sum(grad_heads.astype(jnp.float32) * exact, axis=-1).T
        initial_back = (
            jnp.zeros((rows, HEADS, head_size), jnp.float32),
            jnp.zeros((length, width), jnp.float32),
            jnp.zeros((length, width), jnp.float32),
        )
        fold_key_piece = lax.all_gather(keys, "seq", axis=0, tiled=True)
        fold_value_piece = lax.all_gather(values, "seq", axis=0, tiled=True)
        fold_size, fold_count = key_blocks(fold_key_piece.shape[0])

        def fold_one(block, carry):
            query_grad, key_grads, value_grads = carry
            offset = block * fold_size
            key_block = lax.dynamic_slice_in_dim(fold_key_piece, offset, fold_size, 0).reshape(
                fold_size, HEADS, head_size
            )
            value_block = lax.dynamic_slice_in_dim(fold_value_piece, offset, fold_size, 0).reshape(
                fold_size, HEADS, head_size
            )
            key_pos = offset + jnp.arange(fold_size, dtype=jnp.int32)
            probs = jnp.exp(block_scores(key_block, key_pos) - lse[:, :, None])
            d_probs = jnp.einsum(
                "qhd,khd->hqk", grad_heads, value_block, preferred_element_type=jnp.float32
            )
            d_scores = (probs * (d_probs - delta[:, :, None])).astype(jnp.bfloat16)
            query_grad = (
                query_grad
                + jnp.einsum(
                    "hqk,khd->qhd", d_scores, key_block, preferred_element_type=jnp.float32
                )
                * scale
            )
            key_part = (
                jnp.einsum(
                    "hqk,qhd->khd", d_scores, query_heads, preferred_element_type=jnp.float32
                ).reshape(fold_size, width)
                * scale
            )
            value_part = jnp.einsum(
                "hqk,qhd->khd",
                probs.astype(jnp.bfloat16),
                grad_heads,
                preferred_element_type=jnp.float32,
            ).reshape(fold_size, width)
            key_grads = lax.dynamic_update_slice_in_dim(
                key_grads,
                lax.dynamic_slice_in_dim(key_grads, offset, fold_size, 0) + key_part,
                offset,
                0,
            )
            value_grads = lax.dynamic_update_slice_in_dim(
                value_grads,
                lax.dynamic_slice_in_dim(value_grads, offset, fold_size, 0) + value_part,
                offset,
                0,
            )
            return (query_grad, key_grads, value_grads)

        query_grad, key_grads, value_grads = lax.fori_loop(0, fold_count, fold_one, initial_back)
        key_grad, value_grad = (
            lax.psum_scatter(
                key_grads.astype(jnp.bfloat16), "seq", scatter_dimension=0, tiled=True
            ).astype(jnp.float32),
            lax.psum_scatter(
                value_grads.astype(jnp.bfloat16), "seq", scatter_dimension=0, tiled=True
            ).astype(jnp.float32),
        )
        query_share = query_grad.reshape(rows, width)
        d_queries = query_share.astype(jnp.bfloat16)
        d_keys = key_grad.astype(jnp.bfloat16)
        d_values = value_grad.astype(jnp.bfloat16)
        d_joined = jnp.concatenate([d_queries, d_keys, d_values], axis=1)
        grad_qvb = jnp.concatenate([column_sum(d_queries), column_sum(d_values)], axis=0)
        grad_qkv = left_trans(source, d_joined)
        input_grads.append(d_resid1 + right_trans(d_joined, back_qkv))
        terms = (
            grad_qkv,
            grad_qvb,
            grad_out_w,
            grad_outb,
            grad_g1,
            grad_b1,
            grad_up,
            grad_upb,
            grad_down,
            grad_downb,
            grad_g2,
            grad_b2,
        )
        if totals is None:
            totals = terms
        else:
            totals = tuple((first + second for first, second in zip(totals, terms)))
    shares = lax.psum_scatter(totals, ("dp", "seq"), scatter_dimension=0, tiled=True)
    layer_out = jnp.stack(outputs)[:, None]
    tokens_grad = jnp.stack(input_grads)[:, None]
    return (
        layer_out,
        tokens_grad,
        shares[0],
        shares[1],
        shares[2],
        shares[3],
        shares[4],
        shares[5],
        shares[6],
        shares[7],
        shares[8],
        shares[9],
        shares[10],
        shares[11],
    )


MESH = pl.DeviceIdType.MESH
ZS, CS, YS, XS = 4, 2, 2, 2
def place():
    dp = lax.axis_index("dp"); seq = lax.axis_index("seq")
    return dp // CS, dp % CS, seq // XS, seq % XS
def dev(z, c, y, x):
    return (z * CS + c, y * XS + x)
def greet(z, c, y, x):
    barrier = pltpu.get_barrier_semaphore()
    partners = [dev((z + k) % ZS, c, y, x) for k in (1, 2, 3)]
    partners += [dev(z, 1 - c, y, x), dev(z, c, 1 - y, x), dev(z, c, y, 1 - x)]
    for p in partners:
        pl.semaphore_signal(barrier, inc=1, device_id=p, device_id_type=MESH)
    pl.semaphore_wait(barrier, len(partners))
def gather_body(n, *refs):
    ins, tok = refs[:n], refs[n]
    outs, tout = refs[n + 1:2 * n + 1], refs[2 * n + 1]
    (loc, zs, zr, xs, xr, ys, yr, as_, ar, bs, br, cs, cr, ts, tr) = refs[2 * n + 2:]
    z, c, y, x = place()
    X, Y = 1 - x, 1 - y
    xn, yn, cn = dev(z, c, y, X), dev(z, c, Y, x), dev(z, 1 - c, y, x)
    greet(z, c, y, x)
    def rc(src, dst, s, r, d):
        return pltpu.make_async_remote_copy(src_ref=src, dst_ref=dst, send_sem=s, recv_sem=r, device_id=d, device_id_type=MESH)
    sent = []
    def go(cp):
        cp.start(); sent.append(cp)
    local = []
    for w in range(n):
        cp = pltpu.make_async_copy(ins[w], outs[w].at[z, c, y, x], loc.at[w]); cp.start(); local.append(cp)
    cp = pltpu.make_async_copy(tok, tout.at[y, x], loc.at[n]); cp.start(); local.append(cp)
    for w in range(n):
        o = outs[w].at[z, c, y, x]
        for k in (1, 2, 3):
            go(rc(ins[w], o, zs.at[w, k - 1], zr.at[w, k - 1], dev((z + k) % ZS, c, y, x)))
        go(rc(ins[w], o, xs.at[w, 0], xr.at[w, 0], xn))
        go(rc(ins[w], o, ys.at[w, 0], yr.at[w, 0], yn))
        go(rc(ins[w], o, cs.at[w, 0, 0], cr.at[w, 0, 0], cn))
    to = tout.at[y, x]
    go(rc(tok, to, ts.at[0], tr.at[0], xn))
    go(rc(tok, to, ts.at[1], tr.at[1], yn))
    def half(w):
        return ins[w].shape[-1] // 2
    def relay(w, k):
        q = (z + ZS - k) % ZS
        bx, by = outs[w].at[q, c, y, X], outs[w].at[q, c, Y, x]
        rc(bx, bx, xs.at[w, k], xr.at[w, k], xn).wait_recv()
        h = half(w)
        a = outs[w].at[q, c, y, X, :, pl.ds(0, h)]
        go(rc(a, a, as_.at[w, k], ar.at[w, k], yn))
        go(rc(bx, bx, cs.at[w, k, 1], cr.at[w, k, 1], cn))
        rc(by, by, ys.at[w, k], yr.at[w, k], yn).wait_recv()
        b = outs[w].at[q, c, Y, x, :, pl.ds(h, h)]
        go(rc(b, b, bs.at[w, k], br.at[w, k], xn))
        go(rc(by, by, cs.at[w, k, 2], cr.at[w, k, 2], cn))
    for k in range(ZS):
        if k:
            for w in range(n):
                q = (z + ZS - k) % ZS
                o = outs[w].at[q, c, y, x]
                rc(o, o, zs.at[w, k - 1], zr.at[w, k - 1], xn).wait_recv()
                go(rc(o, o, xs.at[w, k], xr.at[w, k], xn))
                go(rc(o, o, ys.at[w, k], yr.at[w, k], yn))
                go(rc(o, o, cs.at[w, k, 0], cr.at[w, k, 0], cn))
        for w in range(n):
            relay(w, k)
        if k == 0:
            hh = tok.shape[-1] // 2
            bx, by = tout.at[y, X], tout.at[Y, x]
            rc(bx, bx, ts.at[0], tr.at[0], xn).wait_recv()
            a = tout.at[y, X, :, :, pl.ds(0, hh)]
            go(rc(a, a, ts.at[2], tr.at[2], yn))
            rc(by, by, ts.at[1], tr.at[1], yn).wait_recv()
            b = tout.at[Y, x, :, :, pl.ds(hh, hh)]
            go(rc(b, b, ts.at[3], tr.at[3], xn))
    for k in range(ZS):
        q = (z + ZS - k) % ZS
        for w in range(n):
            h = half(w)
            d = outs[w].at[q, c, Y, X]
            a = outs[w].at[q, c, Y, X, :, pl.ds(0, h)]
            b = outs[w].at[q, c, Y, X, :, pl.ds(h, h)]
            rc(a, a, as_.at[w, k], ar.at[w, k], yn).wait_recv()
            rc(b, b, bs.at[w, k], br.at[w, k], xn).wait_recv()
            go(rc(d, d, cs.at[w, k, 3], cr.at[w, k, 3], cn))
    hh = tok.shape[-1] // 2
    a = tout.at[Y, X, :, :, pl.ds(0, hh)]
    b = tout.at[Y, X, :, :, pl.ds(hh, hh)]
    rc(a, a, ts.at[2], tr.at[2], yn).wait_recv()
    rc(b, b, ts.at[3], tr.at[3], xn).wait_recv()
    for k in range(ZS):
        q = (z + ZS - k) % ZS
        for w in range(n):
            for j, (yy, xx) in enumerate(((y, x), (y, X), (Y, x), (Y, X))):
                o = outs[w].at[q, 1 - c, yy, xx]
                rc(o, o, cs.at[w, k, j], cr.at[w, k, j], cn).wait_recv()
    for cp in sent:
        cp.wait_send()
    for cp in local:
        cp.wait()
def gather(shards, tok):
    n = len(shards)
    D = pltpu.SemaphoreType.DMA
    outs = [jax.ShapeDtypeStruct((ZS, CS, YS, XS) + s.shape, s.dtype) for s in shards]
    outs.append(jax.ShapeDtypeStruct((YS, XS) + tok.shape, tok.dtype))
    res = pl.pallas_call(
        functools.partial(gather_body, n),
        out_shape=outs,
        in_specs=[pl.BlockSpec(memory_space=pltpu.VMEM)] * (n + 1),
        out_specs=[pl.BlockSpec(memory_space=pl.ANY)] * (n + 1),
        scratch_shapes=[D((n + 1,)), D((n, 3)), D((n, 3)), D((n, 4)), D((n, 4)), D((n, 4)), D((n, 4)), D((n, 4)), D((n, 4)), D((n, 4)), D((n, 4)), D((n, 4, 4)), D((n, 4, 4)), D((4,)), D((4,))],
        compiler_params=pltpu.CompilerParams(collective_id=0, has_side_effects=True),
        name="gather",
    )(*shards, tok)
    return res[:n], res[n]

def scatter_body(n, *refs):
    gs, tp, base = refs[:n], refs[n], refs[n + 1]
    outs, tout = refs[n + 2:2 * n + 2], refs[2 * n + 2]
    k = 2 * n + 3
    hs, rbs, ras, rys, r2as, r2bs, rzs = (refs[k + i * n:k + (i + 1) * n] for i in range(7))
    k += 7 * n
    (tx, ty, t2a, t2b, own, loc, ss, sr, tss, tsr, tl) = refs[k:]
    z, c, y, x = place()
    X, Y = 1 - x, 1 - y
    xn, yn, cn = dev(z, c, y, X), dev(z, c, Y, x), dev(z, 1 - c, y, x)
    greet(z, c, y, x)
    def rc(src, dst, s, r, d):
        return pltpu.make_async_remote_copy(src_ref=src, dst_ref=dst, send_sem=s, recv_sem=r, device_id=d, device_id_type=MESH)
    sent = []
    def go(cp):
        cp.start(); sent.append(cp)
    half = [h.shape[-1] // 2 for h in hs]
    A = [pl.ds(0, h) for h in half]
    B = [pl.ds(h, h) for h in half]
    f32 = jnp.float32
    def swap(w):
        return rc(gs[w].at[:, 1 - c], rbs[w], ss.at[w, 0], sr.at[w, 0], cn)
    def load(w):
        return pltpu.make_async_copy(gs[w].at[:, c], hs[w], loc.at[w])
    for w in range(n):
        load(w).start()
        go(swap(w))
    hh = tp.shape[-1] // 2
    TA, TB = pl.ds(0, hh), pl.ds(hh, hh)
    tload = pltpu.make_async_copy(tp, own, tl.at[0])
    tload.start()
    go(rc(tp.at[:, X, :, :, TA], tx, tss.at[0], tsr.at[0], xn))
    go(rc(tp.at[Y, :, :, :, TB], ty, tss.at[1], tsr.at[1], yn))
    def s1a(w): return rc(hs[w].at[:, :, X, :, A[w]], ras[w], ss.at[w, 1], sr.at[w, 1], xn)
    def s1b(w): return rc(hs[w].at[:, Y, :, :, B[w]], rys[w], ss.at[w, 2], sr.at[w, 2], yn)
    def s2a(w): return rc(hs[w].at[:, Y, x, :, A[w]], r2as[w], ss.at[w, 3], sr.at[w, 3], yn)
    def s2b(w): return rc(hs[w].at[:, y, X, :, B[w]], r2bs[w], ss.at[w, 4], sr.at[w, 4], xn)
    def s3(w, k): return rc(hs[w].at[(z + k) % ZS, y, x], rzs[w].at[k - 1], ss.at[w, 4 + k], sr.at[w, 4 + k], dev((z + k) % ZS, c, y, x))
    def st0(w):
        load(w).wait()
        swap(w).wait_recv()
        def one(i, _):
            for yy in range(YS):
                for xx in range(XS):
                    hs[w][i, yy, xx] = (hs[w][i, yy, xx].astype(f32) + rbs[w][i, yy, xx].astype(f32)).astype(jnp.bfloat16)
            return 0
        lax.fori_loop(0, ZS, one, 0)
        go(s1a(w)); go(s1b(w))
    def st1(w):
        s1a(w).wait_recv(); s1b(w).wait_recv()
        def one(i, _):
            for j in range(2):
                hs[w][i, j, x, :, A[w]] = (hs[w][i, j, x, :, A[w]].astype(f32) + ras[w][i, j].astype(f32)).astype(jnp.bfloat16)
                hs[w][i, y, j, :, B[w]] = (hs[w][i, y, j, :, B[w]].astype(f32) + rys[w][i, j].astype(f32)).astype(jnp.bfloat16)
            return 0
        lax.fori_loop(0, ZS, one, 0)
        go(s2a(w)); go(s2b(w))
    def st2(w):
        s2a(w).wait_recv(); s2b(w).wait_recv()
        def one(i, _):
            hs[w][i, y, x, :, A[w]] = (hs[w][i, y, x, :, A[w]].astype(f32) + r2as[w][i].astype(f32)).astype(jnp.bfloat16)
            hs[w][i, y, x, :, B[w]] = (hs[w][i, y, x, :, B[w]].astype(f32) + r2bs[w][i].astype(f32)).astype(jnp.bfloat16)
            return 0
        lax.fori_loop(0, ZS, one, 0)
        for k in (1, 2, 3):
            go(s3(w, k))
    def st3(w):
        total = hs[w][z, y, x].astype(f32)
        for k in (1, 2, 3):
            s3(w, k).wait_recv()
            total = total + rzs[w][k - 1].astype(f32)
        outs[w][...] = total
    def t1():
        tload.wait()
        rc(tx, tx, tss.at[0], tsr.at[0], xn).wait_recv()
        rc(ty, ty, tss.at[1], tsr.at[1], yn).wait_recv()
        own[Y, x, :, :, TA] = (own[Y, x, :, :, TA].astype(f32) + tx[Y].astype(f32)).astype(jnp.bfloat16)
        own[y, X, :, :, TB] = (own[y, X, :, :, TB].astype(f32) + ty[X].astype(f32)).astype(jnp.bfloat16)
        go(rc(own.at[Y, x, :, :, TA], t2a, tss.at[2], tsr.at[2], yn))
        go(rc(own.at[y, X, :, :, TB], t2b, tss.at[3], tsr.at[3], xn))
    def t2():
        rc(t2a, t2a, tss.at[2], tsr.at[2], yn).wait_recv()
        rc(t2b, t2b, tss.at[3], tsr.at[3], xn).wait_recv()
        tout[:, :, TA] = base[:, :, TA] + tx[y].astype(f32) + t2a[...].astype(f32)
        tout[:, :, TB] = base[:, :, TB] + ty[x].astype(f32) + t2b[...].astype(f32)
    for t in range(n + 4):
        for s, f in enumerate((st0, st1, st2, st3)):
            if 0 <= t - s < n:
                f(t - s)
        if t == 1: t1()
        if t == n + 1: t2()
    for cp in sent:
        cp.wait_send()

def scatter(grads, tpart, base):
    n = len(grads)
    D = pltpu.SemaphoreType.DMA
    V = pltpu.VMEM
    bf = jnp.bfloat16
    outs = [jax.ShapeDtypeStruct(g.shape[4:], jnp.float32) for g in grads] + [jax.ShapeDtypeStruct(base.shape, jnp.float32)]
    rn = [g.shape[4:] for g in grads]
    scr = [V((ZS, YS, XS, r, m), bf) for r, m in rn]
    scr += [V((ZS, YS, XS, r, m), bf) for r, m in rn]
    scr += [V((ZS, 2, r, m // 2), bf) for r, m in rn] * 2
    scr += [V((ZS, r, m // 2), bf) for r, m in rn] * 2
    scr += [V((ZS - 1, r, m), bf) for r, m in rn]
    ts = tpart.shape[2:]
    th = (ts[0], ts[1], ts[2] // 2)
    scr += [V((2,) + th, bf)] * 2 + [V(th, bf)] * 2 + [V(tpart.shape, bf)]
    scr += [D((n,)), D((n, 8)), D((n, 8)), D((4,)), D((4,)), D((1,))]
    res = pl.pallas_call(
        functools.partial(scatter_body, n),
        out_shape=outs,
        in_specs=[pl.BlockSpec(memory_space=pl.ANY)] * (n + 1) + [pl.BlockSpec(memory_space=V)],
        out_specs=[pl.BlockSpec(memory_space=V)] * (n + 1),
        scratch_shapes=scr,
        compiler_params=pltpu.CompilerParams(collective_id=1, has_side_effects=True, vmem_limit_bytes=60 * 2**20),
        name="scatter",
    )(*grads, tpart, base)
    return res[:n], res[n]


def fits(mesh):
    return mesh.shape["dp"] == ZS * CS and mesh.shape["seq"] == YS * XS


def pack(parts, shape):
    joined = jnp.concatenate(parts, axis=-1)
    size = shape[-1] * shape[-2]
    pad = [(0, 0)] * (joined.ndim - 1) + [(0, size - joined.shape[-1])]
    return jnp.pad(joined, pad).reshape(joined.shape[:-1] + shape)


def fast_device(
    tokens, piece_starts, qkv_weight, qv_bias, out_weight, out_bias, norm1_gain, norm1_bias,
    up_weight, up_bias, down_weight, down_bias, norm2_gain, norm2_bias, grad_out,
):
    f32, bf16 = jnp.float32, jnp.bfloat16
    micro_count, _, rows, width = tokens.shape
    head_size = width // HEADS
    scale = 1.0 / math.sqrt(head_size)
    ranks = YS * XS
    length = rows * ranks
    count = micro_count * rows
    small = (qv_bias, out_bias, norm1_gain, norm1_bias, up_bias, down_bias, norm2_gain, norm2_bias)
    widths = [v.shape[0] for v in small]
    vector = pack(small, (8, 256))
    gathered, tok = gather((qkv_weight, out_weight, up_weight, down_weight, vector), tokens[:, 0])
    wqkv, wout, wup, wdown = (g.reshape(-1, g.shape[-1]) for g in gathered[:4])
    flat = gathered[4].reshape(-1, 8 * 256).astype(f32)
    full, at = [], 0
    for w in widths:
        full.append(flat[:, at : at + w].reshape(-1))
        at += w
    qvb, outb, g1, b1, upb, downb, g2, b2 = full
    tok_all = tok.reshape(ranks, micro_count, rows, width).transpose(1, 0, 2, 3)
    tok_all = tok_all.reshape(micro_count * length, width)
    me = lax.axis_index("seq")
    query_pos = me * rows + jnp.arange(rows, dtype=jnp.int32)
    key_pos = jnp.arange(length, dtype=jnp.int32)
    allowed = jnp.stack(
        [
            visible_mask(query_pos, owners(query_pos, s), key_pos, owners(key_pos, s))
            for s in (piece_starts[m, 0] for m in range(micro_count))
        ]
    )
    source = tokens.reshape(count, width)
    queries = (matmul(source, wqkv[:, :width]) + qvb[:width]).astype(bf16)
    kv = matmul(tok_all, wqkv[:, width:])
    keys = kv[:, :width].astype(bf16)
    values = (kv[:, width:] + qvb[width:]).astype(bf16)
    qh = queries.reshape(micro_count, rows, HEADS, head_size)
    kh = keys.reshape(micro_count, length, HEADS, head_size)
    vh = values.reshape(micro_count, length, HEADS, head_size)

    def dot(eq, a, b):
        return jnp.einsum(eq, a, b, preferred_element_type=f32)

    scores = jnp.where(allowed[:, None], dot("mqhd,mkhd->mhqk", qh, kh) * scale, NEG)
    expo = jnp.exp(scores - jnp.max(scores, axis=-1, keepdims=True))
    probs = expo / jnp.sum(expo, axis=-1, keepdims=True)
    probs_low = probs.astype(bf16)
    attended = dot("mhqk,mkhd->mqhd", probs_low, vh).reshape(count, width).astype(bf16)
    resid1 = source.astype(f32) + matmul(attended, wout) + outb
    normed1, inverse1 = normalize(resid1)
    mixed1 = normed1 * g1 + b1
    inner = mixed1.astype(bf16)
    pre = matmul(inner, wup) + upb
    act, gelu_back = jax.vjp(lambda v: jax.nn.gelu(v, approximate=False), pre)
    act = act.astype(bf16)
    resid2 = mixed1 + matmul(act, wdown) + downb
    normed2, inverse2 = normalize(resid2)
    layer_out = (normed2 * g2 + b2).astype(bf16)
    cotan = grad_out.reshape(count, width).astype(f32)
    d_resid2 = norm_back(cotan, normed2, inverse2, g2)
    d_branch2 = d_resid2.astype(bf16)
    grad_down = left_trans(act, d_branch2)
    d_pre = gelu_back(right_trans(d_branch2, wdown))[0].astype(bf16)
    grad_up = left_trans(inner, d_pre)
    d_mixed1 = d_resid2 + right_trans(d_pre, wup)
    d_resid1 = norm_back(d_mixed1, normed1, inverse1, g1)
    d_branch1 = d_resid1.astype(bf16)
    grad_out_w = left_trans(attended, d_branch1)
    d_attended = right_trans(d_branch1, wout).astype(bf16)
    dh = d_attended.reshape(micro_count, rows, HEADS, head_size)
    d_probs = dot("mqhd,mkhd->mhqk", dh, vh)
    delta = jnp.sum(probs * d_probs, axis=-1, keepdims=True)
    d_scores = (probs * (d_probs - delta)).astype(bf16)
    d_queries = (dot("mhqk,mkhd->mqhd", d_scores, kh) * scale).reshape(count, width).astype(bf16)
    d_keys = dot("mhqk,mqhd->mkhd", d_scores, qh) * scale
    d_values = dot("mhqk,mqhd->mkhd", probs_low, dh)
    d_kv = jnp.concatenate(
        [d_keys.reshape(-1, width).astype(bf16), d_values.reshape(-1, width).astype(bf16)], axis=1
    )
    grad_qkv = jnp.concatenate([left_trans(source, d_queries), left_trans(tok_all, d_kv)], axis=1)
    part = right_trans(d_kv, wqkv[:, width:]).reshape(micro_count, ranks, rows, width)
    own = lax.dynamic_index_in_dim(part, me, 1, keepdims=False)
    base = (d_resid1 + right_trans(d_queries, wqkv[:, :width])).reshape(micro_count, rows, width) + own
    part = part.astype(bf16).transpose(1, 0, 2, 3).reshape(YS, XS, micro_count, rows, width)
    terms = (
        jnp.concatenate([column_sum(d_queries), column_sum(d_kv[:, width:])]),
        column_sum(d_branch1),
        jnp.sum(d_mixed1 * normed1, axis=0),
        jnp.sum(d_mixed1, axis=0),
        column_sum(d_pre),
        column_sum(d_branch2),
        jnp.sum(cotan * normed2, axis=0),
        jnp.sum(cotan, axis=0),
    )
    vec_grad = pack([t.reshape(-1, w) for t, w in zip(terms, widths)], (8, 256))
    grads = [
        g.astype(bf16).reshape((ZS, CS, YS, XS, -1, g.shape[-1]))
        for g in (grad_down, grad_up, grad_out_w, grad_qkv)
    ]
    grads.append(vec_grad.astype(bf16).reshape(ZS, CS, YS, XS, 8, 256))
    shares, tokens_grad = scatter(grads, part, base)
    flat = shares[4].reshape(-1)
    vec, at = [], 0
    for w in widths:
        vec.append(flat[at : at + w])
        at += w
    return (
        layer_out.reshape(tokens.shape), tokens_grad.reshape(tokens.shape),
        shares[3], vec[0], shares[2], vec[1], vec[2], vec[3], shares[1], vec[4], shares[0],
        vec[5], vec[6], vec[7],
    )


def solution(mesh):
    return jax.shard_map(
        fast_device if fits(mesh) else on_device,
        mesh=mesh,
        in_specs=(
            P(None, "dp", "seq", None),
            P(None, "dp", None),
            P(("dp", "seq"), None),
            P(("dp", "seq")),
            P(("dp", "seq"), None),
            P(("dp", "seq")),
            P(("dp", "seq")),
            P(("dp", "seq")),
            P(("dp", "seq"), None),
            P(("dp", "seq")),
            P(("dp", "seq"), None),
            P(("dp", "seq")),
            P(("dp", "seq")),
            P(("dp", "seq")),
            P(None, "dp", "seq", None),
        ),
        out_specs=(
            P(None, "dp", "seq", None),
            P(None, "dp", "seq", None),
            P(("dp", "seq"), None),
            P(("dp", "seq")),
            P(("dp", "seq"), None),
            P(("dp", "seq")),
            P(("dp", "seq")),
            P(("dp", "seq")),
            P(("dp", "seq"), None),
            P(("dp", "seq")),
            P(("dp", "seq"), None),
            P(("dp", "seq")),
            P(("dp", "seq")),
            P(("dp", "seq")),
        ),
        check_vma=False,
    )
```

```python
import functools
import math

import jax
import jax.numpy as jnp
from jax import lax
from jax.experimental import pallas as pl
from jax.experimental.pallas import tpu as pltpu
from jax.sharding import PartitionSpec as P

HEADS = 12
PIC = 256


NEG = -1e30
EPS = 1e-05


def owners(positions, starts):
    inside = (positions[:, None] >= starts[None, :]) & (positions[:, None] < starts[None, :] + PIC)
    return jnp.max(jnp.where(inside, starts[None, :], -1), axis=1)


def visible_mask(query_pos, query_owner, key_pos, key_owner):
    later = key_pos[None, :] <= query_pos[:, None]
    shared = (key_owner[None, :] == query_owner[:, None]) & (query_owner[:, None] >= 0)
    return later | shared


def normalize(values):
    centre = values - jnp.mean(values, axis=-1, keepdims=True)
    inverse = lax.rsqrt(jnp.mean(centre * centre, axis=-1, keepdims=True) + EPS)
    return (centre * inverse, inverse)


def norm_back(upstream, normed, inverse, gain):
    scaled = upstream * gain
    return inverse * (
        scaled
        - jnp.mean(scaled, axis=-1, keepdims=True)
        - normed * jnp.mean(scaled * normed, axis=-1, keepdims=True)
    )


def matmul(left, right):
    return jnp.dot(left, right, preferred_element_type=jnp.float32)


def left_trans(left, right):
    return lax.dot_general(
        left, right, (((0,), (0,)), ((), ())), preferred_element_type=jnp.float32
    )


def right_trans(left, right):
    return lax.dot_general(
        left, right, (((1,), (1,)), ((), ())), preferred_element_type=jnp.float32
    )


def key_blocks(count):
    size = math.gcd(count, 1024)
    return (size, count // size)


def gather_forward(shards):
    return (
        lax.all_gather(shards[0], ("dp", "seq"), axis=0, tiled=True),
        lax.all_gather(shards[1], ("dp", "seq"), axis=0, tiled=True),
        lax.all_gather(shards[2], ("dp", "seq"), axis=0, tiled=True),
        lax.all_gather(shards[3], ("dp", "seq"), axis=0, tiled=True),
        lax.all_gather(shards[4], ("dp", "seq"), axis=0, tiled=True),
        lax.all_gather(shards[5], ("dp", "seq"), axis=0, tiled=True),
        lax.all_gather(shards[6], ("dp", "seq"), axis=0, tiled=True),
        lax.all_gather(shards[7], ("dp", "seq"), axis=0, tiled=True),
        lax.all_gather(shards[8], ("dp", "seq"), axis=0, tiled=True),
        lax.all_gather(shards[9], ("dp", "seq"), axis=0, tiled=True),
        lax.all_gather(shards[10], ("dp", "seq"), axis=0, tiled=True),
        lax.all_gather(shards[11], ("dp", "seq"), axis=0, tiled=True),
    )


def gather_backward(shards):
    return (
        lax.all_gather(shards[0], ("dp", "seq"), axis=0, tiled=True),
        lax.all_gather(shards[1], ("dp", "seq"), axis=0, tiled=True),
        lax.all_gather(shards[2], ("dp", "seq"), axis=0, tiled=True),
        lax.all_gather(shards[3], ("dp", "seq"), axis=0, tiled=True),
        lax.all_gather(shards[4], ("dp", "seq"), axis=0, tiled=True),
        lax.all_gather(shards[5], ("dp", "seq"), axis=0, tiled=True),
        lax.all_gather(shards[6], ("dp", "seq"), axis=0, tiled=True),
        lax.all_gather(shards[7], ("dp", "seq"), axis=0, tiled=True),
        lax.all_gather(shards[8], ("dp", "seq"), axis=0, tiled=True),
        lax.all_gather(shards[9], ("dp", "seq"), axis=0, tiled=True),
        lax.all_gather(shards[10], ("dp", "seq"), axis=0, tiled=True),
        lax.all_gather(shards[11], ("dp", "seq"), axis=0, tiled=True),
    )


def column_sum(values):
    return jnp.sum(values.astype(jnp.float32), axis=0)


def on_device(
    tokens,
    piece_starts,
    qkv_weight,
    qv_bias,
    out_weight,
    out_bias,
    norm1_gain,
    norm1_bias,
    up_weight,
    up_bias,
    down_weight,
    down_bias,
    norm2_gain,
    norm2_bias,
    grad_out,
):
    shards = (
        qkv_weight,
        qv_bias,
        out_weight,
        out_bias,
        norm1_gain,
        norm1_bias,
        up_weight,
        up_bias,
        down_weight,
        down_bias,
        norm2_gain,
        norm2_bias,
    )
    micro_count = tokens.shape[0]
    rows = tokens.shape[2]
    width = tokens.shape[3]
    head_size = width // HEADS
    scale = 1.0 / math.sqrt(head_size)
    length = rows * lax.axis_size("seq")
    query_pos = lax.axis_index("seq") * rows + jnp.arange(rows, dtype=jnp.int32)
    totals = None
    outputs = []
    input_grads = []
    for micro in range(micro_count):
        params = gather_forward(shards)
        (
            full_qkv,
            full_qvb,
            full_out,
            full_outb,
            full_g1,
            full_b1,
            full_up,
            full_upb,
            full_down,
            full_downb,
            full_g2,
            full_b2,
        ) = params
        starts = piece_starts[micro, 0]
        query_owner = owners(query_pos, starts)
        source = tokens[micro, 0]
        joined = matmul(source, full_qkv)
        queries = (joined[:, :width] + full_qvb[:width].astype(jnp.float32)).astype(jnp.bfloat16)
        keys = joined[:, width : 2 * width].astype(jnp.bfloat16)
        values = (joined[:, 2 * width :] + full_qvb[width:].astype(jnp.float32)).astype(
            jnp.bfloat16
        )
        query_heads = queries.reshape(rows, HEADS, head_size)

        def block_scores(key_block, key_pos):
            scores = (
                jnp.einsum(
                    "qhd,khd->hqk", query_heads, key_block, preferred_element_type=jnp.float32
                )
                * scale
            )
            allowed = visible_mask(query_pos, query_owner, key_pos, owners(key_pos, starts))
            return jnp.where(allowed[None], scores, NEG)

        initial = (
            jnp.full((HEADS, rows), NEG, jnp.float32),
            jnp.zeros((HEADS, rows), jnp.float32),
            jnp.zeros((HEADS, rows, head_size), jnp.float32),
        )
        key_piece = lax.all_gather(keys, "seq", axis=0, tiled=True)
        value_piece = lax.all_gather(values, "seq", axis=0, tiled=True)
        size, count = key_blocks(key_piece.shape[0])

        def one(block, carry):
            run_max, total, accum = carry
            key_block = lax.dynamic_slice_in_dim(key_piece, block * size, size, 0).reshape(
                size, HEADS, head_size
            )
            value_block = lax.dynamic_slice_in_dim(value_piece, block * size, size, 0).reshape(
                size, HEADS, head_size
            )
            key_pos = block * size + jnp.arange(size, dtype=jnp.int32)
            scores = block_scores(key_block, key_pos)
            new_max = jnp.maximum(run_max, jnp.max(scores, axis=-1))
            factor = jnp.exp(run_max - new_max)
            weights = jnp.exp(scores - new_max[:, :, None])
            total = total * factor + jnp.sum(weights, axis=-1)
            accum = accum * factor[:, :, None] + jnp.einsum(
                "hqk,khd->hqd",
                weights.astype(jnp.bfloat16),
                value_block,
                preferred_element_type=jnp.float32,
            )
            return (new_max, total, accum)

        run_max, total, accum = lax.fori_loop(0, count, one, initial)
        lse = run_max + jnp.log(total)
        exact = (accum / total[:, :, None]).transpose(1, 0, 2)
        attended = exact.reshape(rows, width).astype(jnp.bfloat16)
        resid1 = (
            source.astype(jnp.float32) + matmul(attended, full_out) + full_outb.astype(jnp.float32)
        )
        normed1, inverse1 = normalize(resid1)
        gain1 = full_g1.astype(jnp.float32)
        mixed1 = normed1 * gain1 + full_b1.astype(jnp.float32)
        inner = mixed1.astype(jnp.bfloat16)
        pre = matmul(inner, full_up) + full_upb.astype(jnp.float32)
        act = jax.nn.gelu(pre, approximate=False).astype(jnp.bfloat16)
        resid2 = mixed1 + matmul(act, full_down) + full_downb.astype(jnp.float32)
        normed2, inverse2 = normalize(resid2)
        gain2 = full_g2.astype(jnp.float32)
        outputs.append((normed2 * gain2 + full_b2.astype(jnp.float32)).astype(jnp.bfloat16))
        back = gather_backward(shards)
        back_qkv = back[0]
        back_out = back[2]
        back_up = back[6]
        back_down = back[8]
        cotan = grad_out[micro, 0].astype(jnp.float32)
        d_resid2 = norm_back(cotan, normed2, inverse2, gain2)
        grad_g2 = jnp.sum(cotan * normed2, axis=0)
        grad_b2 = jnp.sum(cotan, axis=0)
        d_branch2 = d_resid2.astype(jnp.bfloat16)
        grad_downb = column_sum(d_branch2)
        grad_down = left_trans(act, d_branch2)
        d_act = right_trans(d_branch2, back_down)
        gelu_value, gelu_back = jax.vjp(lambda value: jax.nn.gelu(value, approximate=False), pre)
        d_pre = gelu_back(d_act)[0].astype(jnp.bfloat16)
        grad_upb = column_sum(d_pre)
        grad_up = left_trans(inner, d_pre)
        d_mixed1 = d_resid2 + right_trans(d_pre, back_up)
        d_resid1 = norm_back(d_mixed1, normed1, inverse1, gain1)
        grad_g1 = jnp.sum(d_mixed1 * normed1, axis=0)
        grad_b1 = jnp.sum(d_mixed1, axis=0)
        d_branch1 = d_resid1.astype(jnp.bfloat16)
        grad_outb = column_sum(d_branch1)
        grad_out_w = left_trans(attended, d_branch1)
        d_attended = right_trans(d_branch1, back_out).astype(jnp.bfloat16)
        grad_heads = d_attended.reshape(rows, HEADS, head_size)
        delta = jnp.sum(grad_heads.astype(jnp.float32) * exact, axis=-1).T
        initial_back = (
            jnp.zeros((rows, HEADS, head_size), jnp.float32),
            jnp.zeros((length, width), jnp.float32),
            jnp.zeros((length, width), jnp.float32),
        )
        fold_key_piece = lax.all_gather(keys, "seq", axis=0, tiled=True)
        fold_value_piece = lax.all_gather(values, "seq", axis=0, tiled=True)
        fold_size, fold_count = key_blocks(fold_key_piece.shape[0])

        def fold_one(block, carry):
            query_grad, key_grads, value_grads = carry
            offset = block * fold_size
            key_block = lax.dynamic_slice_in_dim(fold_key_piece, offset, fold_size, 0).reshape(
                fold_size, HEADS, head_size
            )
            value_block = lax.dynamic_slice_in_dim(fold_value_piece, offset, fold_size, 0).reshape(
                fold_size, HEADS, head_size
            )
            key_pos = offset + jnp.arange(fold_size, dtype=jnp.int32)
            probs = jnp.exp(block_scores(key_block, key_pos) - lse[:, :, None])
            d_probs = jnp.einsum(
                "qhd,khd->hqk", grad_heads, value_block, preferred_element_type=jnp.float32
            )
            d_scores = (probs * (d_probs - delta[:, :, None])).astype(jnp.bfloat16)
            query_grad = (
                query_grad
                + jnp.einsum(
                    "hqk,khd->qhd", d_scores, key_block, preferred_element_type=jnp.float32
                )
                * scale
            )
            key_part = (
                jnp.einsum(
                    "hqk,qhd->khd", d_scores, query_heads, preferred_element_type=jnp.float32
                ).reshape(fold_size, width)
                * scale
            )
            value_part = jnp.einsum(
                "hqk,qhd->khd",
                probs.astype(jnp.bfloat16),
                grad_heads,
                preferred_element_type=jnp.float32,
            ).reshape(fold_size, width)
            key_grads = lax.dynamic_update_slice_in_dim(
                key_grads,
                lax.dynamic_slice_in_dim(key_grads, offset, fold_size, 0) + key_part,
                offset,
                0,
            )
            value_grads = lax.dynamic_update_slice_in_dim(
                value_grads,
                lax.dynamic_slice_in_dim(value_grads, offset, fold_size, 0) + value_part,
                offset,
                0,
            )
            return (query_grad, key_grads, value_grads)

        query_grad, key_grads, value_grads = lax.fori_loop(0, fold_count, fold_one, initial_back)
        key_grad, value_grad = (
            lax.psum_scatter(
                key_grads.astype(jnp.bfloat16), "seq", scatter_dimension=0, tiled=True
            ).astype(jnp.float32),
            lax.psum_scatter(
                value_grads.astype(jnp.bfloat16), "seq", scatter_dimension=0, tiled=True
            ).astype(jnp.float32),
        )
        query_share = query_grad.reshape(rows, width)
        d_queries = query_share.astype(jnp.bfloat16)
        d_keys = key_grad.astype(jnp.bfloat16)
        d_values = value_grad.astype(jnp.bfloat16)
        d_joined = jnp.concatenate([d_queries, d_keys, d_values], axis=1)
        grad_qvb = jnp.concatenate([column_sum(d_queries), column_sum(d_values)], axis=0)
        grad_qkv = left_trans(source, d_joined)
        input_grads.append(d_resid1 + right_trans(d_joined, back_qkv))
        terms = (
            grad_qkv,
            grad_qvb,
            grad_out_w,
            grad_outb,
            grad_g1,
            grad_b1,
            grad_up,
            grad_upb,
            grad_down,
            grad_downb,
            grad_g2,
            grad_b2,
        )
        if totals is None:
            totals = terms
        else:
            totals = tuple((first + second for first, second in zip(totals, terms)))
    shares = lax.psum_scatter(totals, ("dp", "seq"), scatter_dimension=0, tiled=True)
    layer_out = jnp.stack(outputs)[:, None]
    tokens_grad = jnp.stack(input_grads)[:, None]
    return (
        layer_out,
        tokens_grad,
        shares[0],
        shares[1],
        shares[2],
        shares[3],
        shares[4],
        shares[5],
        shares[6],
        shares[7],
        shares[8],
        shares[9],
        shares[10],
        shares[11],
    )


MESH = pl.DeviceIdType.MESH
ZS, CS, YS, XS = 4, 2, 2, 2
def place():
    dp = lax.axis_index("dp"); seq = lax.axis_index("seq")
    return dp // CS, dp % CS, seq // XS, seq % XS
def dev(z, c, y, x):
    return (z * CS + c, y * XS + x)
def greet(z, c, y, x):
    barrier = pltpu.get_barrier_semaphore()
    partners = [dev((z + k) % ZS, c, y, x) for k in (1, 2, 3)]
    partners += [dev(z, 1 - c, y, x), dev(z, c, 1 - y, x), dev(z, c, y, 1 - x)]
    for p in partners:
        pl.semaphore_signal(barrier, inc=1, device_id=p, device_id_type=MESH)
    pl.semaphore_wait(barrier, len(partners))
def block(ref, r, z, c, y, x, *cols):
    at = pl.multiple_of((((z * CS + c) * YS + y) * XS + x) * r, 8)
    return ref.at[(pl.ds(at, r),) + cols]


def gather_tasks(ins, tok, outs, tout, sems):
    n = len(ins)
    (loc, zs, zr, xs, xr, ys, yr, as_, ar, bs, br, cs, cr, ts, tr) = sems
    z, c, y, x = place()
    X, Y = 1 - x, 1 - y
    xn, yn, cn = dev(z, c, y, X), dev(z, c, Y, x), dev(z, 1 - c, y, x)

    def rc(src, dst, s, r, d):
        return pltpu.make_async_remote_copy(src_ref=src, dst_ref=dst, send_sem=s, recv_sem=r, device_id=d, device_id_type=MESH)

    sent, local = [], []

    def go(cp):
        cp.start()
        sent.append(cp)

    hh = tok.shape[-1] // 2

    def begin():
        greet(z, c, y, x)
        for w in range(n + 1):
            pair = (ins[w], block(outs[w], ins[w].shape[0], z, c, y, x)) if w < n else (tok, tout.at[y, x])
            cp = pltpu.make_async_copy(*pair, loc.at[w])
            cp.start()
            local.append(cp)
        for w in range(n):
            o = block(outs[w], ins[w].shape[0], z, c, y, x)
            for k in (1, 2, 3):
                go(rc(ins[w], o, zs.at[w, k - 1], zr.at[w, k - 1], dev((z + k) % ZS, c, y, x)))
            go(rc(ins[w], o, xs.at[w, 0], xr.at[w, 0], xn))
            go(rc(ins[w], o, ys.at[w, 0], yr.at[w, 0], yn))
            go(rc(ins[w], o, cs.at[w, 0, 0], cr.at[w, 0, 0], cn))
            if w == 1:
                to = tout.at[y, x]
                go(rc(tok, to, ts.at[0], tr.at[0], xn))
                go(rc(tok, to, ts.at[1], tr.at[1], yn))

    def line(w, k):
        o = block(outs[w], ins[w].shape[0], (z + ZS - k) % ZS, c, y, x)
        rc(o, o, zs.at[w, k - 1], zr.at[w, k - 1], xn).wait_recv()
        go(rc(o, o, xs.at[w, k], xr.at[w, k], xn))
        go(rc(o, o, ys.at[w, k], yr.at[w, k], yn))
        go(rc(o, o, cs.at[w, k, 0], cr.at[w, k, 0], cn))

    def relay(w, k):
        q = (z + ZS - k) % ZS
        bx, by = block(outs[w], ins[w].shape[0], q, c, y, X), block(outs[w], ins[w].shape[0], q, c, Y, x)
        h = ins[w].shape[-1] // 2
        rc(bx, bx, xs.at[w, k], xr.at[w, k], xn).wait_recv()
        a = block(outs[w], ins[w].shape[0], q, c, y, X, pl.ds(0, h))
        go(rc(a, a, as_.at[w, k], ar.at[w, k], yn))
        go(rc(bx, bx, cs.at[w, k, 1], cr.at[w, k, 1], cn))
        rc(by, by, ys.at[w, k], yr.at[w, k], yn).wait_recv()
        b = block(outs[w], ins[w].shape[0], q, c, Y, x, pl.ds(h, h))
        go(rc(b, b, bs.at[w, k], br.at[w, k], xn))
        go(rc(by, by, cs.at[w, k, 2], cr.at[w, k, 2], cn))

    def corner(w, k):
        h = ins[w].shape[-1] // 2
        q = (z + ZS - k) % ZS
        d = block(outs[w], ins[w].shape[0], q, c, Y, X)
        a = block(outs[w], ins[w].shape[0], q, c, Y, X, pl.ds(0, h))
        b = block(outs[w], ins[w].shape[0], q, c, Y, X, pl.ds(h, h))
        rc(a, a, as_.at[w, k], ar.at[w, k], yn).wait_recv()
        rc(b, b, bs.at[w, k], br.at[w, k], xn).wait_recv()
        go(rc(d, d, cs.at[w, k, 3], cr.at[w, k, 3], cn))

    def arrive(w, k):
        q = (z + ZS - k) % ZS
        for j, (yy, xx) in enumerate(((y, x), (y, X), (Y, x), (Y, X))):
            o = block(outs[w], ins[w].shape[0], q, 1 - c, yy, xx)
            rc(o, o, cs.at[w, k, j], cr.at[w, k, j], cn).wait_recv()

    def own(w):
        local[w].wait()

    def tok_relay():
        bx, by = tout.at[y, X], tout.at[Y, x]
        rc(bx, bx, ts.at[0], tr.at[0], xn).wait_recv()
        a = tout.at[y, X, :, :, pl.ds(0, hh)]
        go(rc(a, a, ts.at[2], tr.at[2], yn))
        rc(by, by, ts.at[1], tr.at[1], yn).wait_recv()
        b = tout.at[Y, x, :, :, pl.ds(hh, hh)]
        go(rc(b, b, ts.at[3], tr.at[3], xn))

    def tok_corner():
        a = tout.at[Y, X, :, :, pl.ds(0, hh)]
        b = tout.at[Y, X, :, :, pl.ds(hh, hh)]
        rc(a, a, ts.at[2], tr.at[2], yn).wait_recv()
        rc(b, b, ts.at[3], tr.at[3], xn).wait_recv()
        local[n].wait()

    def finish():
        for cp in sent:
            cp.wait_send()

    P = functools.partial
    tasks = {"start": [begin], "end": [finish]}
    K = range(ZS)

    def lines(w): return [P(line, w, k) for k in K if k]
    def relays(w): return [P(relay, w, k) for k in K]
    def ends(w): return [P(corner, w, k) for k in K]
    def last(w): return [P(arrive, w, k) for k in K] + [P(own, w)]

    tasks[0] = lines(0) + lines(1) + relays(0) + relays(1) + [tok_relay] + lines(2) + lines(3) + ends(0) + ends(1)
    tasks[1] = lines(4) + relays(2) + last(0) + last(1)
    tasks[(2, 0)] = [tok_corner] + relays(3)[:2]
    tasks[(2, 1)] = relays(3)[2:] + ends(2)
    tasks[(2, 2)] = relays(4)[:1] + last(2)
    tasks[(3, 0)] = relays(4)[1:2] + ends(3)[:1]
    tasks[(3, 1)] = relays(4)[2:3] + ends(3)[1:2]
    tasks[(3, 2)] = relays(4)[3:] + ends(3)[2:]
    tasks[(3, 3)] = ends(4)[:2] + last(3)
    tasks[4] = ends(4)[2:] + last(4)
    return tasks


F32, BF16 = jnp.float32, jnp.bfloat16
LANE = 128


def nt(a, b):
    return lax.dot_general(a, b, (((1,), (1,)), ((), ())), preferred_element_type=F32)


def tn(a, b):
    return lax.dot_general(a, b, (((0,), (0,)), ((), ())), preferred_element_type=F32)


def chunks(total, size, body):
    def one(i, _):
        body(pl.ds(pl.multiple_of(i * size, size), size))
        return 0

    lax.fori_loop(0, total // size, one, 0)


def spread(width, per, owners_count):
    n = lax.broadcasted_iota(jnp.int32, (1, width), 1)
    block = jnp.floor((n.astype(F32) + 0.5) / per).astype(jnp.int32)
    pick = lax.broadcasted_iota(jnp.int32, (LANE, width), 0) == n - block * per
    mine = lax.broadcasted_iota(jnp.int32, (owners_count, width), 0) == block
    return pick.astype(F32), mine.astype(F32)


def split_heads(v):
    low = lax.broadcasted_iota(jnp.int32, v.shape, 1) < v.shape[1] // 2
    return jnp.concatenate([jnp.where(low, v, 0.0), jnp.where(low, 0.0, v)], axis=0).astype(BF16)


def join_heads(v):
    half = v.shape[0] // 2
    low = lax.broadcasted_iota(jnp.int32, (half, v.shape[1]), 1) < v.shape[1] // 2
    return jnp.where(low, v[:half], v[half:])


def front_body(widths, *refs):
    (svec, sqkv, sout, sup, sdown, tok, cot, starts) = refs[:8]
    (gvec, gqkv, gout, gup, gdown, tout, lout, probs, qs, kv, att, normed1, inv1, inner, act, gp, dres2, rows, sums) = refs[8:27]
    (wqkv, wout, wup, wdown, vecs, bias, mixed, wsem) = refs[27:35]
    comm = refs[35:]
    micro, nrow, width = tok.shape
    count = micro * nrow
    length = nrow * YS * XS
    ff = sup.shape[1]
    ins = (svec, sqkv, sout, sup, sdown)
    outs = (gvec, gqkv, gout, gup, gdown)
    tasks = gather_tasks(ins, tok, outs, tout, comm)
    run = lambda name: [f() for f in tasks[name]]
    run("start")
    lin = [(gvec, vecs), (gqkv, wqkv), (gout, wout), (gup, wup), (gdown, wdown)]

    def fetch(w):
        src, dst = lin[w]
        cp = pltpu.make_async_copy(src.reshape(dst.shape) if w == 0 else src, dst, wsem.at[w])
        cp.start()
        return cp

    seq = lax.axis_index("seq")
    qpos = seq * nrow + lax.broadcasted_iota(jnp.int32, (nrow, length), 0)
    kpos = lax.broadcasted_iota(jnp.int32, (nrow, length), 1)
    for m in range(micro):
        ok = kpos <= qpos
        for j in range(starts.shape[1]):
            s = starts[m, j]
            both = (qpos >= s) & (qpos < s + PIC) & (kpos >= s) & (kpos < s + PIC)
            ok = ok | both
        bias[m] = jnp.where(ok, 0.0, NEG)
    run(0)
    run(1)
    first = [fetch(0), fetch(1)]
    for cp in first:
        cp.wait()
    nown = vecs.shape[0]
    made = {}
    for r, n in enumerate(widths):
        if n not in made:
            made[n] = spread(n * nown, n, nown)
        pick, mine = made[n]
        got = jnp.dot(vecs[:, r, 0:LANE], pick, preferred_element_type=F32)
        rows[r : r + 1, 0 : n * nown] = jnp.sum(got * mine, axis=0, keepdims=True)
    src = tok[...].reshape(count, width)
    head_scale = 1.0 / math.sqrt(width // HEADS)

    def make_q(at):
        qs[:, at] = (jnp.dot(tok[...].reshape(count, width), wqkv[:, at], preferred_element_type=F32) + rows[0:1, at]).astype(BF16)

    chunks(width, 384, make_q)
    run((2, 0))
    for m in range(micro):
        whole = tout[:, :, m].reshape(length, width)

        def make_k(i, _):
            at = pl.ds(pl.multiple_of(width + i * 384, 128), 384)
            to = pl.ds(pl.multiple_of(i * 384, 128), 384)
            kv[m, :, to] = jnp.dot(whole, wqkv[:, at], preferred_element_type=F32).astype(BF16)
            return 0

        def make_v(i, _):
            at = pl.ds(pl.multiple_of(2 * width + i * 384, 128), 384)
            to = pl.ds(pl.multiple_of(width + i * 384, 128), 384)
            kv[m, :, to] = (jnp.dot(whole, wqkv[:, at], preferred_element_type=F32) + rows[0:1, to]).astype(BF16)
            return 0

        lax.fori_loop(0, width // 384, make_k, 0)
        lax.fori_loop(0, width // 384, make_v, 0)
        run((2, 1 + m))
    pairs = width // LANE
    for m in range(micro):
        both = jnp.concatenate([bias[m], bias[m]], axis=0)

        def attend(p, _):
            at = pl.ds(pl.multiple_of(p * LANE, LANE), LANE)
            vat = pl.ds(pl.multiple_of(width + p * LANE, LANE), LANE)
            q2 = split_heads(qs[m * nrow : (m + 1) * nrow, at].astype(F32) * head_scale)
            score = nt(q2, kv[m, :, at]) + jnp.concatenate([bias[m], bias[m]], axis=0)
            expo = jnp.exp(score - jnp.max(score, axis=1, keepdims=True))
            low = (expo * (1.0 / jnp.sum(expo, axis=1, keepdims=True))).astype(BF16)
            probs[m * pairs + p] = low
            o = join_heads(jnp.dot(low, kv[m, :, vat], preferred_element_type=F32))
            att[m * nrow : (m + 1) * nrow, at] = o.astype(BF16)
            return 0

        for part in range(2):
            lax.fori_loop(part * pairs // 2, (part + 1) * pairs // 2, attend, 0)
            run((3, 2 * m + part))
    cp = [fetch(2), fetch(3)]
    cp[0].wait()

    def project(at):
        normed1[:, at] = tok[:, :, at].reshape(count, 384).astype(F32) + jnp.dot(att[...], wout[:, at], preferred_element_type=F32) + rows[1:2, at]

    chunks(width, 384, project)
    res = normed1[...]
    centre = res - jnp.mean(res, axis=1, keepdims=True)
    inverse = lax.rsqrt(jnp.mean(centre * centre, axis=1, keepdims=True) + EPS)
    norm = centre * inverse
    normed1[...] = norm
    inv1[...] = jnp.broadcast_to(inverse, inv1.shape)
    mix = norm * rows[2:3, 0:width] + rows[3:4, 0:width]
    mixed[...] = mix
    inner[...] = mix.astype(BF16)
    cp[1].wait()

    def feed(at):
        pre = jnp.dot(inner[...], wup[:, at], preferred_element_type=F32) + rows[4:5, at]
        cdf = 0.5 * (1.0 + lax.erf(pre * math.sqrt(0.5)))
        act[:, at] = (pre * cdf).astype(BF16)
        gp[:, at] = (cdf + pre * jnp.exp(-0.5 * pre * pre) * (1.0 / math.sqrt(2.0 * math.pi))).astype(BF16)

    chunks(ff, 512, feed)
    run(4)
    last = fetch(4)
    last.wait()

    def out2(at):
        dres2[:, at] = mixed[:, at] + jnp.dot(act[...], wdown[:, at], preferred_element_type=F32) + rows[5:6, at]

    chunks(width, 256, out2)
    res = dres2[...]
    centre = res - jnp.mean(res, axis=1, keepdims=True)
    inverse = lax.rsqrt(jnp.mean(centre * centre, axis=1, keepdims=True) + EPS)
    norm = centre * inverse
    gain = rows[6:7, 0:width]
    lout[...] = (norm * gain + rows[7:8, 0:width]).astype(BF16)
    up = cot[...].astype(F32)
    scaled = up * gain
    dres = inverse * (scaled - jnp.mean(scaled, axis=1, keepdims=True) - norm * jnp.mean(scaled * norm, axis=1, keepdims=True))
    dres2[...] = dres
    sums[0:1] = jnp.sum(dres.astype(BF16).astype(F32), axis=0, keepdims=True)
    sums[1:2] = jnp.sum(up * norm, axis=0, keepdims=True)
    sums[2:3] = jnp.sum(up, axis=0, keepdims=True)
    run("end")


def front(shards, tok, cot, starts, widths):
    n = len(shards)
    D, V, ANY = pltpu.SemaphoreType.DMA, pltpu.VMEM, pl.ANY
    micro, nrow, width = tok.shape
    count, length, ff = micro * nrow, nrow * YS * XS, shards[3].shape[1]
    pairs = micro * width // LANE
    S = jax.ShapeDtypeStruct
    outs = [S((ZS * CS * YS * XS * s.shape[0], s.shape[1]), s.dtype) for s in shards]
    vm = [
        S((YS, XS) + tok.shape, BF16), S((count, width), BF16), S((pairs, 2 * nrow, length), BF16),
        S((count, width), BF16), S((micro, length, 2 * width), BF16), S((count, width), BF16),
        S((count, width), F32), S((count, LANE), F32), S((count, width), BF16), S((count, ff), BF16),
        S((count, ff), BF16), S((count, width), F32), S((8, ff), F32), S((8, width), F32),
    ]
    total = ZS * CS * YS * XS
    scr = [V((total * s.shape[0], s.shape[1]), BF16) for s in shards[1:]]
    scr += [V((total,) + shards[0].shape, F32), V((micro, nrow, length), F32), V((count, width), F32), D((n,))]
    scr += [D((n + 1,)), D((n, 3)), D((n, 3))] + [D((n, 4))] * 8 + [D((n, 4, 4))] * 2 + [D((4,))] * 2
    return pl.pallas_call(
        functools.partial(front_body, widths),
        out_shape=outs + vm,
        in_specs=[pl.BlockSpec(memory_space=V)] * (n + 2) + [pl.BlockSpec(memory_space=pltpu.SMEM)],
        out_specs=[pl.BlockSpec(memory_space=ANY)] * n + [pl.BlockSpec(memory_space=V)] * len(vm),
        scratch_shapes=scr,
        compiler_params=pltpu.CompilerParams(collective_id=0, has_side_effects=True, vmem_limit_bytes=63 * 2**20),
        name="front",
    )(*shards, tok, cot, starts)


def scatter_tasks(gs, stage, tparts, outs, tout, hold, sems):
    n = len(gs)
    hs, rbs, ras, rys, r2as, r2bs, rzs = (hold[i * n : (i + 1) * n] for i in range(7))
    tx, ty, t2a, t2b, base = hold[7 * n :]
    loc, wr, ss, sr, tss, tsr, cs, cr = sems
    z, c, y, x = place()
    X, Y = 1 - x, 1 - y
    xn, yn, cn = dev(z, c, y, X), dev(z, c, Y, x), dev(z, 1 - c, y, x)

    def rc(src, dst, s, r, d):
        return pltpu.make_async_remote_copy(src_ref=src, dst_ref=dst, send_sem=s, recv_sem=r, device_id=d, device_id_type=MESH)

    sent = []

    def go(cp):
        cp.start()
        sent.append(cp)

    A = [pl.ds(0, h.shape[-1] // 2) for h in hs]
    B = [pl.ds(h.shape[-1] // 2, h.shape[-1] // 2) for h in hs]
    hh = tparts.shape[-1] // 2
    TA, TB = pl.ds(0, hh), pl.ds(hh, hh)

    def write(w):
        return pltpu.make_async_copy(stage[w], gs[w].reshape(stage[w].shape) if w == n - 1 else gs[w], wr.at[w])

    spots = [(i, yy, xx) for i in range(ZS) for yy in range(YS) for xx in range(XS)]

    def load(w, k):
        i, yy, xx = spots[k]
        return pltpu.make_async_copy(block(gs[w], hs[w].shape[3], i, c, yy, xx), hs[w].at[i, yy, xx], loc.at[w, k])

    def swap(w, k):
        i, yy, xx = spots[k]
        return rc(block(gs[w], hs[w].shape[3], i, 1 - c, yy, xx), rbs[w].at[i, yy, xx], cs.at[w, k], cr.at[w, k], cn)

    def s1a(w): return rc(hs[w].at[:, :, X, :, A[w]], ras[w], ss.at[w, 1], sr.at[w, 1], xn)
    def s1b(w): return rc(hs[w].at[:, Y, :, :, B[w]], rys[w], ss.at[w, 2], sr.at[w, 2], yn)
    def s2a(w): return rc(hs[w].at[:, Y, x, :, A[w]], r2as[w], ss.at[w, 3], sr.at[w, 3], yn)
    def s2b(w): return rc(hs[w].at[:, y, X, :, B[w]], r2bs[w], ss.at[w, 4], sr.at[w, 4], xn)
    def s3(w, k): return rc(hs[w].at[(z + k) % ZS, y, x], rzs[w].at[k - 1], ss.at[w, 4 + k], sr.at[w, 4 + k], dev((z + k) % ZS, c, y, x))

    def put(w):
        write(w).start()

    def post(w):
        write(w).wait()
        for k in range(len(spots)):
            load(w, k).start()
            go(swap(w, k))

    def plus(a, b, t):
        return (a.astype(F32) + b.astype(F32)).astype(t)

    def st0(w):
        for k in range(len(spots)):
            load(w, k).wait()
            swap(w, k).wait_recv()

        def one(i, _):
            for yy in range(YS):
                for xx in range(XS):
                    hs[w][i, yy, xx] = plus(hs[w][i, yy, xx], rbs[w][i, yy, xx], hs[w].dtype)
            return 0

        lax.fori_loop(0, ZS, one, 0)
        go(s1a(w))
        go(s1b(w))

    def st1(w):
        s1a(w).wait_recv()
        s1b(w).wait_recv()

        def one(i, _):
            for j in range(2):
                hs[w][i, j, x, :, A[w]] = plus(hs[w][i, j, x, :, A[w]], ras[w][i, j], hs[w].dtype)
                hs[w][i, y, j, :, B[w]] = plus(hs[w][i, y, j, :, B[w]], rys[w][i, j], hs[w].dtype)
            return 0

        lax.fori_loop(0, ZS, one, 0)
        go(s2a(w))
        go(s2b(w))

    def st2(w):
        s2a(w).wait_recv()
        s2b(w).wait_recv()

        def one(i, _):
            hs[w][i, y, x, :, A[w]] = plus(hs[w][i, y, x, :, A[w]], r2as[w][i], hs[w].dtype)
            hs[w][i, y, x, :, B[w]] = plus(hs[w][i, y, x, :, B[w]], r2bs[w][i], hs[w].dtype)
            return 0

        lax.fori_loop(0, ZS, one, 0)
        for k in (1, 2, 3):
            go(s3(w, k))

    def st3(w):
        total = hs[w][z, y, x].astype(F32)
        for k in (1, 2, 3):
            s3(w, k).wait_recv()
            total = total + rzs[w][k - 1].astype(F32)
        outs[w][...] = total

    def t0():
        go(rc(tparts.at[:, X, :, :, TA], tx, tss.at[0], tsr.at[0], xn))
        go(rc(tparts.at[Y, :, :, :, TB], ty, tss.at[1], tsr.at[1], yn))

    def t1():
        rc(tx, tx, tss.at[0], tsr.at[0], xn).wait_recv()
        rc(ty, ty, tss.at[1], tsr.at[1], yn).wait_recv()
        tparts[Y, x, :, :, TA] = plus(tparts[Y, x, :, :, TA], tx[Y], BF16)
        tparts[y, X, :, :, TB] = plus(tparts[y, X, :, :, TB], ty[X], BF16)
        go(rc(tparts.at[Y, x, :, :, TA], t2a, tss.at[2], tsr.at[2], yn))
        go(rc(tparts.at[y, X, :, :, TB], t2b, tss.at[3], tsr.at[3], xn))

    def t2():
        rc(t2a, t2a, tss.at[2], tsr.at[2], yn).wait_recv()
        rc(t2b, t2b, tss.at[3], tsr.at[3], xn).wait_recv()
        own = base[...].reshape(tout.shape) + tparts[y, x].astype(F32)
        low = jnp.concatenate([tx[y].astype(F32) + t2a[...].astype(F32), ty[x].astype(F32) + t2b[...].astype(F32)], axis=2)
        tout[...] = own + low

    def done():
        for cp in sent:
            cp.wait_send()

    return lambda: greet(z, c, y, x), put, post, (st0, st1, st2, st3), (t0, t1, t2), done


def back_body(widths, *refs):
    (wg, tok, probs, qs, kv, att, normed1, inv1, inner, act, gp, dres2, rows, sums) = (refs[0:4],) + refs[4:17]
    k = 17
    outs, tout, gs = refs[k : k + 5], refs[k + 5], refs[k + 6 : k + 11]
    k += 11
    wdown, wup, wout, wqkv, dpre, dkv, dq, datt, tpart, vscr = refs[k : k + 10]
    k += 10
    hold = refs[k : k + 40]
    base = hold[39]
    wsem, gsem = refs[k + 40 : k + 42]
    sems = refs[k + 42 :]
    micro, nrow, width = tok.shape[2:]
    count, length = micro * nrow, nrow * YS * XS
    ff = act.shape[1]
    pairs = width // LANE
    seq = lax.axis_index("seq")
    stage = (wdown, wup, wout, wqkv, vscr)
    begin, put, post, (st0, st1, st2, st3), (t0, t1, t2), done = scatter_tasks(gs, stage, tpart, outs, tout, hold, sems)
    loads = [pltpu.make_async_copy(wg[i], stage[i], wsem.at[i]) for i in range(4)]
    gload = pltpu.make_async_copy(gp, dpre, gsem.at[0])
    gload.start()
    for cp in loads:
        cp.start()
    begin()
    head_scale = 1.0 / math.sqrt(width // HEADS)
    vscr[...] = jnp.zeros(vscr.shape, F32)
    nown = vscr.shape[0]

    def vec(r, value):
        n = widths[r]
        pick, mine = spread(n * nown, n, nown)
        vscr[:, r, 0:LANE] = lax.dot_general(value * mine, pick, (((1,), (1,)), ((), ())), precision=lax.Precision.HIGHEST, preferred_element_type=F32)

    gload.wait()
    loads[0].wait()
    half = 512

    def feed(at):
        d = nt(dres2[...].astype(BF16), wdown[at, :])
        dpre[:, at] = (d * dpre[:, at].astype(F32)).astype(BF16)

    chunks(ff, half, feed)

    def gdown(at):
        wdown[at, :] = tn(act[:, at], dres2[...].astype(BF16)).astype(BF16)

    chunks(ff, half, gdown)
    put(0)
    loads[1].wait()

    def dmix(at):
        base[:, at] = dres2[:, at] + nt(dpre[...], wup[at, :])

    chunks(width, 256, dmix)
    post(0)

    def gup(at):
        wup[:, at] = tn(inner[...], dpre[:, at]).astype(BF16)

    chunks(ff, half, gup)
    put(1)
    dm, normed = base[...], normed1[...]
    vec(2, jnp.sum(dm * normed, axis=0, keepdims=True))
    vec(3, jnp.sum(dm, axis=0, keepdims=True))
    scaled = dm * rows[2:3, 0:width]
    d1 = inv1[:, 0:1] * (scaled - jnp.mean(scaled, axis=1, keepdims=True) - normed * jnp.mean(scaled * normed, axis=1, keepdims=True))
    base[...] = d1
    vec(1, jnp.sum(d1.astype(BF16).astype(F32), axis=0, keepdims=True))
    post(1)
    st0(0)
    loads[2].wait()

    def back_out(at):
        datt[:, at] = nt(base[...].astype(BF16), wout[at, :]).astype(BF16)

    chunks(width, 384, back_out)

    def gout(at):
        wout[:, at] = tn(att[...], base[:, at].astype(BF16)).astype(BF16)

    chunks(width, 384, gout)
    put(2)
    pumps = [lambda: st0(1), lambda: (post(2), st1(0)), lambda: (st0(2), st1(1), st2(0)), lambda: (st1(2), st2(1))]
    for m in range(micro):
        mrow = slice(m * nrow, (m + 1) * nrow)

        def attend(p, _):
            at = pl.ds(pl.multiple_of(p * LANE, LANE), LANE)
            vat = pl.ds(pl.multiple_of(width + p * LANE, LANE), LANE)
            q2 = split_heads(qs[mrow, at].astype(F32) * head_scale)
            o2 = split_heads(datt[mrow, at].astype(F32))
            low = probs[m * pairs + p]
            prob = low.astype(F32)
            dprob = nt(o2, kv[m, :, vat])
            delta = jnp.sum(prob * dprob, axis=1, keepdims=True)
            ds = (prob * (dprob - delta)).astype(BF16)
            dq[mrow, at] = (join_heads(jnp.dot(ds, kv[m, :, at], preferred_element_type=F32)) * head_scale).astype(BF16)
            dkv[m, :, at] = tn(ds, q2).astype(BF16)
            dkv[m, :, vat] = tn(low, o2).astype(BF16)
            return 0

        for part in range(2):
            lax.fori_loop(part * pairs // 2, (part + 1) * pairs // 2, attend, 0)
            pumps[2 * m + part]()
    loads[3].wait()
    for m in range(micro):

        def piece(i, _):
            at = pl.ds(pl.multiple_of(i * 256, 256), 256)
            got = nt(dkv[m], wqkv[at, width : 3 * width])
            tpart[:, :, m, :, at] = got.reshape(YS, XS, nrow, 256).astype(BF16)
            return 0

        lax.fori_loop(0, width // 256, piece, 0)
    t0()

    def dsrc(at):
        base[:, at] = base[:, at] + nt(dq[...], wqkv[at, 0:width])

    chunks(width, 256, dsrc)
    st2(2)
    src = tok.at[seq // XS, seq % XS]

    def gq(at):
        wqkv[:, at] = tn(src[...].reshape(count, width), dq[:, at]).astype(BF16)

    chunks(width, 384, gq)

    def gkv(i, _):
        at = pl.ds(pl.multiple_of(i * 384, 128), 384)
        to = pl.ds(pl.multiple_of(width + i * 384, 128), 384)
        total = tn(tok[:, :, 0].reshape(length, width), dkv[0, :, at])
        for m in range(1, micro):
            total = total + tn(tok[:, :, m].reshape(length, width), dkv[m, :, at])
        wqkv[:, to] = total.astype(BF16)
        return 0

    lax.fori_loop(0, 2 * width // 384, gkv, 0)
    put(3)
    dv = sum(jnp.sum(dkv[m, :, width:].astype(F32), axis=0, keepdims=True) for m in range(micro))
    vec(0, jnp.concatenate([jnp.sum(dq[...].astype(F32), axis=0, keepdims=True), dv], axis=1))
    vec(4, jnp.sum(dpre[...].astype(F32), axis=0, keepdims=True))
    post(3)
    for r in range(3):
        vec(5 + r, sums[r : r + 1])
    put(4)
    st3(0)
    post(4)
    st0(3)
    t1()
    st3(1)
    st0(4)
    st3(2)
    st1(3)
    st1(4)
    t2()
    st2(3)
    st2(4)
    st3(3)
    st3(4)
    done()


def back(weights, saved, widths):
    D, V, ANY = pltpu.SemaphoreType.DMA, pltpu.VMEM, pl.ANY
    S = jax.ShapeDtypeStruct
    tok = saved[0]
    total = ZS * CS * YS * XS
    micro, nrow, width = tok.shape[2:]
    count, length = micro * nrow, nrow * YS * XS
    ff = saved[8].shape[1]
    blocks = [(w.shape[0] // total, w.shape[1]) for w in weights] + [(8, 256)]
    kinds = [BF16] * 4 + [F32]
    both = list(zip(blocks, kinds))
    outs = [S(b, F32) for b in blocks] + [S((micro, nrow, width), F32)]
    outs += [S((total * b[0], b[1]), t) for b, t in both]
    scr = [V((total * b[0], b[1]), BF16) for b in blocks[:4]]
    scr += [V((count, ff), BF16), V((micro, length, 2 * width), BF16), V((count, width), BF16), V((count, width), BF16)]
    scr += [V(tok.shape, BF16), V((total, 8, 256), F32)]
    scr += [V((ZS, YS, XS) + b, t) for b, t in both] * 2
    scr += [V((ZS, 2, b[0], b[1] // 2), t) for b, t in both] * 2
    scr += [V((ZS, b[0], b[1] // 2), t) for b, t in both] * 2
    scr += [V((ZS - 1,) + b, t) for b, t in both]
    th = (micro, nrow, width // 2)
    scr += [V((2,) + th, BF16)] * 2 + [V(th, BF16)] * 2 + [V((count, width), F32)]
    scr += [D((4,)), D((1,)), D((5, 16)), D((5,)), D((5, 8)), D((5, 8)), D((4,)), D((4,)), D((5, 16)), D((5, 16))]
    spec = lambda s: pl.BlockSpec(memory_space=s)
    return pl.pallas_call(
        functools.partial(back_body, widths),
        out_shape=outs,
        in_specs=[spec(ANY)] * 4 + [spec(V)] * 9 + [spec(ANY)] + [spec(V)] * 3,
        out_specs=[spec(V)] * 6 + [spec(ANY)] * 5,
        scratch_shapes=scr,
        compiler_params=pltpu.CompilerParams(collective_id=1, has_side_effects=True, vmem_limit_bytes=67043328),
        name="back",
    )(*weights, *saved)


def fits(mesh):
    return mesh.shape["dp"] == ZS * CS and mesh.shape["seq"] == YS * XS


def fast_device(
    tokens, piece_starts, qkv_weight, qv_bias, out_weight, out_bias, norm1_gain, norm1_bias,
    up_weight, up_bias, down_weight, down_bias, norm2_gain, norm2_bias, grad_out,
):
    micro, _, nrow, width = tokens.shape
    small = (qv_bias, out_bias, norm1_gain, norm1_bias, up_bias, down_bias, norm2_gain, norm2_bias)
    widths = tuple(v.shape[0] for v in small)
    vector = jnp.stack([jnp.pad(v.astype(F32), (0, 256 - v.shape[0])) for v in small])
    cot = grad_out.reshape(micro * nrow, width)
    got = front(
        (vector, qkv_weight, out_weight, up_weight, down_weight), tokens[:, 0], cot, piece_starts[:, 0], widths
    )
    gqkv, gout, gup, gdown = got[1:5]
    layer_out = got[6]
    shares = back((gdown, gup, gout, gqkv), (got[5],) + tuple(got[7:]), widths)
    down, up, out, qkv, vec, tokens_grad = shares[:6]
    v = [vec[r, :n] for r, n in enumerate(widths)]
    return (
        layer_out.reshape(tokens.shape), tokens_grad.reshape(tokens.shape),
        qkv, v[0], out, v[1], v[2], v[3], up, v[4], down, v[5], v[6], v[7],
    )


def solution(mesh):
    return jax.shard_map(
        fast_device if fits(mesh) else on_device,
        mesh=mesh,
        in_specs=(
            P(None, "dp", "seq", None),
            P(None, "dp", None),
            P(("dp", "seq"), None),
            P(("dp", "seq")),
            P(("dp", "seq"), None),
            P(("dp", "seq")),
            P(("dp", "seq")),
            P(("dp", "seq")),
            P(("dp", "seq"), None),
            P(("dp", "seq")),
            P(("dp", "seq"), None),
            P(("dp", "seq")),
            P(("dp", "seq")),
            P(("dp", "seq")),
            P(None, "dp", "seq", None),
        ),
        out_specs=(
            P(None, "dp", "seq", None),
            P(None, "dp", "seq", None),
            P(("dp", "seq"), None),
            P(("dp", "seq")),
            P(("dp", "seq"), None),
            P(("dp", "seq")),
            P(("dp", "seq")),
            P(("dp", "seq")),
            P(("dp", "seq"), None),
            P(("dp", "seq")),
            P(("dp", "seq"), None),
            P(("dp", "seq")),
            P(("dp", "seq")),
            P(("dp", "seq")),
        ),
        check_vma=False,
    )
```

```python
import functools
import math

import jax
import jax.numpy as jnp
from jax import lax
from jax.experimental import pallas as pl
from jax.experimental.pallas import tpu as pltpu
from jax.sharding import PartitionSpec as P

HEADS = 12
PIC = 256


NEG = -1e30
EPS = 1e-05


def owners(positions, starts):
    inside = (positions[:, None] >= starts[None, :]) & (positions[:, None] < starts[None, :] + PIC)
    return jnp.max(jnp.where(inside, starts[None, :], -1), axis=1)


def visible_mask(query_pos, query_owner, key_pos, key_owner):
    later = key_pos[None, :] <= query_pos[:, None]
    shared = (key_owner[None, :] == query_owner[:, None]) & (query_owner[:, None] >= 0)
    return later | shared


def normalize(values):
    centre = values - jnp.mean(values, axis=-1, keepdims=True)
    inverse = lax.rsqrt(jnp.mean(centre * centre, axis=-1, keepdims=True) + EPS)
    return (centre * inverse, inverse)


def norm_back(upstream, normed, inverse, gain):
    scaled = upstream * gain
    return inverse * (
        scaled
        - jnp.mean(scaled, axis=-1, keepdims=True)
        - normed * jnp.mean(scaled * normed, axis=-1, keepdims=True)
    )


def matmul(left, right):
    return jnp.dot(left, right, preferred_element_type=jnp.float32)


def left_trans(left, right):
    return lax.dot_general(
        left, right, (((0,), (0,)), ((), ())), preferred_element_type=jnp.float32
    )


def right_trans(left, right):
    return lax.dot_general(
        left, right, (((1,), (1,)), ((), ())), preferred_element_type=jnp.float32
    )


def key_blocks(count):
    size = math.gcd(count, 1024)
    return (size, count // size)


def gather_forward(shards):
    return (
        lax.all_gather(shards[0], ("dp", "seq"), axis=0, tiled=True),
        lax.all_gather(shards[1], ("dp", "seq"), axis=0, tiled=True),
        lax.all_gather(shards[2], ("dp", "seq"), axis=0, tiled=True),
        lax.all_gather(shards[3], ("dp", "seq"), axis=0, tiled=True),
        lax.all_gather(shards[4], ("dp", "seq"), axis=0, tiled=True),
        lax.all_gather(shards[5], ("dp", "seq"), axis=0, tiled=True),
        lax.all_gather(shards[6], ("dp", "seq"), axis=0, tiled=True),
        lax.all_gather(shards[7], ("dp", "seq"), axis=0, tiled=True),
        lax.all_gather(shards[8], ("dp", "seq"), axis=0, tiled=True),
        lax.all_gather(shards[9], ("dp", "seq"), axis=0, tiled=True),
        lax.all_gather(shards[10], ("dp", "seq"), axis=0, tiled=True),
        lax.all_gather(shards[11], ("dp", "seq"), axis=0, tiled=True),
    )


def gather_backward(shards):
    return (
        lax.all_gather(shards[0], ("dp", "seq"), axis=0, tiled=True),
        lax.all_gather(shards[1], ("dp", "seq"), axis=0, tiled=True),
        lax.all_gather(shards[2], ("dp", "seq"), axis=0, tiled=True),
        lax.all_gather(shards[3], ("dp", "seq"), axis=0, tiled=True),
        lax.all_gather(shards[4], ("dp", "seq"), axis=0, tiled=True),
        lax.all_gather(shards[5], ("dp", "seq"), axis=0, tiled=True),
        lax.all_gather(shards[6], ("dp", "seq"), axis=0, tiled=True),
        lax.all_gather(shards[7], ("dp", "seq"), axis=0, tiled=True),
        lax.all_gather(shards[8], ("dp", "seq"), axis=0, tiled=True),
        lax.all_gather(shards[9], ("dp", "seq"), axis=0, tiled=True),
        lax.all_gather(shards[10], ("dp", "seq"), axis=0, tiled=True),
        lax.all_gather(shards[11], ("dp", "seq"), axis=0, tiled=True),
    )


def column_sum(values):
    return jnp.sum(values.astype(jnp.float32), axis=0)


def on_device(
    tokens,
    piece_starts,
    qkv_weight,
    qv_bias,
    out_weight,
    out_bias,
    norm1_gain,
    norm1_bias,
    up_weight,
    up_bias,
    down_weight,
    down_bias,
    norm2_gain,
    norm2_bias,
    grad_out,
):
    shards = (
        qkv_weight,
        qv_bias,
        out_weight,
        out_bias,
        norm1_gain,
        norm1_bias,
        up_weight,
        up_bias,
        down_weight,
        down_bias,
        norm2_gain,
        norm2_bias,
    )
    micro_count = tokens.shape[0]
    rows = tokens.shape[2]
    width = tokens.shape[3]
    head_size = width // HEADS
    scale = 1.0 / math.sqrt(head_size)
    length = rows * lax.axis_size("seq")
    query_pos = lax.axis_index("seq") * rows + jnp.arange(rows, dtype=jnp.int32)
    totals = None
    outputs = []
    input_grads = []
    for micro in range(micro_count):
        params = gather_forward(shards)
        (
            full_qkv,
            full_qvb,
            full_out,
            full_outb,
            full_g1,
            full_b1,
            full_up,
            full_upb,
            full_down,
            full_downb,
            full_g2,
            full_b2,
        ) = params
        starts = piece_starts[micro, 0]
        query_owner = owners(query_pos, starts)
        source = tokens[micro, 0]
        joined = matmul(source, full_qkv)
        queries = (joined[:, :width] + full_qvb[:width].astype(jnp.float32)).astype(jnp.bfloat16)
        keys = joined[:, width : 2 * width].astype(jnp.bfloat16)
        values = (joined[:, 2 * width :] + full_qvb[width:].astype(jnp.float32)).astype(
            jnp.bfloat16
        )
        query_heads = queries.reshape(rows, HEADS, head_size)

        def block_scores(key_block, key_pos):
            scores = (
                jnp.einsum(
                    "qhd,khd->hqk", query_heads, key_block, preferred_element_type=jnp.float32
                )
                * scale
            )
            allowed = visible_mask(query_pos, query_owner, key_pos, owners(key_pos, starts))
            return jnp.where(allowed[None], scores, NEG)

        initial = (
            jnp.full((HEADS, rows), NEG, jnp.float32),
            jnp.zeros((HEADS, rows), jnp.float32),
            jnp.zeros((HEADS, rows, head_size), jnp.float32),
        )
        key_piece = lax.all_gather(keys, "seq", axis=0, tiled=True)
        value_piece = lax.all_gather(values, "seq", axis=0, tiled=True)
        size, count = key_blocks(key_piece.shape[0])

        def one(block, carry):
            run_max, total, accum = carry
            key_block = lax.dynamic_slice_in_dim(key_piece, block * size, size, 0).reshape(
                size, HEADS, head_size
            )
            value_block = lax.dynamic_slice_in_dim(value_piece, block * size, size, 0).reshape(
                size, HEADS, head_size
            )
            key_pos = block * size + jnp.arange(size, dtype=jnp.int32)
            scores = block_scores(key_block, key_pos)
            new_max = jnp.maximum(run_max, jnp.max(scores, axis=-1))
            factor = jnp.exp(run_max - new_max)
            weights = jnp.exp(scores - new_max[:, :, None])
            total = total * factor + jnp.sum(weights, axis=-1)
            accum = accum * factor[:, :, None] + jnp.einsum(
                "hqk,khd->hqd",
                weights.astype(jnp.bfloat16),
                value_block,
                preferred_element_type=jnp.float32,
            )
            return (new_max, total, accum)

        run_max, total, accum = lax.fori_loop(0, count, one, initial)
        lse = run_max + jnp.log(total)
        exact = (accum / total[:, :, None]).transpose(1, 0, 2)
        attended = exact.reshape(rows, width).astype(jnp.bfloat16)
        resid1 = (
            source.astype(jnp.float32) + matmul(attended, full_out) + full_outb.astype(jnp.float32)
        )
        normed1, inverse1 = normalize(resid1)
        gain1 = full_g1.astype(jnp.float32)
        mixed1 = normed1 * gain1 + full_b1.astype(jnp.float32)
        inner = mixed1.astype(jnp.bfloat16)
        pre = matmul(inner, full_up) + full_upb.astype(jnp.float32)
        act = jax.nn.gelu(pre, approximate=False).astype(jnp.bfloat16)
        resid2 = mixed1 + matmul(act, full_down) + full_downb.astype(jnp.float32)
        normed2, inverse2 = normalize(resid2)
        gain2 = full_g2.astype(jnp.float32)
        outputs.append((normed2 * gain2 + full_b2.astype(jnp.float32)).astype(jnp.bfloat16))
        back = gather_backward(shards)
        back_qkv = back[0]
        back_out = back[2]
        back_up = back[6]
        back_down = back[8]
        cotan = grad_out[micro, 0].astype(jnp.float32)
        d_resid2 = norm_back(cotan, normed2, inverse2, gain2)
        grad_g2 = jnp.sum(cotan * normed2, axis=0)
        grad_b2 = jnp.sum(cotan, axis=0)
        d_branch2 = d_resid2.astype(jnp.bfloat16)
        grad_downb = column_sum(d_branch2)
        grad_down = left_trans(act, d_branch2)
        d_act = right_trans(d_branch2, back_down)
        gelu_value, gelu_back = jax.vjp(lambda value: jax.nn.gelu(value, approximate=False), pre)
        d_pre = gelu_back(d_act)[0].astype(jnp.bfloat16)
        grad_upb = column_sum(d_pre)
        grad_up = left_trans(inner, d_pre)
        d_mixed1 = d_resid2 + right_trans(d_pre, back_up)
        d_resid1 = norm_back(d_mixed1, normed1, inverse1, gain1)
        grad_g1 = jnp.sum(d_mixed1 * normed1, axis=0)
        grad_b1 = jnp.sum(d_mixed1, axis=0)
        d_branch1 = d_resid1.astype(jnp.bfloat16)
        grad_outb = column_sum(d_branch1)
        grad_out_w = left_trans(attended, d_branch1)
        d_attended = right_trans(d_branch1, back_out).astype(jnp.bfloat16)
        grad_heads = d_attended.reshape(rows, HEADS, head_size)
        delta = jnp.sum(grad_heads.astype(jnp.float32) * exact, axis=-1).T
        initial_back = (
            jnp.zeros((rows, HEADS, head_size), jnp.float32),
            jnp.zeros((length, width), jnp.float32),
            jnp.zeros((length, width), jnp.float32),
        )
        fold_key_piece = lax.all_gather(keys, "seq", axis=0, tiled=True)
        fold_value_piece = lax.all_gather(values, "seq", axis=0, tiled=True)
        fold_size, fold_count = key_blocks(fold_key_piece.shape[0])

        def fold_one(block, carry):
            query_grad, key_grads, value_grads = carry
            offset = block * fold_size
            key_block = lax.dynamic_slice_in_dim(fold_key_piece, offset, fold_size, 0).reshape(
                fold_size, HEADS, head_size
            )
            value_block = lax.dynamic_slice_in_dim(fold_value_piece, offset, fold_size, 0).reshape(
                fold_size, HEADS, head_size
            )
            key_pos = offset + jnp.arange(fold_size, dtype=jnp.int32)
            probs = jnp.exp(block_scores(key_block, key_pos) - lse[:, :, None])
            d_probs = jnp.einsum(
                "qhd,khd->hqk", grad_heads, value_block, preferred_element_type=jnp.float32
            )
            d_scores = (probs * (d_probs - delta[:, :, None])).astype(jnp.bfloat16)
            query_grad = (
                query_grad
                + jnp.einsum(
                    "hqk,khd->qhd", d_scores, key_block, preferred_element_type=jnp.float32
                )
                * scale
            )
            key_part = (
                jnp.einsum(
                    "hqk,qhd->khd", d_scores, query_heads, preferred_element_type=jnp.float32
                ).reshape(fold_size, width)
                * scale
            )
            value_part = jnp.einsum(
                "hqk,qhd->khd",
                probs.astype(jnp.bfloat16),
                grad_heads,
                preferred_element_type=jnp.float32,
            ).reshape(fold_size, width)
            key_grads = lax.dynamic_update_slice_in_dim(
                key_grads,
                lax.dynamic_slice_in_dim(key_grads, offset, fold_size, 0) + key_part,
                offset,
                0,
            )
            value_grads = lax.dynamic_update_slice_in_dim(
                value_grads,
                lax.dynamic_slice_in_dim(value_grads, offset, fold_size, 0) + value_part,
                offset,
                0,
            )
            return (query_grad, key_grads, value_grads)

        query_grad, key_grads, value_grads = lax.fori_loop(0, fold_count, fold_one, initial_back)
        key_grad, value_grad = (
            lax.psum_scatter(
                key_grads.astype(jnp.bfloat16), "seq", scatter_dimension=0, tiled=True
            ).astype(jnp.float32),
            lax.psum_scatter(
                value_grads.astype(jnp.bfloat16), "seq", scatter_dimension=0, tiled=True
            ).astype(jnp.float32),
        )
        query_share = query_grad.reshape(rows, width)
        d_queries = query_share.astype(jnp.bfloat16)
        d_keys = key_grad.astype(jnp.bfloat16)
        d_values = value_grad.astype(jnp.bfloat16)
        d_joined = jnp.concatenate([d_queries, d_keys, d_values], axis=1)
        grad_qvb = jnp.concatenate([column_sum(d_queries), column_sum(d_values)], axis=0)
        grad_qkv = left_trans(source, d_joined)
        input_grads.append(d_resid1 + right_trans(d_joined, back_qkv))
        terms = (
            grad_qkv,
            grad_qvb,
            grad_out_w,
            grad_outb,
            grad_g1,
            grad_b1,
            grad_up,
            grad_upb,
            grad_down,
            grad_downb,
            grad_g2,
            grad_b2,
        )
        if totals is None:
            totals = terms
        else:
            totals = tuple((first + second for first, second in zip(totals, terms)))
    shares = lax.psum_scatter(totals, ("dp", "seq"), scatter_dimension=0, tiled=True)
    layer_out = jnp.stack(outputs)[:, None]
    tokens_grad = jnp.stack(input_grads)[:, None]
    return (
        layer_out,
        tokens_grad,
        shares[0],
        shares[1],
        shares[2],
        shares[3],
        shares[4],
        shares[5],
        shares[6],
        shares[7],
        shares[8],
        shares[9],
        shares[10],
        shares[11],
    )


MESH = pl.DeviceIdType.MESH
ZS, CS, YS, XS = 4, 2, 2, 2
def place():
    dp = lax.axis_index("dp"); seq = lax.axis_index("seq")
    return dp // CS, dp % CS, seq // XS, seq % XS
def dev(z, c, y, x):
    return (z * CS + c, y * XS + x)
def greet(z, c, y, x):
    barrier = pltpu.get_barrier_semaphore()
    partners = [dev((z + k) % ZS, c, y, x) for k in (1, 2, 3)]
    partners += [dev(z, 1 - c, y, x), dev(z, c, 1 - y, x), dev(z, c, y, 1 - x)]
    for p in partners:
        pl.semaphore_signal(barrier, inc=1, device_id=p, device_id_type=MESH)
    pl.semaphore_wait(barrier, len(partners))
def block(ref, r, z, c, y, x, *cols):
    at = pl.multiple_of((((z * CS + c) * YS + y) * XS + x) * r, 8)
    return ref.at[(pl.ds(at, r),) + cols]


def gather_tasks(ins, tok, outs, tout, sems):
    n = len(ins)
    (loc, zs, zr, xs, xr, ys, yr, as_, ar, bs, br, cs, cr, ts, tr) = sems
    z, c, y, x = place()
    X, Y = 1 - x, 1 - y
    xn, yn, cn = dev(z, c, y, X), dev(z, c, Y, x), dev(z, 1 - c, y, x)

    def rc(src, dst, s, r, d):
        return pltpu.make_async_remote_copy(src_ref=src, dst_ref=dst, send_sem=s, recv_sem=r, device_id=d, device_id_type=MESH)

    sent, local = [], []

    def go(cp):
        cp.start()
        sent.append(cp)

    hh = tok.shape[-1] // 2

    def begin():
        greet(z, c, y, x)
        for w in range(n + 1):
            pair = (ins[w], block(outs[w], ins[w].shape[0], z, c, y, x)) if w < n else (tok, tout.at[y, x])
            cp = pltpu.make_async_copy(*pair, loc.at[w])
            cp.start()
            local.append(cp)
        for w in range(n):
            o = block(outs[w], ins[w].shape[0], z, c, y, x)
            for k in (1, 2, 3):
                go(rc(ins[w], o, zs.at[w, k - 1], zr.at[w, k - 1], dev((z + k) % ZS, c, y, x)))
            go(rc(ins[w], o, xs.at[w, 0], xr.at[w, 0], xn))
            go(rc(ins[w], o, ys.at[w, 0], yr.at[w, 0], yn))
            go(rc(ins[w], o, cs.at[w, 0, 0], cr.at[w, 0, 0], cn))
            if w == 1:
                to = tout.at[y, x]
                go(rc(tok, to, ts.at[0], tr.at[0], xn))
                go(rc(tok, to, ts.at[1], tr.at[1], yn))

    def line(w, k):
        o = block(outs[w], ins[w].shape[0], (z + ZS - k) % ZS, c, y, x)
        rc(o, o, zs.at[w, k - 1], zr.at[w, k - 1], xn).wait_recv()
        go(rc(o, o, xs.at[w, k], xr.at[w, k], xn))
        go(rc(o, o, ys.at[w, k], yr.at[w, k], yn))
        go(rc(o, o, cs.at[w, k, 0], cr.at[w, k, 0], cn))

    def relay(w, k):
        q = (z + ZS - k) % ZS
        bx, by = block(outs[w], ins[w].shape[0], q, c, y, X), block(outs[w], ins[w].shape[0], q, c, Y, x)
        h = ins[w].shape[-1] // 2
        rc(bx, bx, xs.at[w, k], xr.at[w, k], xn).wait_recv()
        a = block(outs[w], ins[w].shape[0], q, c, y, X, pl.ds(0, h))
        go(rc(a, a, as_.at[w, k], ar.at[w, k], yn))
        go(rc(bx, bx, cs.at[w, k, 1], cr.at[w, k, 1], cn))
        rc(by, by, ys.at[w, k], yr.at[w, k], yn).wait_recv()
        b = block(outs[w], ins[w].shape[0], q, c, Y, x, pl.ds(h, h))
        go(rc(b, b, bs.at[w, k], br.at[w, k], xn))
        go(rc(by, by, cs.at[w, k, 2], cr.at[w, k, 2], cn))

    def corner(w, k):
        h = ins[w].shape[-1] // 2
        q = (z + ZS - k) % ZS
        d = block(outs[w], ins[w].shape[0], q, c, Y, X)
        a = block(outs[w], ins[w].shape[0], q, c, Y, X, pl.ds(0, h))
        b = block(outs[w], ins[w].shape[0], q, c, Y, X, pl.ds(h, h))
        rc(a, a, as_.at[w, k], ar.at[w, k], yn).wait_recv()
        rc(b, b, bs.at[w, k], br.at[w, k], xn).wait_recv()
        go(rc(d, d, cs.at[w, k, 3], cr.at[w, k, 3], cn))

    def arrive(w, k):
        q = (z + ZS - k) % ZS
        for j, (yy, xx) in enumerate(((y, x), (y, X), (Y, x), (Y, X))):
            o = block(outs[w], ins[w].shape[0], q, 1 - c, yy, xx)
            rc(o, o, cs.at[w, k, j], cr.at[w, k, j], cn).wait_recv()

    def own(w):
        local[w].wait()

    def tok_relay():
        bx, by = tout.at[y, X], tout.at[Y, x]
        rc(bx, bx, ts.at[0], tr.at[0], xn).wait_recv()
        a = tout.at[y, X, :, :, pl.ds(0, hh)]
        go(rc(a, a, ts.at[2], tr.at[2], yn))
        rc(by, by, ts.at[1], tr.at[1], yn).wait_recv()
        b = tout.at[Y, x, :, :, pl.ds(hh, hh)]
        go(rc(b, b, ts.at[3], tr.at[3], xn))

    def tok_corner():
        a = tout.at[Y, X, :, :, pl.ds(0, hh)]
        b = tout.at[Y, X, :, :, pl.ds(hh, hh)]
        rc(a, a, ts.at[2], tr.at[2], yn).wait_recv()
        rc(b, b, ts.at[3], tr.at[3], xn).wait_recv()
        local[n].wait()

    def finish():
        for cp in sent:
            cp.wait_send()

    P = functools.partial
    tasks = {"start": [begin], "end": [finish]}
    K = range(ZS)

    def lines(w): return [P(line, w, k) for k in K if k]
    def relays(w): return [P(relay, w, k) for k in K]
    def ends(w): return [P(corner, w, k) for k in K]
    def last(w): return [P(arrive, w, k) for k in K] + [P(own, w)]

    tasks[0] = lines(0) + lines(1) + relays(0) + relays(1) + [tok_relay] + lines(2) + lines(3) + ends(0) + ends(1)
    tasks[1] = lines(4) + relays(2) + last(0) + last(1)
    tasks[(2, 0)] = [tok_corner] + relays(3)[:2]
    tasks[(2, 1)] = relays(3)[2:] + ends(2)
    tasks[(2, 2)] = relays(4)[:1] + last(2)
    tasks[(3, 0)] = relays(4)[1:2] + ends(3)[:1]
    tasks[(3, 1)] = relays(4)[2:3] + ends(3)[1:2]
    tasks[(3, 2)] = relays(4)[3:] + ends(3)[2:]
    tasks[(3, 3)] = ends(4)[:2] + last(3)
    tasks[4] = ends(4)[2:] + last(4)
    return tasks


F32, BF16 = jnp.float32, jnp.bfloat16
LANE = 128


def nt(a, b):
    return lax.dot_general(a, b, (((1,), (1,)), ((), ())), preferred_element_type=F32)


def tn(a, b):
    return lax.dot_general(a, b, (((0,), (0,)), ((), ())), preferred_element_type=F32)


def chunks(total, size, body):
    def one(i, _):
        body(pl.ds(pl.multiple_of(i * size, size), size))
        return 0

    lax.fori_loop(0, total // size, one, 0)


def spread(width, per, owners_count):
    n = lax.broadcasted_iota(jnp.int32, (1, width), 1)
    block = jnp.floor((n.astype(F32) + 0.5) / per).astype(jnp.int32)
    pick = lax.broadcasted_iota(jnp.int32, (LANE, width), 0) == n - block * per
    mine = lax.broadcasted_iota(jnp.int32, (owners_count, width), 0) == block
    return pick.astype(F32), mine.astype(F32)


def split_heads(v):
    low = lax.broadcasted_iota(jnp.int32, v.shape, 1) < v.shape[1] // 2
    return jnp.concatenate([jnp.where(low, v, 0.0), jnp.where(low, 0.0, v)], axis=0).astype(BF16)


def join_heads(v):
    half = v.shape[0] // 2
    low = lax.broadcasted_iota(jnp.int32, (half, v.shape[1]), 1) < v.shape[1] // 2
    return jnp.where(low, v[:half], v[half:])


def scatter_tasks(gs, pieces, tparts, outs, tout, hold, sems):
    n = len(pieces)
    hs, rbs, ras, rys, r2as, r2bs, rzs = (hold[i * n : (i + 1) * n] for i in range(7))
    tx, ty, t2a, t2b, base = hold[7 * n :]
    loc, ss, sr, tss, tsr, cs, cr = sems
    z, c, y, x = place()
    X, Y = 1 - x, 1 - y
    xn, yn, cn = dev(z, c, y, X), dev(z, c, Y, x), dev(z, 1 - c, y, x)

    def rc(src, dst, s, r, d):
        return pltpu.make_async_remote_copy(src_ref=src, dst_ref=dst, send_sem=s, recv_sem=r, device_id=d, device_id_type=MESH)

    sent = []

    def go(cp):
        cp.start()
        sent.append(cp)

    A = [pl.ds(0, h.shape[-1] // 2) for h in hs]
    B = [pl.ds(h.shape[-1] // 2, h.shape[-1] // 2) for h in hs]
    hh = tparts.shape[-1] // 2
    TA, TB = pl.ds(0, hh), pl.ds(hh, hh)

    spots = [(i, yy, xx) for i in range(ZS) for yy in range(YS) for xx in range(XS)]

    def load(w, k):
        i, yy, xx = spots[k]
        return pltpu.make_async_copy(block(gs[pieces[w][0]], hs[w].shape[3], i, c, yy, xx, pl.ds(*pieces[w][1:])), hs[w].at[i, yy, xx], loc.at[w, k])

    def swap(w, k):
        i, yy, xx = spots[k]
        return rc(block(gs[pieces[w][0]], hs[w].shape[3], i, 1 - c, yy, xx, pl.ds(*pieces[w][1:])), rbs[w].at[i, yy, xx], cs.at[w, k], cr.at[w, k], cn)

    def s1a(w): return rc(hs[w].at[:, :, X, :, A[w]], ras[w], ss.at[w, 1], sr.at[w, 1], xn)
    def s1b(w): return rc(hs[w].at[:, Y, :, :, B[w]], rys[w], ss.at[w, 2], sr.at[w, 2], yn)
    def s2a(w): return rc(hs[w].at[:, Y, x, :, A[w]], r2as[w], ss.at[w, 3], sr.at[w, 3], yn)
    def s2b(w): return rc(hs[w].at[:, y, X, :, B[w]], r2bs[w], ss.at[w, 4], sr.at[w, 4], xn)
    def s3(w, k): return rc(hs[w].at[(z + k) % ZS, y, x], rzs[w].at[k - 1], ss.at[w, 4 + k], sr.at[w, 4 + k], dev((z + k) % ZS, c, y, x))

    def post(w):
        for k in range(len(spots)):
            load(w, k).start()
            go(swap(w, k))

    def plus(a, b, t):
        return (a.astype(F32) + b.astype(F32)).astype(t)

    def st0(w):
        for k in range(len(spots)):
            load(w, k).wait()
            swap(w, k).wait_recv()

        def one(i, _):
            for yy in range(YS):
                for xx in range(XS):
                    hs[w][i, yy, xx] = plus(hs[w][i, yy, xx], rbs[w][i, yy, xx], hs[w].dtype)
            return 0

        lax.fori_loop(0, ZS, one, 0)
        go(s1a(w))
        go(s1b(w))

    def st1(w):
        s1a(w).wait_recv()
        s1b(w).wait_recv()

        def one(i, _):
            for j in range(2):
                hs[w][i, j, x, :, A[w]] = plus(hs[w][i, j, x, :, A[w]], ras[w][i, j], hs[w].dtype)
                hs[w][i, y, j, :, B[w]] = plus(hs[w][i, y, j, :, B[w]], rys[w][i, j], hs[w].dtype)
            return 0

        lax.fori_loop(0, ZS, one, 0)
        go(s2a(w))
        go(s2b(w))

    def st2(w):
        s2a(w).wait_recv()
        s2b(w).wait_recv()

        def one(i, _):
            hs[w][i, y, x, :, A[w]] = plus(hs[w][i, y, x, :, A[w]], r2as[w][i], hs[w].dtype)
            hs[w][i, y, x, :, B[w]] = plus(hs[w][i, y, x, :, B[w]], r2bs[w][i], hs[w].dtype)
            return 0

        lax.fori_loop(0, ZS, one, 0)
        for k in (1, 2, 3):
            go(s3(w, k))

    def st3(w):
        total = hs[w][z, y, x].astype(F32)
        for k in (1, 2, 3):
            s3(w, k).wait_recv()
            total = total + rzs[w][k - 1].astype(F32)
        outs[pieces[w][0]][:, pl.ds(*pieces[w][1:])] = total

    def t0():
        go(rc(tparts.at[:, X, :, :, TA], tx, tss.at[0], tsr.at[0], xn))
        go(rc(tparts.at[Y, :, :, :, TB], ty, tss.at[1], tsr.at[1], yn))

    def t1():
        rc(tx, tx, tss.at[0], tsr.at[0], xn).wait_recv()
        rc(ty, ty, tss.at[1], tsr.at[1], yn).wait_recv()
        tparts[Y, x, :, :, TA] = plus(tparts[Y, x, :, :, TA], tx[Y], BF16)
        tparts[y, X, :, :, TB] = plus(tparts[y, X, :, :, TB], ty[X], BF16)
        go(rc(tparts.at[Y, x, :, :, TA], t2a, tss.at[2], tsr.at[2], yn))
        go(rc(tparts.at[y, X, :, :, TB], t2b, tss.at[3], tsr.at[3], xn))

    def t2():
        rc(t2a, t2a, tss.at[2], tsr.at[2], yn).wait_recv()
        rc(t2b, t2b, tss.at[3], tsr.at[3], xn).wait_recv()
        own = base[...].reshape(tout.shape) + tparts[y, x].astype(F32)
        low = jnp.concatenate([tx[y].astype(F32) + t2a[...].astype(F32), ty[x].astype(F32) + t2b[...].astype(F32)], axis=2)
        tout[...] = own + low

    def done():
        for cp in sent:
            cp.wait_send()

    return post, (st0, st1, st2, st3), (t0, t1, t2), done


def mega_body(widths, pieces, *refs):
    nv = len(widths)
    small = refs[:nv]
    (sqkv, sout, sup, sdown, tok, cot, starts) = refs[nv : nv + 7]
    k = nv + 7
    gweights = refs[k : k + 5]
    gs = refs[k + 5 : k + 10]
    lout = refs[k + 10]
    shares, tgrad = refs[k + 11 : k + 16], refs[k + 16]
    k += 17
    (svec, tout, probs, qs, kv, att, normed1, inv1, inner, act, dpre, dres2, rows, sums) = refs[k : k + 14]
    k += 14
    (wqkv, wout, wup, wdown, vecs, bias, datt, dstage) = refs[k : k + 8]
    k += 8
    np_ = len(pieces)
    hold = refs[k : k + 7 * np_ + 5]
    base = hold[-1]
    k += 7 * np_ + 5
    wsem, psem, dsem = refs[k : k + 3]
    comm = refs[k + 3 : k + 18]
    sems = refs[k + 18 :]
    gvec, gqkv, gout, gup, gdown = gweights
    mixed, gp, vscr = base, dpre, vecs
    spare = tok.shape[0] * tok.shape[1] * YS * XS
    tpart = wdown.at[pl.ds(0, spare)].reshape((YS, XS) + tok.shape)
    svec[...] = jnp.zeros(svec.shape, F32)
    for r, v in enumerate(small):
        svec[r : r + 1, 0 : widths[r]] = v[...].astype(F32)
    micro, nrow, width = tok.shape
    count = micro * nrow
    length = nrow * YS * XS
    ff = sup.shape[1]
    ins = (svec, sqkv, sout, sup, sdown)
    outs = (gvec, gqkv, gout, gup, gdown)
    tasks = gather_tasks(ins, tok, outs, tout, comm)
    run = lambda name: [f() for f in tasks[name]]
    run("start")
    lin = [(gvec, vecs), (gqkv, wqkv), (gout, wout), (gup, wup), (gdown, wdown)]

    def fetch(w):
        src, dst = lin[w]
        cp = pltpu.make_async_copy(src.reshape(dst.shape) if w == 0 else src, dst, wsem.at[w])
        cp.start()
        return cp

    seq = lax.axis_index("seq")
    qpos = seq * nrow + lax.broadcasted_iota(jnp.int32, (nrow, length), 0)
    kpos = lax.broadcasted_iota(jnp.int32, (nrow, length), 1)
    for m in range(micro):
        ok = kpos <= qpos
        for j in range(starts.shape[1]):
            s = starts[m, j]
            both = (qpos >= s) & (qpos < s + PIC) & (kpos >= s) & (kpos < s + PIC)
            ok = ok | both
        bias[m] = jnp.where(ok, 0.0, NEG)
    run(0)
    run(1)
    first = [fetch(0), fetch(1)]
    for cp in first:
        cp.wait()
    nown = vecs.shape[0]
    made = {}
    for r, n in enumerate(widths):
        if n not in made:
            made[n] = spread(n * nown, n, nown)
        pick, mine = made[n]
        got = jnp.dot(vecs[:, r, 0:LANE], pick, preferred_element_type=F32)
        rows[r : r + 1, 0 : n * nown] = jnp.sum(got * mine, axis=0, keepdims=True)
    src = tok[...].reshape(count, width)
    head_scale = 1.0 / math.sqrt(width // HEADS)

    def make_q(at):
        qs[:, at] = (jnp.dot(tok[...].reshape(count, width), wqkv[:, at], preferred_element_type=F32) + rows[0:1, at]).astype(BF16)

    chunks(width, 384, make_q)
    run((2, 0))
    for m in range(micro):
        whole = tout[:, :, m].reshape(length, width)

        def make_k(i, _):
            at = pl.ds(pl.multiple_of(width + i * 384, 128), 384)
            to = pl.ds(pl.multiple_of(i * 384, 128), 384)
            kv[m, :, to] = jnp.dot(whole, wqkv[:, at], preferred_element_type=F32).astype(BF16)
            return 0

        def make_v(i, _):
            at = pl.ds(pl.multiple_of(2 * width + i * 384, 128), 384)
            to = pl.ds(pl.multiple_of(width + i * 384, 128), 384)
            kv[m, :, to] = (jnp.dot(whole, wqkv[:, at], preferred_element_type=F32) + rows[0:1, to]).astype(BF16)
            return 0

        lax.fori_loop(0, width // 384, make_k, 0)
        lax.fori_loop(0, width // 384, make_v, 0)
        run((2, 1 + m))
    pairs = width // LANE
    for m in range(micro):
        both = jnp.concatenate([bias[m], bias[m]], axis=0)

        def attend(p, _):
            at = pl.ds(pl.multiple_of(p * LANE, LANE), LANE)
            vat = pl.ds(pl.multiple_of(width + p * LANE, LANE), LANE)
            q2 = split_heads(qs[m * nrow : (m + 1) * nrow, at].astype(F32) * head_scale)
            score = nt(q2, kv[m, :, at]) + jnp.concatenate([bias[m], bias[m]], axis=0)
            expo = jnp.exp(score - jnp.max(score, axis=1, keepdims=True))
            low = (expo * (1.0 / jnp.sum(expo, axis=1, keepdims=True))).astype(BF16)
            probs[m * pairs + p] = low
            o = join_heads(jnp.dot(low, kv[m, :, vat], preferred_element_type=F32))
            att[m * nrow : (m + 1) * nrow, at] = o.astype(BF16)
            return 0

        for part in range(2):
            lax.fori_loop(part * pairs // 2, (part + 1) * pairs // 2, attend, 0)
            run((3, 2 * m + part))
    cp = [fetch(2), fetch(3)]
    cp[0].wait()

    def project(at):
        normed1[:, at] = tok[:, :, at].reshape(count, 384).astype(F32) + jnp.dot(att[...], wout[:, at], preferred_element_type=F32) + rows[1:2, at]

    chunks(width, 384, project)
    res = normed1[...]
    centre = res - jnp.mean(res, axis=1, keepdims=True)
    inverse = lax.rsqrt(jnp.mean(centre * centre, axis=1, keepdims=True) + EPS)
    norm = centre * inverse
    normed1[...] = norm
    inv1[...] = jnp.broadcast_to(inverse, inv1.shape)
    mix = norm * rows[2:3, 0:width] + rows[3:4, 0:width]
    mixed[...] = mix
    inner[...] = mix.astype(BF16)
    cp[1].wait()

    def feed(at):
        pre = jnp.dot(inner[...], wup[:, at], preferred_element_type=F32) + rows[4:5, at]
        cdf = 0.5 * (1.0 + lax.erf(pre * math.sqrt(0.5)))
        act[:, at] = (pre * cdf).astype(BF16)
        gp[:, at] = (cdf + pre * jnp.exp(-0.5 * pre * pre) * (1.0 / math.sqrt(2.0 * math.pi))).astype(BF16)

    chunks(ff, 512, feed)
    run(4)
    last = fetch(4)
    last.wait()

    def out2(at):
        dres2[:, at] = mixed[:, at] + jnp.dot(act[...], wdown[:, at], preferred_element_type=F32) + rows[5:6, at]

    chunks(width, 256, out2)
    res = dres2[...]
    centre = res - jnp.mean(res, axis=1, keepdims=True)
    inverse = lax.rsqrt(jnp.mean(centre * centre, axis=1, keepdims=True) + EPS)
    norm = centre * inverse
    gain = rows[6:7, 0:width]
    lout[...] = (norm * gain + rows[7:8, 0:width]).astype(BF16)
    up = cot[...].astype(F32)
    scaled = up * gain
    dres = inverse * (scaled - jnp.mean(scaled, axis=1, keepdims=True) - norm * jnp.mean(scaled * norm, axis=1, keepdims=True))
    dres2[...] = dres
    sums[0:1] = jnp.sum(dres.astype(BF16).astype(F32), axis=0, keepdims=True)
    sums[1:2] = jnp.sum(up * norm, axis=0, keepdims=True)
    sums[2:3] = jnp.sum(up, axis=0, keepdims=True)
    pairs = width // LANE
    vscr[...] = jnp.zeros(vscr.shape, F32)

    def vec(r, value):
        n = widths[r]
        pick, mine = made[n]
        vscr[:, r, 0:LANE] = lax.dot_general(value * mine, pick, (((1,), (1,)), ((), ())), precision=lax.Precision.HIGHEST, preferred_element_type=F32)

    post, (st0, st1, st2, st3), (t0, t1, t2), done = scatter_tasks(gs, pieces, tpart, shares, tgrad, hold, sems)
    D0, D1, U0, U1, OUT, KV, QQ, VEC = range(8)
    step = dstage.shape[1]

    def drain(slot):
        pltpu.make_async_copy(dstage.at[slot], gs[0].at[pl.ds(0, step)], dsem.at[slot]).wait()

    def gdown_part(i, _):
        slot = lax.rem(i, 2)

        @pl.when(i >= 2)
        def _():
            drain(slot)

        at = pl.ds(pl.multiple_of(i * step, step), step)
        dstage[slot] = tn(act[:, at], dres2[...].astype(BF16)).astype(BF16)
        pltpu.make_async_copy(dstage.at[slot], gs[0].at[at], dsem.at[slot]).start()
        return 0

    lax.fori_loop(0, ff // step, gdown_part, 0)
    drain(0)
    drain(1)
    post(D0)
    post(D1)

    def put(i, src, dst):
        cp = pltpu.make_async_copy(src, dst, psem.at[i])
        cp.start()
        return cp

    def feed_back(at):
        d = nt(dres2[...].astype(BF16), wdown[at, :])
        dpre[:, at] = (d * dpre[:, at].astype(F32)).astype(BF16)

    chunks(ff, 512, feed_back)

    def dmix(at):
        base[:, at] = dres2[:, at] + nt(dpre[...], wup[at, :])

    chunks(width, 256, dmix)
    st0(D0)

    def gup_part(at):
        wup[:, at] = tn(inner[...], dpre[:, at]).astype(BF16)

    chunks(ff, 512, gup_part)
    cp = put(0, wup, gs[1])
    st0(D1)
    dm, normed = base[...], normed1[...]
    vec(2, jnp.sum(dm * normed, axis=0, keepdims=True))
    vec(3, jnp.sum(dm, axis=0, keepdims=True))
    scaled = dm * rows[2:3, 0:width]
    d1 = inv1[:, 0:1] * (scaled - jnp.mean(scaled, axis=1, keepdims=True) - normed * jnp.mean(scaled * normed, axis=1, keepdims=True))
    base[...] = d1
    vec(1, jnp.sum(d1.astype(BF16).astype(F32), axis=0, keepdims=True))
    cp.wait()
    post(U0)
    post(U1)
    st1(D0)

    def back_out(at):
        datt[:, at] = nt(base[...].astype(BF16), wout[at, :]).astype(BF16)

    chunks(width, 384, back_out)

    def gout_part(at):
        wout[:, at] = tn(att[...], base[:, at].astype(BF16)).astype(BF16)

    chunks(width, 384, gout_part)
    cp = put(1, wout, gs[2])
    st0(U0)
    pumps = [[(cp.wait,), (post, OUT), (st1, D1), (st2, D0)], [(st0, U1), (st1, U0)], [(st0, OUT), (st2, D1), (st2, U0)], [(st1, U1), (st1, OUT)]]
    for m in range(micro):
        mrow = slice(m * nrow, (m + 1) * nrow)

        def attend_back(p, _):
            at = pl.ds(pl.multiple_of(p * LANE, LANE), LANE)
            vat = pl.ds(pl.multiple_of(width + p * LANE, LANE), LANE)
            q2 = split_heads(qs[mrow, at].astype(F32) * head_scale)
            o2 = split_heads(datt[mrow, at].astype(F32))
            low = probs[m * pairs + p]
            prob = low.astype(F32)
            dprob = nt(o2, kv[m, :, vat])
            delta = jnp.sum(prob * dprob, axis=1, keepdims=True)
            ds = (prob * (dprob - delta)).astype(BF16)
            datt[mrow, at] = (join_heads(jnp.dot(ds, kv[m, :, at], preferred_element_type=F32)) * head_scale).astype(BF16)
            kv[m, :, at] = tn(ds, q2).astype(BF16)
            kv[m, :, vat] = tn(low, o2).astype(BF16)
            return 0

        for part in range(2):
            lax.fori_loop(part * pairs // 2, (part + 1) * pairs // 2, attend_back, 0)
            for f, *a in pumps[2 * m + part]:
                f(*a)
    dq, dkv = datt, kv
    for m in range(micro):

        def piece(i, _):
            at = pl.ds(pl.multiple_of(i * 256, 256), 256)
            got = nt(dkv[m], wqkv[at, width : 3 * width])
            tpart[:, :, m, :, at] = got.reshape(YS, XS, nrow, 256).astype(BF16)
            return 0

        lax.fori_loop(0, width // 256, piece, 0)
    t0()
    st2(U1)

    def gkv(i, _):
        at = pl.ds(pl.multiple_of(i * 384, 128), 384)
        to = pl.ds(pl.multiple_of(width + i * 384, 128), 384)
        total = tn(tout[:, :, 0].reshape(length, width), dkv[0, :, at])
        for m in range(1, micro):
            total = total + tn(tout[:, :, m].reshape(length, width), dkv[m, :, at])
        wqkv[:, to] = total.astype(BF16)
        return 0

    lax.fori_loop(0, 2 * width // 384, gkv, 0)
    cp = put(2, wqkv.at[:, pl.ds(width, 2 * width)], gs[3].at[:, pl.ds(width, 2 * width)])
    st2(OUT)
    cp.wait()
    post(KV)

    def dsrc(at):
        base[:, at] = base[:, at] + nt(dq[...], wqkv[at, 0:width])

    chunks(width, 256, dsrc)

    def gq(at):
        wqkv[:, at] = tn(tok[...].reshape(count, width), dq[:, at]).astype(BF16)

    chunks(width, 384, gq)
    cp = put(3, wqkv.at[:, pl.ds(0, width)], gs[3].at[:, pl.ds(0, width)])
    dv = sum(jnp.sum(dkv[m, :, width:].astype(F32), axis=0, keepdims=True) for m in range(micro))
    vec(0, jnp.concatenate([jnp.sum(dq[...].astype(F32), axis=0, keepdims=True), dv], axis=1))
    vec(4, jnp.sum(dpre[...].astype(F32), axis=0, keepdims=True))
    for r in range(3):
        vec(5 + r, sums[r : r + 1])
    cp.wait()
    post(QQ)
    st0(KV)
    cp = put(4, vscr, gs[4].reshape(vscr.shape))
    t1()
    cp.wait()
    post(VEC)
    st0(QQ)
    st0(VEC)
    for w in (D0, D1, U0, U1):
        st3(w)
    st1(KV)
    st1(QQ)
    st1(VEC)
    t2()
    st3(OUT)
    for w in (KV, QQ, VEC):
        st2(w)
    for w in (KV, QQ, VEC):
        st3(w)
    done()
    run("end")


def mega(small, shards, tok, cot, starts):
    D, V, ANY = pltpu.SemaphoreType.DMA, pltpu.VMEM, pl.ANY
    micro, nrow, width = tok.shape
    count, length, ff = micro * nrow, nrow * YS * XS, shards[2].shape[1]
    pairs = micro * width // LANE
    S = jax.ShapeDtypeStruct
    widths = tuple(v.shape[1] for v in small)
    total = ZS * CS * YS * XS
    vshape = (8, 256)
    order = (3, 2, 1, 0)
    garr = [(shards[i].shape, BF16) for i in order] + [(vshape, F32)]
    pieces = ((0, 0, width // 3), (0, width // 3, width - width // 3), (1, 0, ff // 2), (1, ff // 2, ff // 2), (2, 0, width), (3, width, 2 * width), (3, 0, width), (4, 0, 256))
    outs = [S((total * vshape[0], vshape[1]), F32)] + [S((total * s.shape[0], s.shape[1]), BF16) for s in shards]
    outs += [S((total * b[0], b[1]), t) for b, t in garr]
    res = [S((count, width), BF16)] + [S(b, F32) for b, _ in garr] + [S((micro, nrow, width), F32)]
    scr = [
        V(vshape, F32), V((YS, XS) + tok.shape, BF16), V((pairs, 2 * nrow, length), BF16), V((count, width), BF16),
        V((micro, length, 2 * width), BF16), V((count, width), BF16), V((count, width), F32), V((count, LANE), F32),
        V((count, width), BF16), V((count, ff), BF16), V((count, ff), BF16), V((count, width), F32), V((8, ff), F32), V((8, width), F32),
    ]
    scr += [V((total * s.shape[0], s.shape[1]), BF16) for s in shards]
    scr += [V((total,) + vshape, F32), V((micro, nrow, length), F32), V((count, width), BF16), V((2, 512, width), BF16)]
    both = [((garr[a][0][0], m), garr[a][1]) for a, _, m in pieces]
    scr += [V((ZS, YS, XS) + b, t) for b, t in both] * 2
    scr += [V((ZS, 2, b[0], b[1] // 2), t) for b, t in both] * 2
    scr += [V((ZS, b[0], b[1] // 2), t) for b, t in both] * 2
    scr += [V((ZS - 1,) + b, t) for b, t in both]
    th = (micro, nrow, width // 2)
    scr += [V((2,) + th, BF16)] * 2 + [V(th, BF16)] * 2 + [V((count, width), F32)]
    n, q = 5, len(pieces)
    scr += [D((n,)), D((n,)), D((2,))]
    scr += [D((n + 1,)), D((n, 3)), D((n, 3))] + [D((n, 4))] * 8 + [D((n, 4, 4))] * 2 + [D((4,))] * 2
    scr += [D((q, 16)), D((q, 8)), D((q, 8)), D((4,)), D((4,)), D((q, 16)), D((q, 16))]
    spec = lambda s: pl.BlockSpec(memory_space=s)
    got = pl.pallas_call(
        functools.partial(mega_body, widths, pieces),
        out_shape=outs + res,
        in_specs=[spec(V)] * (len(small) + 6) + [spec(pltpu.SMEM)],
        out_specs=[spec(ANY)] * 10 + [spec(V)] * len(res),
        scratch_shapes=scr,
        compiler_params=pltpu.CompilerParams(collective_id=0, has_side_effects=True, vmem_limit_bytes=67043328),
        name="layer",
    )(*small, *shards, tok, cot, starts)
    return got[10:]


def finish_body(widths, *refs):
    n = 6
    ins, vec, outs, small = refs[:n], refs[n], refs[n + 1 : 2 * n + 1], refs[2 * n + 1 :]
    for a, b in zip(ins, outs):
        b[...] = a[...]
    for r, o in enumerate(small):
        o[...] = vec[r : r + 1, 0 : widths[r]]


def finish(arrays, vec, widths):
    S = jax.ShapeDtypeStruct
    outs = [S(a.shape, a.dtype) for a in arrays] + [S((1, w), F32) for w in widths]
    spec = pl.BlockSpec(memory_space=pltpu.VMEM)
    return pl.pallas_call(
        functools.partial(finish_body, widths), out_shape=outs,
        in_specs=[spec] * (len(arrays) + 1), out_specs=[spec] * len(outs), name="finish",
    )(*arrays, vec)


def fits(mesh):
    return mesh.shape["dp"] == ZS * CS and mesh.shape["seq"] == YS * XS


def fast_device(
    tokens, piece_starts, qkv_weight, qv_bias, out_weight, out_bias, norm1_gain, norm1_bias,
    up_weight, up_bias, down_weight, down_bias, norm2_gain, norm2_bias, grad_out,
):
    micro, _, nrow, width = tokens.shape
    small = (qv_bias, out_bias, norm1_gain, norm1_bias, up_bias, down_bias, norm2_gain, norm2_bias)
    widths = tuple(v.shape[0] for v in small)
    got = mega(
        tuple(v.reshape(1, -1) for v in small), (qkv_weight, out_weight, up_weight, down_weight),
        tokens[:, 0], grad_out.reshape(micro * nrow, width), piece_starts[:, 0],
    )
    lout, down, up, out, qkv, vec, tgrad = got
    done = finish((lout, tgrad, qkv, out, up, down), vec, widths)
    lout, tgrad, qkv, out, up, down = done[:6]
    v = [a.reshape(-1) for a in done[6:]]
    return (
        lout.reshape(tokens.shape), tgrad.reshape(tokens.shape),
        qkv, v[0], out, v[1], v[2], v[3], up, v[4], down, v[5], v[6], v[7],
    )


def solution(mesh):
    return jax.shard_map(
        fast_device if fits(mesh) else on_device,
        mesh=mesh,
        in_specs=(
            P(None, "dp", "seq", None),
            P(None, "dp", None),
            P(("dp", "seq"), None),
            P(("dp", "seq")),
            P(("dp", "seq"), None),
            P(("dp", "seq")),
            P(("dp", "seq")),
            P(("dp", "seq")),
            P(("dp", "seq"), None),
            P(("dp", "seq")),
            P(("dp", "seq"), None),
            P(("dp", "seq")),
            P(("dp", "seq")),
            P(("dp", "seq")),
            P(None, "dp", "seq", None),
        ),
        out_specs=(
            P(None, "dp", "seq", None),
            P(None, "dp", "seq", None),
            P(("dp", "seq"), None),
            P(("dp", "seq")),
            P(("dp", "seq"), None),
            P(("dp", "seq")),
            P(("dp", "seq")),
            P(("dp", "seq")),
            P(("dp", "seq"), None),
            P(("dp", "seq")),
            P(("dp", "seq"), None),
            P(("dp", "seq")),
            P(("dp", "seq")),
            P(("dp", "seq")),
        ),
        check_vma=False,
    )
```

```python
import functools
import math

import jax
import jax.numpy as jnp
from jax import lax
from jax.experimental import pallas as pl
from jax.experimental.pallas import tpu as pltpu
from jax.sharding import PartitionSpec as P

HEADS = 12
PIC = 256


NEG = -1e30
EPS = 1e-05


def owners(positions, starts):
    inside = (positions[:, None] >= starts[None, :]) & (positions[:, None] < starts[None, :] + PIC)
    return jnp.max(jnp.where(inside, starts[None, :], -1), axis=1)


def visible_mask(query_pos, query_owner, key_pos, key_owner):
    later = key_pos[None, :] <= query_pos[:, None]
    shared = (key_owner[None, :] == query_owner[:, None]) & (query_owner[:, None] >= 0)
    return later | shared


def normalize(values):
    centre = values - jnp.mean(values, axis=-1, keepdims=True)
    inverse = lax.rsqrt(jnp.mean(centre * centre, axis=-1, keepdims=True) + EPS)
    return (centre * inverse, inverse)


def norm_back(upstream, normed, inverse, gain):
    scaled = upstream * gain
    return inverse * (
        scaled
        - jnp.mean(scaled, axis=-1, keepdims=True)
        - normed * jnp.mean(scaled * normed, axis=-1, keepdims=True)
    )


def matmul(left, right):
    return jnp.dot(left, right, preferred_element_type=jnp.float32)


def left_trans(left, right):
    return lax.dot_general(
        left, right, (((0,), (0,)), ((), ())), preferred_element_type=jnp.float32
    )


def right_trans(left, right):
    return lax.dot_general(
        left, right, (((1,), (1,)), ((), ())), preferred_element_type=jnp.float32
    )


def key_blocks(count):
    size = math.gcd(count, 1024)
    return (size, count // size)


def gather_forward(shards):
    return (
        lax.all_gather(shards[0], ("dp", "seq"), axis=0, tiled=True),
        lax.all_gather(shards[1], ("dp", "seq"), axis=0, tiled=True),
        lax.all_gather(shards[2], ("dp", "seq"), axis=0, tiled=True),
        lax.all_gather(shards[3], ("dp", "seq"), axis=0, tiled=True),
        lax.all_gather(shards[4], ("dp", "seq"), axis=0, tiled=True),
        lax.all_gather(shards[5], ("dp", "seq"), axis=0, tiled=True),
        lax.all_gather(shards[6], ("dp", "seq"), axis=0, tiled=True),
        lax.all_gather(shards[7], ("dp", "seq"), axis=0, tiled=True),
        lax.all_gather(shards[8], ("dp", "seq"), axis=0, tiled=True),
        lax.all_gather(shards[9], ("dp", "seq"), axis=0, tiled=True),
        lax.all_gather(shards[10], ("dp", "seq"), axis=0, tiled=True),
        lax.all_gather(shards[11], ("dp", "seq"), axis=0, tiled=True),
    )


def gather_backward(shards):
    return (
        lax.all_gather(shards[0], ("dp", "seq"), axis=0, tiled=True),
        lax.all_gather(shards[1], ("dp", "seq"), axis=0, tiled=True),
        lax.all_gather(shards[2], ("dp", "seq"), axis=0, tiled=True),
        lax.all_gather(shards[3], ("dp", "seq"), axis=0, tiled=True),
        lax.all_gather(shards[4], ("dp", "seq"), axis=0, tiled=True),
        lax.all_gather(shards[5], ("dp", "seq"), axis=0, tiled=True),
        lax.all_gather(shards[6], ("dp", "seq"), axis=0, tiled=True),
        lax.all_gather(shards[7], ("dp", "seq"), axis=0, tiled=True),
        lax.all_gather(shards[8], ("dp", "seq"), axis=0, tiled=True),
        lax.all_gather(shards[9], ("dp", "seq"), axis=0, tiled=True),
        lax.all_gather(shards[10], ("dp", "seq"), axis=0, tiled=True),
        lax.all_gather(shards[11], ("dp", "seq"), axis=0, tiled=True),
    )


def column_sum(values):
    return jnp.sum(values.astype(jnp.float32), axis=0)


def on_device(
    tokens,
    piece_starts,
    qkv_weight,
    qv_bias,
    out_weight,
    out_bias,
    norm1_gain,
    norm1_bias,
    up_weight,
    up_bias,
    down_weight,
    down_bias,
    norm2_gain,
    norm2_bias,
    grad_out,
):
    shards = (
        qkv_weight,
        qv_bias,
        out_weight,
        out_bias,
        norm1_gain,
        norm1_bias,
        up_weight,
        up_bias,
        down_weight,
        down_bias,
        norm2_gain,
        norm2_bias,
    )
    micro_count = tokens.shape[0]
    rows = tokens.shape[2]
    width = tokens.shape[3]
    head_size = width // HEADS
    scale = 1.0 / math.sqrt(head_size)
    length = rows * lax.axis_size("seq")
    query_pos = lax.axis_index("seq") * rows + jnp.arange(rows, dtype=jnp.int32)
    totals = None
    outputs = []
    input_grads = []
    for micro in range(micro_count):
        params = gather_forward(shards)
        (
            full_qkv,
            full_qvb,
            full_out,
            full_outb,
            full_g1,
            full_b1,
            full_up,
            full_upb,
            full_down,
            full_downb,
            full_g2,
            full_b2,
        ) = params
        starts = piece_starts[micro, 0]
        query_owner = owners(query_pos, starts)
        source = tokens[micro, 0]
        joined = matmul(source, full_qkv)
        queries = (joined[:, :width] + full_qvb[:width].astype(jnp.float32)).astype(jnp.bfloat16)
        keys = joined[:, width : 2 * width].astype(jnp.bfloat16)
        values = (joined[:, 2 * width :] + full_qvb[width:].astype(jnp.float32)).astype(
            jnp.bfloat16
        )
        query_heads = queries.reshape(rows, HEADS, head_size)

        def block_scores(key_block, key_pos):
            scores = (
                jnp.einsum(
                    "qhd,khd->hqk", query_heads, key_block, preferred_element_type=jnp.float32
                )
                * scale
            )
            allowed = visible_mask(query_pos, query_owner, key_pos, owners(key_pos, starts))
            return jnp.where(allowed[None], scores, NEG)

        initial = (
            jnp.full((HEADS, rows), NEG, jnp.float32),
            jnp.zeros((HEADS, rows), jnp.float32),
            jnp.zeros((HEADS, rows, head_size), jnp.float32),
        )
        key_piece = lax.all_gather(keys, "seq", axis=0, tiled=True)
        value_piece = lax.all_gather(values, "seq", axis=0, tiled=True)
        size, count = key_blocks(key_piece.shape[0])

        def one(block, carry):
            run_max, total, accum = carry
            key_block = lax.dynamic_slice_in_dim(key_piece, block * size, size, 0).reshape(
                size, HEADS, head_size
            )
            value_block = lax.dynamic_slice_in_dim(value_piece, block * size, size, 0).reshape(
                size, HEADS, head_size
            )
            key_pos = block * size + jnp.arange(size, dtype=jnp.int32)
            scores = block_scores(key_block, key_pos)
            new_max = jnp.maximum(run_max, jnp.max(scores, axis=-1))
            factor = jnp.exp(run_max - new_max)
            weights = jnp.exp(scores - new_max[:, :, None])
            total = total * factor + jnp.sum(weights, axis=-1)
            accum = accum * factor[:, :, None] + jnp.einsum(
                "hqk,khd->hqd",
                weights.astype(jnp.bfloat16),
                value_block,
                preferred_element_type=jnp.float32,
            )
            return (new_max, total, accum)

        run_max, total, accum = lax.fori_loop(0, count, one, initial)
        lse = run_max + jnp.log(total)
        exact = (accum / total[:, :, None]).transpose(1, 0, 2)
        attended = exact.reshape(rows, width).astype(jnp.bfloat16)
        resid1 = (
            source.astype(jnp.float32) + matmul(attended, full_out) + full_outb.astype(jnp.float32)
        )
        normed1, inverse1 = normalize(resid1)
        gain1 = full_g1.astype(jnp.float32)
        mixed1 = normed1 * gain1 + full_b1.astype(jnp.float32)
        inner = mixed1.astype(jnp.bfloat16)
        pre = matmul(inner, full_up) + full_upb.astype(jnp.float32)
        act = jax.nn.gelu(pre, approximate=False).astype(jnp.bfloat16)
        resid2 = mixed1 + matmul(act, full_down) + full_downb.astype(jnp.float32)
        normed2, inverse2 = normalize(resid2)
        gain2 = full_g2.astype(jnp.float32)
        outputs.append((normed2 * gain2 + full_b2.astype(jnp.float32)).astype(jnp.bfloat16))
        back = gather_backward(shards)
        back_qkv = back[0]
        back_out = back[2]
        back_up = back[6]
        back_down = back[8]
        cotan = grad_out[micro, 0].astype(jnp.float32)
        d_resid2 = norm_back(cotan, normed2, inverse2, gain2)
        grad_g2 = jnp.sum(cotan * normed2, axis=0)
        grad_b2 = jnp.sum(cotan, axis=0)
        d_branch2 = d_resid2.astype(jnp.bfloat16)
        grad_downb = column_sum(d_branch2)
        grad_down = left_trans(act, d_branch2)
        d_act = right_trans(d_branch2, back_down)
        gelu_value, gelu_back = jax.vjp(lambda value: jax.nn.gelu(value, approximate=False), pre)
        d_pre = gelu_back(d_act)[0].astype(jnp.bfloat16)
        grad_upb = column_sum(d_pre)
        grad_up = left_trans(inner, d_pre)
        d_mixed1 = d_resid2 + right_trans(d_pre, back_up)
        d_resid1 = norm_back(d_mixed1, normed1, inverse1, gain1)
        grad_g1 = jnp.sum(d_mixed1 * normed1, axis=0)
        grad_b1 = jnp.sum(d_mixed1, axis=0)
        d_branch1 = d_resid1.astype(jnp.bfloat16)
        grad_outb = column_sum(d_branch1)
        grad_out_w = left_trans(attended, d_branch1)
        d_attended = right_trans(d_branch1, back_out).astype(jnp.bfloat16)
        grad_heads = d_attended.reshape(rows, HEADS, head_size)
        delta = jnp.sum(grad_heads.astype(jnp.float32) * exact, axis=-1).T
        initial_back = (
            jnp.zeros((rows, HEADS, head_size), jnp.float32),
            jnp.zeros((length, width), jnp.float32),
            jnp.zeros((length, width), jnp.float32),
        )
        fold_key_piece = lax.all_gather(keys, "seq", axis=0, tiled=True)
        fold_value_piece = lax.all_gather(values, "seq", axis=0, tiled=True)
        fold_size, fold_count = key_blocks(fold_key_piece.shape[0])

        def fold_one(block, carry):
            query_grad, key_grads, value_grads = carry
            offset = block * fold_size
            key_block = lax.dynamic_slice_in_dim(fold_key_piece, offset, fold_size, 0).reshape(
                fold_size, HEADS, head_size
            )
            value_block = lax.dynamic_slice_in_dim(fold_value_piece, offset, fold_size, 0).reshape(
                fold_size, HEADS, head_size
            )
            key_pos = offset + jnp.arange(fold_size, dtype=jnp.int32)
            probs = jnp.exp(block_scores(key_block, key_pos) - lse[:, :, None])
            d_probs = jnp.einsum(
                "qhd,khd->hqk", grad_heads, value_block, preferred_element_type=jnp.float32
            )
            d_scores = (probs * (d_probs - delta[:, :, None])).astype(jnp.bfloat16)
            query_grad = (
                query_grad
                + jnp.einsum(
                    "hqk,khd->qhd", d_scores, key_block, preferred_element_type=jnp.float32
                )
                * scale
            )
            key_part = (
                jnp.einsum(
                    "hqk,qhd->khd", d_scores, query_heads, preferred_element_type=jnp.float32
                ).reshape(fold_size, width)
                * scale
            )
            value_part = jnp.einsum(
                "hqk,qhd->khd",
                probs.astype(jnp.bfloat16),
                grad_heads,
                preferred_element_type=jnp.float32,
            ).reshape(fold_size, width)
            key_grads = lax.dynamic_update_slice_in_dim(
                key_grads,
                lax.dynamic_slice_in_dim(key_grads, offset, fold_size, 0) + key_part,
                offset,
                0,
            )
            value_grads = lax.dynamic_update_slice_in_dim(
                value_grads,
                lax.dynamic_slice_in_dim(value_grads, offset, fold_size, 0) + value_part,
                offset,
                0,
            )
            return (query_grad, key_grads, value_grads)

        query_grad, key_grads, value_grads = lax.fori_loop(0, fold_count, fold_one, initial_back)
        key_grad, value_grad = (
            lax.psum_scatter(
                key_grads.astype(jnp.bfloat16), "seq", scatter_dimension=0, tiled=True
            ).astype(jnp.float32),
            lax.psum_scatter(
                value_grads.astype(jnp.bfloat16), "seq", scatter_dimension=0, tiled=True
            ).astype(jnp.float32),
        )
        query_share = query_grad.reshape(rows, width)
        d_queries = query_share.astype(jnp.bfloat16)
        d_keys = key_grad.astype(jnp.bfloat16)
        d_values = value_grad.astype(jnp.bfloat16)
        d_joined = jnp.concatenate([d_queries, d_keys, d_values], axis=1)
        grad_qvb = jnp.concatenate([column_sum(d_queries), column_sum(d_values)], axis=0)
        grad_qkv = left_trans(source, d_joined)
        input_grads.append(d_resid1 + right_trans(d_joined, back_qkv))
        terms = (
            grad_qkv,
            grad_qvb,
            grad_out_w,
            grad_outb,
            grad_g1,
            grad_b1,
            grad_up,
            grad_upb,
            grad_down,
            grad_downb,
            grad_g2,
            grad_b2,
        )
        if totals is None:
            totals = terms
        else:
            totals = tuple((first + second for first, second in zip(totals, terms)))
    shares = lax.psum_scatter(totals, ("dp", "seq"), scatter_dimension=0, tiled=True)
    layer_out = jnp.stack(outputs)[:, None]
    tokens_grad = jnp.stack(input_grads)[:, None]
    return (
        layer_out,
        tokens_grad,
        shares[0],
        shares[1],
        shares[2],
        shares[3],
        shares[4],
        shares[5],
        shares[6],
        shares[7],
        shares[8],
        shares[9],
        shares[10],
        shares[11],
    )


MESH = pl.DeviceIdType.MESH
ZS, CS, YS, XS = 4, 2, 2, 2
MIDS = ()
RMIDS = (0, 1)
def place():
    dp = lax.axis_index("dp"); seq = lax.axis_index("seq")
    return dp // CS, dp % CS, seq // XS, seq % XS
def dev(z, c, y, x):
    return (z * CS + c, y * XS + x)
def greet(z, c, y, x):
    barrier = pltpu.get_barrier_semaphore()
    partners = [dev((z + k) % ZS, c, y, x) for k in (1, 2, 3)]
    partners += [dev(z, 1 - c, y, x), dev(z, c, 1 - y, x), dev(z, c, y, 1 - x)]
    for p in partners:
        pl.semaphore_signal(barrier, inc=1, device_id=p, device_id_type=MESH)
    pl.semaphore_wait(barrier, len(partners))
def block(ref, r, z, c, y, x, *cols):
    at = pl.multiple_of((((z * CS + c) * YS + y) * XS + x) * r, 8)
    return ref.at[(pl.ds(at, r),) + cols]


def gather_tasks(ins, tok, outs, tout, sems):
    n = len(ins)
    (loc, zs, zr, xs, xr, ys, yr, as_, ar, bs, br, cs, cr, ts, tr, es, er, us, ur, vs, vr) = sems
    z, c, y, x = place()
    X, Y = 1 - x, 1 - y
    xn, yn, cn = dev(z, c, y, X), dev(z, c, Y, x), dev(z, 1 - c, y, x)

    def rc(src, dst, s, r, d):
        return pltpu.make_async_remote_copy(src_ref=src, dst_ref=dst, send_sem=s, recv_sem=r, device_id=d, device_id_type=MESH)

    sent, local, maybe = [], [], []

    def go(cp):
        cp.start()
        sent.append(cp)

    hh = tok.shape[-1] // 2

    def far(k):
        return (z == 0) & (k == 3) | (z == ZS - 1) & (k == 1)

    def zcast(at, s, r):
        for k in (1, 2, 3):
            cp = rc(at(z)[0], at(z)[1], s.at[k - 1], r.at[k - 1], dev((z + k) % ZS, c, y, x))
            if k == 2:
                go(cp)
                continue
            there = jnp.logical_not(far(k))
            pl.when(there)(cp.start)
            maybe.append((there, cp))

    def zpass(at, s, r):
        inner = (z == 1) | (z == 2)
        b = at(jnp.where(z == 2, 0, ZS - 1))[1]
        cp = rc(b, b, s.at[3], r.at[jnp.where(z == 2, 2, 0)], dev(jnp.where(z == 2, ZS - 1, 0), c, y, x))
        pl.when(inner)(cp.start)
        maybe.append((inner, cp))

    def own_at(w):
        return lambda q: (ins[w] if q is z else None, block(outs[w], ins[w].shape[0], q, c, y, x))

    def a_at(w):
        h = ins[w].shape[-1] // 2
        return lambda q: (block(outs[w], ins[w].shape[0], q, c, y, X, pl.ds(0, h)),) * 2

    def b_at(w):
        h = ins[w].shape[-1] // 2
        return lambda q: (block(outs[w], ins[w].shape[0], q, c, Y, x, pl.ds(h, h)),) * 2

    def begin():
        greet(z, c, y, x)
        for w in range(n + 1):
            pair = (ins[w], block(outs[w], ins[w].shape[0], z, c, y, x)) if w < n else (tok, tout.at[y, x])
            cp = pltpu.make_async_copy(*pair, loc.at[w])
            cp.start()
            local.append(cp)
        for w in range(n):
            o = block(outs[w], ins[w].shape[0], z, c, y, x)
            go(rc(ins[w], o, xs.at[w, 0], xr.at[w, 0], xn))
            go(rc(ins[w], o, ys.at[w, 0], yr.at[w, 0], yn))
            go(rc(ins[w], o, cs.at[w, 0, 0], cr.at[w, 0, 0], cn))
            cast(w)
            if w == 1:
                to = tout.at[y, x]
                go(rc(tok, to, ts.at[0], tr.at[0], xn))
                go(rc(tok, to, ts.at[1], tr.at[1], yn))

    def cast(w):
        zcast(own_at(w), zs.at[w], zr.at[w])

    def line(w, k):
        q = (z + ZS - k) % ZS
        h = ins[w].shape[-1] // 2
        r = ins[w].shape[0]
        o = block(outs[w], r, q, c, y, x)
        rc(o, o, zs.at[w, k - 1], zr.at[w, k - 1], xn).wait_recv()
        if k == 2:
            zpass(own_at(w), zs.at[w], zr.at[w])
        a, b = block(outs[w], r, q, c, y, x, pl.ds(0, h)), block(outs[w], r, q, c, y, x, pl.ds(h, h))
        go(rc(b if w in MIDS else o, b if w in MIDS else o, xs.at[w, k], xr.at[w, k], xn))
        go(rc(a if w in MIDS else o, a if w in MIDS else o, ys.at[w, k], yr.at[w, k], yn))
        go(rc(o, o, cs.at[w, k, 0], cr.at[w, k, 0], cn))

    def sides(w, k):
        if w not in MIDS:
            return
        q = (z + ZS - k) % ZS
        a, b = a_at(w)(q)[0], b_at(w)(q)[0]
        rc(a, a, us.at[w, k - 1], ur.at[w, k - 1], xn).wait_recv()
        if k == 2:
            zpass(a_at(w), us.at[w], ur.at[w])
        go(rc(a, a, as_.at[w, k], ar.at[w, k], yn))
        rc(b, b, vs.at[w, k - 1], vr.at[w, k - 1], xn).wait_recv()
        if k == 2:
            zpass(b_at(w), vs.at[w], vr.at[w])
        go(rc(b, b, bs.at[w, k], br.at[w, k], xn))

    def pairs(w, k):
        q = (z + ZS - k) % ZS
        h = ins[w].shape[-1] // 2
        r = ins[w].shape[0]
        bx, by = block(outs[w], r, q, c, y, X), block(outs[w], r, q, c, Y, x)
        b, a = block(outs[w], r, q, c, y, X, pl.ds(h, h)), block(outs[w], r, q, c, Y, x, pl.ds(0, h))
        got = (b, a) if w in MIDS else (bx, by)
        rc(got[0], got[0], xs.at[w, k], xr.at[w, k], xn).wait_recv()
        if w not in MIDS:
            near = a_at(w)(q)[0]
            go(rc(near, near, as_.at[w, k], ar.at[w, k], yn))
        go(rc(bx, bx, cs.at[w, k, 1], cr.at[w, k, 1], cn))
        rc(got[1], got[1], ys.at[w, k], yr.at[w, k], yn).wait_recv()
        if w not in MIDS:
            near = b_at(w)(q)[0]
            go(rc(near, near, bs.at[w, k], br.at[w, k], xn))
        go(rc(by, by, cs.at[w, k, 2], cr.at[w, k, 2], cn))

    def relay(w):
        bx, by = block(outs[w], ins[w].shape[0], z, c, y, X), block(outs[w], ins[w].shape[0], z, c, Y, x)
        rc(bx, bx, xs.at[w, 0], xr.at[w, 0], xn).wait_recv()
        a = a_at(w)(z)[0]
        go(rc(a, a, as_.at[w, 0], ar.at[w, 0], yn))
        if w in MIDS:
            zcast(a_at(w), us.at[w], ur.at[w])
        go(rc(bx, bx, cs.at[w, 0, 1], cr.at[w, 0, 1], cn))
        rc(by, by, ys.at[w, 0], yr.at[w, 0], yn).wait_recv()
        b = b_at(w)(z)[0]
        go(rc(b, b, bs.at[w, 0], br.at[w, 0], xn))
        if w in MIDS:
            zcast(b_at(w), vs.at[w], vr.at[w])
        go(rc(by, by, cs.at[w, 0, 2], cr.at[w, 0, 2], cn))

    def corner(w, k):
        h = ins[w].shape[-1] // 2
        q = (z + ZS - k) % ZS
        d = block(outs[w], ins[w].shape[0], q, c, Y, X)
        a = block(outs[w], ins[w].shape[0], q, c, Y, X, pl.ds(0, h))
        b = block(outs[w], ins[w].shape[0], q, c, Y, X, pl.ds(h, h))
        rc(a, a, as_.at[w, k], ar.at[w, k], yn).wait_recv()
        rc(b, b, bs.at[w, k], br.at[w, k], xn).wait_recv()
        go(rc(d, d, cs.at[w, k, 3], cr.at[w, k, 3], cn))

    def arrive(w, k):
        q = (z + ZS - k) % ZS
        for j, (yy, xx) in enumerate(((y, x), (y, X), (Y, x), (Y, X))):
            o = block(outs[w], ins[w].shape[0], q, 1 - c, yy, xx)
            rc(o, o, cs.at[w, k, j], cr.at[w, k, j], cn).wait_recv()

    def own(w):
        local[w].wait()

    def tok_relay():
        bx, by = tout.at[y, X], tout.at[Y, x]
        rc(bx, bx, ts.at[0], tr.at[0], xn).wait_recv()
        a = tout.at[y, X, :, :, pl.ds(0, hh)]
        go(rc(a, a, ts.at[2], tr.at[2], yn))
        rc(by, by, ts.at[1], tr.at[1], yn).wait_recv()
        b = tout.at[Y, x, :, :, pl.ds(hh, hh)]
        go(rc(b, b, ts.at[3], tr.at[3], xn))

    def tok_corner():
        a = tout.at[Y, X, :, :, pl.ds(0, hh)]
        b = tout.at[Y, X, :, :, pl.ds(hh, hh)]
        rc(a, a, ts.at[2], tr.at[2], yn).wait_recv()
        rc(b, b, ts.at[3], tr.at[3], xn).wait_recv()
        local[n].wait()

    def finish():
        for cp in sent:
            cp.wait_send()
        for there, cp in maybe:
            pl.when(there)(cp.wait_send)

    P = functools.partial
    tasks = {"start": [begin], "end": [finish]}
    K = range(ZS)

    ks = (2, 1, 3)

    def mid(w): return [P(f, w, k) for k in ks for f in (line, sides)]
    def meet(w): return [P(pairs, w, k) for k in ks]
    def ends(w): return [P(corner, w, k) for k in (0,) + ks]
    def last(w): return [P(arrive, w, k) for k in (0,) + ks] + [P(own, w)]

    tasks[0] = [P(relay, 0), P(relay, 1), P(relay, 2), tok_relay, P(relay, 3), P(relay, 4)] + mid(0) + mid(1) + mid(2)
    m3, m4, e3 = mid(3), mid(4), meet(3)
    tasks[1] = m3 + meet(0) + meet(1) + m4[:4] + meet(2) + ends(0) + ends(1) + m4[4:] + last(0) + last(1)
    tasks[(2, 0)] = [tok_corner] + e3[:1]
    tasks[(2, 1)] = e3[1:] + ends(2)
    tasks[(2, 2)] = meet(4)[:1] + last(2)
    tasks[(3, 0)] = meet(4)[1:2] + ends(3)[:2]
    tasks[(3, 1)] = meet(4)[2:]
    tasks[(3, 2)] = ends(3)[2:]
    e4 = ends(4)
    tasks[(3, 3)] = last(3) + e4[:1]
    for part in range(3):
        tasks[(4, part)] = [e4[part + 1]]
    tasks[4] = last(4)
    return tasks


F32, BF16 = jnp.float32, jnp.bfloat16
LANE = 128


def nt(a, b):
    return lax.dot_general(a, b, (((1,), (1,)), ((), ())), preferred_element_type=F32)


def tn(a, b):
    return lax.dot_general(a, b, (((0,), (0,)), ((), ())), preferred_element_type=F32)


def chunks(total, size, body):
    def one(i, _):
        body(pl.ds(pl.multiple_of(i * size, size), size))
        return 0

    lax.fori_loop(0, total // size, one, 0)


def spread(width, per, owners_count):
    n = lax.broadcasted_iota(jnp.int32, (1, width), 1)
    block = jnp.floor((n.astype(F32) + 0.5) / per).astype(jnp.int32)
    pick = lax.broadcasted_iota(jnp.int32, (LANE, width), 0) == n - block * per
    mine = lax.broadcasted_iota(jnp.int32, (owners_count, width), 0) == block
    return pick.astype(F32), mine.astype(F32)


def split_heads(v):
    low = lax.broadcasted_iota(jnp.int32, v.shape, 1) < v.shape[1] // 2
    return jnp.concatenate([jnp.where(low, v, 0.0), jnp.where(low, 0.0, v)], axis=0).astype(BF16)


def join_heads(v):
    half = v.shape[0] // 2
    low = lax.broadcasted_iota(jnp.int32, (half, v.shape[1]), 1) < v.shape[1] // 2
    return jnp.where(low, v[:half], v[half:])


def scatter_tasks(gs, pieces, tparts, outs, tout, hold, sems):
    n = len(pieces)
    hs, rbs, ras, rys, r2as, r2bs, rzs = (hold[i * n : (i + 1) * n] for i in range(7))
    tx, ty, t2a, t2b, base = hold[7 * n :]
    loc, ss, sr, tss, tsr, cs, cr = sems
    z, c, y, x = place()
    X, Y = 1 - x, 1 - y
    xn, yn, cn = dev(z, c, y, X), dev(z, c, Y, x), dev(z, 1 - c, y, x)

    def rc(src, dst, s, r, d):
        return pltpu.make_async_remote_copy(src_ref=src, dst_ref=dst, send_sem=s, recv_sem=r, device_id=d, device_id_type=MESH)

    sent = []

    def go(cp):
        cp.start()
        sent.append(cp)

    A = [pl.ds(0, h.shape[-1] // 2) for h in hs]
    B = [pl.ds(h.shape[-1] // 2, h.shape[-1] // 2) for h in hs]
    hh = tparts.shape[-1] // 2
    TA, TB = pl.ds(0, hh), pl.ds(hh, hh)

    spots = [(i, yy, xx) for i in range(ZS) for yy in range(YS) for xx in range(XS)]

    def load(w, k):
        i, yy, xx = spots[k]
        return pltpu.make_async_copy(block(gs[pieces[w][0]], hs[w].shape[3], i, c, yy, xx, pl.ds(*pieces[w][1:])), hs[w].at[i, yy, xx], loc.at[w, k])

    def swap(w, k):
        i, yy, xx = spots[k]
        return rc(block(gs[pieces[w][0]], hs[w].shape[3], i, 1 - c, yy, xx, pl.ds(*pieces[w][1:])), rbs[w].at[i, yy, xx], cs.at[w, k], cr.at[w, k], cn)

    def s1a(w): return rc(hs[w].at[:, :, X, :, A[w]], ras[w], ss.at[w, 1], sr.at[w, 1], xn)
    def s1b(w): return rc(hs[w].at[:, Y, :, :, B[w]], rys[w], ss.at[w, 2], sr.at[w, 2], yn)
    def s2a(w): return rc(hs[w].at[:, Y, x, :, A[w]], r2as[w], ss.at[w, 3], sr.at[w, 3], yn)
    def s2b(w): return rc(hs[w].at[:, y, X, :, B[w]], r2bs[w], ss.at[w, 4], sr.at[w, 4], xn)
    def s3(w, k): return rc(hs[w].at[(z + k) % ZS, y, x], rzs[w].at[k - 1], ss.at[w, 4 + k], sr.at[w, 4 + k], dev((z + k) % ZS, c, y, x))

    def m1a(w): return rc(hs[w].at[:, Y, :, :, A[w]], ras[w], ss.at[w, 1], sr.at[w, 1], yn)
    def m1b(w): return rc(hs[w].at[:, :, X, :, B[w]], rys[w], ss.at[w, 2], sr.at[w, 2], xn)

    def m2a(w, k):
        q = (z + k) % ZS
        return rc(hs[w].at[q, y, :, :, A[w]], r2as[w].at[k - 1], ss.at[w, 2 + k], sr.at[w, 2 + k], dev(q, c, y, x))

    def m2b(w, k):
        q = (z + k) % ZS
        return rc(hs[w].at[q, :, x, :, B[w]], r2bs[w].at[k - 1], ss.at[w, 5 + k], sr.at[w, 5 + k], dev(q, c, y, x))

    def m3a(w): return rc(hs[w].at[z, y, X, :, A[w]], rzs[w].at[0], ss.at[w, 9], sr.at[w, 9], xn)
    def m3b(w): return rc(hs[w].at[z, Y, x, :, B[w]], rzs[w].at[1], ss.at[w, 10], sr.at[w, 10], yn)

    def post(w):
        for k in range(len(spots)):
            load(w, k).start()
            go(swap(w, k))

    def plus(a, b, t):
        return (a.astype(F32) + b.astype(F32)).astype(t)

    def st0(w):
        for k in range(len(spots)):
            load(w, k).wait()
            swap(w, k).wait_recv()

        def one(i, _):
            for yy in range(YS):
                for xx in range(XS):
                    hs[w][i, yy, xx] = plus(hs[w][i, yy, xx], rbs[w][i, yy, xx], hs[w].dtype)
            return 0

        lax.fori_loop(0, ZS, one, 0)
        go(m1a(w) if w in RMIDS else s1a(w))
        go(m1b(w) if w in RMIDS else s1b(w))

    def mid1(w):
        m1a(w).wait_recv()
        m1b(w).wait_recv()

        def one(i, _):
            for j in range(2):
                hs[w][i, y, j, :, A[w]] = plus(hs[w][i, y, j, :, A[w]], ras[w][i, j], hs[w].dtype)
                hs[w][i, j, x, :, B[w]] = plus(hs[w][i, j, x, :, B[w]], rys[w][i, j], hs[w].dtype)
            return 0

        lax.fori_loop(0, ZS, one, 0)
        for k in (2, 1, 3):
            go(m2a(w, k))
            go(m2b(w, k))

    def mid2(w):
        for k in (1, 2, 3):
            m2a(w, k).wait_recv()
            m2b(w, k).wait_recv()
        for j in range(2):
            a, b = hs[w][z, y, j, :, A[w]].astype(F32), hs[w][z, j, x, :, B[w]].astype(F32)
            for k in range(ZS - 1):
                a = a + r2as[w][k, j].astype(F32)
                b = b + r2bs[w][k, j].astype(F32)
            hs[w][z, y, j, :, A[w]] = a.astype(hs[w].dtype)
            hs[w][z, j, x, :, B[w]] = b.astype(hs[w].dtype)
        go(m3a(w))
        go(m3b(w))

    def mid3(w):
        m3a(w).wait_recv()
        m3b(w).wait_recv()
        arr, col, size = pieces[w]
        for i, cols in enumerate((A[w], B[w])):
            own = hs[w][z, y, x, :, cols].astype(F32) + rzs[w][i].astype(F32)
            outs[arr][:, pl.ds(col + i * (size // 2), size // 2)] = own

    def st1(w):
        if w in RMIDS:
            return mid1(w)
        s1a(w).wait_recv()
        s1b(w).wait_recv()

        def one(i, _):
            for j in range(2):
                hs[w][i, j, x, :, A[w]] = plus(hs[w][i, j, x, :, A[w]], ras[w][i, j], hs[w].dtype)
                hs[w][i, y, j, :, B[w]] = plus(hs[w][i, y, j, :, B[w]], rys[w][i, j], hs[w].dtype)
            return 0

        lax.fori_loop(0, ZS, one, 0)
        go(s2a(w))
        go(s2b(w))

    def st2(w):
        if w in RMIDS:
            return mid2(w)
        s2a(w).wait_recv()
        s2b(w).wait_recv()

        def one(i, _):
            hs[w][i, y, x, :, A[w]] = plus(hs[w][i, y, x, :, A[w]], r2as[w][i], hs[w].dtype)
            hs[w][i, y, x, :, B[w]] = plus(hs[w][i, y, x, :, B[w]], r2bs[w][i], hs[w].dtype)
            return 0

        lax.fori_loop(0, ZS, one, 0)
        for k in (1, 2, 3):
            go(s3(w, k))

    def st3(w):
        if w in RMIDS:
            return mid3(w)
        total = hs[w][z, y, x].astype(F32)
        for k in (1, 2, 3):
            s3(w, k).wait_recv()
            total = total + rzs[w][k - 1].astype(F32)
        outs[pieces[w][0]][:, pl.ds(*pieces[w][1:])] = total

    def t0():
        go(rc(tparts.at[:, X, :, :, TA], tx, tss.at[0], tsr.at[0], xn))
        go(rc(tparts.at[Y, :, :, :, TB], ty, tss.at[1], tsr.at[1], yn))

    def t1():
        rc(tx, tx, tss.at[0], tsr.at[0], xn).wait_recv()
        rc(ty, ty, tss.at[1], tsr.at[1], yn).wait_recv()
        tparts[Y, x, :, :, TA] = plus(tparts[Y, x, :, :, TA], tx[Y], BF16)
        tparts[y, X, :, :, TB] = plus(tparts[y, X, :, :, TB], ty[X], BF16)
        go(rc(tparts.at[Y, x, :, :, TA], t2a, tss.at[2], tsr.at[2], yn))
        go(rc(tparts.at[y, X, :, :, TB], t2b, tss.at[3], tsr.at[3], xn))

    def t2():
        rc(t2a, t2a, tss.at[2], tsr.at[2], yn).wait_recv()
        rc(t2b, t2b, tss.at[3], tsr.at[3], xn).wait_recv()
        own = base[...].reshape(tout.shape) + tparts[y, x].astype(F32)
        low = jnp.concatenate([tx[y].astype(F32) + t2a[...].astype(F32), ty[x].astype(F32) + t2b[...].astype(F32)], axis=2)
        tout[...] = own + low

    def done():
        for cp in sent:
            cp.wait_send()

    return post, (st0, st1, st2, st3), (t0, t1, t2), done


def mega_body(widths, pieces, *refs):
    nv = len(widths)
    small = refs[:nv]
    (sqkv, sout, sup, sdown, tok, cot, starts) = refs[nv : nv + 7]
    k = nv + 7
    gweights = refs[k : k + 5]
    gs = refs[k + 5 : k + 10]
    lout = refs[k + 10]
    shares, tgrad = refs[k + 11 : k + 16], refs[k + 16]
    k += 17
    (svec, tout, probs, qs, kv, att, normed1, inv1, inner, act, dpre, dres2, rows, sums) = refs[k : k + 14]
    k += 14
    (wqkv, wout, wup, wdown, vecs, bias, datt, dstage) = refs[k : k + 8]
    k += 8
    np_ = len(pieces)
    hold = refs[k : k + 7 * np_ + 5]
    base = hold[-1]
    k += 7 * np_ + 5
    wsem, psem, dsem = refs[k : k + 3]
    comm = refs[k + 3 : k + 24]
    sems = refs[k + 24 :]
    gvec, gqkv, gout, gup, gdown = gweights
    mixed, gp, vscr = base, dpre, vecs
    spare = tok.shape[0] * tok.shape[1] * YS * XS
    tpart = wdown.at[pl.ds(0, spare)].reshape((YS, XS) + tok.shape)
    svec[...] = jnp.zeros(svec.shape, F32)
    for r, v in enumerate(small):
        svec[r : r + 1, 0 : widths[r]] = v[...].astype(F32)
    micro, nrow, width = tok.shape
    count = micro * nrow
    length = nrow * YS * XS
    ff = sup.shape[1]
    ins = (svec, sqkv, sout, sup, sdown)
    outs = (gvec, gqkv, gout, gup, gdown)
    tasks = gather_tasks(ins, tok, outs, tout, comm)
    run = lambda name: [f() for f in tasks[name]]
    run("start")
    lin = [(gvec, vecs), (gqkv, wqkv), (gout, wout), (gup, wup), (gdown, wdown)]

    def fetch(w):
        src, dst = lin[w]
        cp = pltpu.make_async_copy(src.reshape(dst.shape) if w == 0 else src, dst, wsem.at[w])
        cp.start()
        return cp

    seq = lax.axis_index("seq")
    qpos = seq * nrow + lax.broadcasted_iota(jnp.int32, (nrow, length), 0)
    kpos = lax.broadcasted_iota(jnp.int32, (nrow, length), 1)
    for m in range(micro):
        ok = kpos <= qpos
        for j in range(starts.shape[1]):
            s = starts[m, j]
            both = (qpos >= s) & (qpos < s + PIC) & (kpos >= s) & (kpos < s + PIC)
            ok = ok | both
        bias[m] = jnp.where(ok, 0.0, NEG)
    run(0)
    run(1)
    first = [fetch(0), fetch(1)]
    for cp in first:
        cp.wait()
    nown = vecs.shape[0]
    made = {}
    for r, n in enumerate(widths):
        if n not in made:
            made[n] = spread(n * nown, n, nown)
        pick, mine = made[n]
        got = jnp.dot(vecs[:, r, 0:LANE], pick, preferred_element_type=F32)
        rows[r : r + 1, 0 : n * nown] = jnp.sum(got * mine, axis=0, keepdims=True)
    src = tok[...].reshape(count, width)
    head_scale = 1.0 / math.sqrt(width // HEADS)

    def make_q(at):
        qs[:, at] = (jnp.dot(tok[...].reshape(count, width), wqkv[:, at], preferred_element_type=F32) + rows[0:1, at]).astype(BF16)

    chunks(width, 384, make_q)
    run((2, 0))
    for m in range(micro):
        whole = tout[:, :, m].reshape(length, width)

        def make_k(i, _):
            at = pl.ds(pl.multiple_of(width + i * 384, 128), 384)
            to = pl.ds(pl.multiple_of(i * 384, 128), 384)
            kv[m, :, to] = jnp.dot(whole, wqkv[:, at], preferred_element_type=F32).astype(BF16)
            return 0

        def make_v(i, _):
            at = pl.ds(pl.multiple_of(2 * width + i * 384, 128), 384)
            to = pl.ds(pl.multiple_of(width + i * 384, 128), 384)
            kv[m, :, to] = (jnp.dot(whole, wqkv[:, at], preferred_element_type=F32) + rows[0:1, to]).astype(BF16)
            return 0

        lax.fori_loop(0, width // 384, make_k, 0)
        lax.fori_loop(0, width // 384, make_v, 0)
        run((2, 1 + m))
    pairs = width // LANE
    for m in range(micro):
        both = jnp.concatenate([bias[m], bias[m]], axis=0)

        def attend(p, _):
            at = pl.ds(pl.multiple_of(p * LANE, LANE), LANE)
            vat = pl.ds(pl.multiple_of(width + p * LANE, LANE), LANE)
            q2 = split_heads(qs[m * nrow : (m + 1) * nrow, at].astype(F32) * head_scale)
            score = nt(q2, kv[m, :, at]) + jnp.concatenate([bias[m], bias[m]], axis=0)
            expo = jnp.exp(score - jnp.max(score, axis=1, keepdims=True))
            low = (expo * (1.0 / jnp.sum(expo, axis=1, keepdims=True))).astype(BF16)
            probs[m * pairs + p] = low
            o = join_heads(jnp.dot(low, kv[m, :, vat], preferred_element_type=F32))
            att[m * nrow : (m + 1) * nrow, at] = o.astype(BF16)
            return 0

        for part in range(2):
            lax.fori_loop(part * pairs // 2, (part + 1) * pairs // 2, attend, 0)
            run((3, 2 * m + part))
    cp = [fetch(2), fetch(3)]
    cp[0].wait()

    def project(at):
        normed1[:, at] = tok[:, :, at].reshape(count, 384).astype(F32) + jnp.dot(att[...], wout[:, at], preferred_element_type=F32) + rows[1:2, at]

    chunks(width, 384, project)
    res = normed1[...]
    centre = res - jnp.mean(res, axis=1, keepdims=True)
    inverse = lax.rsqrt(jnp.mean(centre * centre, axis=1, keepdims=True) + EPS)
    norm = centre * inverse
    normed1[...] = norm
    inv1[...] = jnp.broadcast_to(inverse, inv1.shape)
    mix = norm * rows[2:3, 0:width] + rows[3:4, 0:width]
    mixed[...] = mix
    inner[...] = mix.astype(BF16)
    cp[1].wait()

    def feed(at):
        pre = jnp.dot(inner[...], wup[:, at], preferred_element_type=F32) + rows[4:5, at]
        cdf = 0.5 * (1.0 + lax.erf(pre * math.sqrt(0.5)))
        act[:, at] = (pre * cdf).astype(BF16)
        gp[:, at] = (cdf + pre * jnp.exp(-0.5 * pre * pre) * (1.0 / math.sqrt(2.0 * math.pi))).astype(BF16)

    for part in range(3):
        lax.fori_loop(2 * part, 2 * part + 2, lambda i, _: (feed(pl.ds(pl.multiple_of(i * (ff // 6), 128), ff // 6)), 0)[1], 0)
        run((4, part))
    run(4)
    last = fetch(4)
    last.wait()

    def out2(at):
        dres2[:, at] = mixed[:, at] + jnp.dot(act[...], wdown[:, at], preferred_element_type=F32) + rows[5:6, at]

    chunks(width, 256, out2)
    res = dres2[...]
    centre = res - jnp.mean(res, axis=1, keepdims=True)
    inverse = lax.rsqrt(jnp.mean(centre * centre, axis=1, keepdims=True) + EPS)
    norm = centre * inverse
    gain = rows[6:7, 0:width]
    lout[...] = (norm * gain + rows[7:8, 0:width]).astype(BF16)
    up = cot[...].astype(F32)
    scaled = up * gain
    dres = inverse * (scaled - jnp.mean(scaled, axis=1, keepdims=True) - norm * jnp.mean(scaled * norm, axis=1, keepdims=True))
    dres2[...] = dres
    sums[0:1] = jnp.sum(dres.astype(BF16).astype(F32), axis=0, keepdims=True)
    sums[1:2] = jnp.sum(up * norm, axis=0, keepdims=True)
    sums[2:3] = jnp.sum(up, axis=0, keepdims=True)
    pairs = width // LANE
    vscr[...] = jnp.zeros(vscr.shape, F32)

    def vec(r, value):
        n = widths[r]
        pick, mine = made[n]
        vscr[:, r, 0:LANE] = lax.dot_general(value * mine, pick, (((1,), (1,)), ((), ())), precision=lax.Precision.HIGHEST, preferred_element_type=F32)

    post, (st0, st1, st2, st3), (t0, t1, t2), done = scatter_tasks(gs, pieces, tpart, shares, tgrad, hold, sems)
    D0, D1, U0, U1, OUT, KV, QQ, VEC = range(8)
    step = dstage.shape[1]

    def gdown_cols(col, size):
        cols = pl.ds(col, size)

        def send(slot, at):
            return pltpu.make_async_copy(dstage.at[slot, :, pl.ds(0, size)], gs[0].at[at, cols], dsem.at[slot])

        def one(i, _):
            slot = lax.rem(i, 2)

            @pl.when(i >= 2)
            def _():
                send(slot, pl.ds(0, step)).wait()

            at = pl.ds(pl.multiple_of(i * step, step), step)
            dstage[slot, :, 0:size] = tn(act[:, at], dres2[:, cols].astype(BF16)).astype(BF16)
            send(slot, at).start()
            return 0

        lax.fori_loop(0, ff // step, one, 0)
        send(0, pl.ds(0, step)).wait()
        send(1, pl.ds(0, step)).wait()

    gdown_cols(*pieces[D0][1:])
    post(D0)
    gdown_cols(*pieces[D1][1:])
    post(D1)

    def put(i, src, dst):
        cp = pltpu.make_async_copy(src, dst, psem.at[i])
        cp.start()
        return cp

    def feed_back(at):
        d = nt(dres2[...].astype(BF16), wdown[at, :])
        dpre[:, at] = (d * dpre[:, at].astype(F32)).astype(BF16)

    st0(D0)
    chunks(ff, 512, feed_back)
    st0(D1)

    def dmix(at):
        base[:, at] = dres2[:, at] + nt(dpre[...], wup[at, :])

    chunks(width, 256, dmix)
    st1(D0)

    def gup_part(at):
        wup[:, at] = tn(inner[...], dpre[:, at]).astype(BF16)

    chunks(ff, 512, gup_part)
    cp = put(0, wup, gs[1])
    dm, normed = base[...], normed1[...]
    vec(2, jnp.sum(dm * normed, axis=0, keepdims=True))
    vec(3, jnp.sum(dm, axis=0, keepdims=True))
    scaled = dm * rows[2:3, 0:width]
    d1 = inv1[:, 0:1] * (scaled - jnp.mean(scaled, axis=1, keepdims=True) - normed * jnp.mean(scaled * normed, axis=1, keepdims=True))
    base[...] = d1
    vec(1, jnp.sum(d1.astype(BF16).astype(F32), axis=0, keepdims=True))
    cp.wait()
    post(U0)
    post(U1)

    def back_out(at):
        datt[:, at] = nt(base[...].astype(BF16), wout[at, :]).astype(BF16)

    chunks(width, 384, back_out)

    def gout_part(at):
        wout[:, at] = tn(att[...], base[:, at].astype(BF16)).astype(BF16)

    chunks(width, 384, gout_part)
    cp = put(1, wout, gs[2])
    st1(D1)
    st0(U0)
    pumps = [[(cp.wait,), (post, OUT), (st2, D0)], [(st0, U1), (st1, U0)], [(st0, OUT), (st2, D1), (st2, U0)], [(st1, U1), (st1, OUT)]]
    for m in range(micro):
        mrow = slice(m * nrow, (m + 1) * nrow)

        def attend_back(p, _):
            at = pl.ds(pl.multiple_of(p * LANE, LANE), LANE)
            vat = pl.ds(pl.multiple_of(width + p * LANE, LANE), LANE)
            q2 = split_heads(qs[mrow, at].astype(F32) * head_scale)
            o2 = split_heads(datt[mrow, at].astype(F32))
            low = probs[m * pairs + p]
            prob = low.astype(F32)
            dprob = nt(o2, kv[m, :, vat])
            delta = jnp.sum(prob * dprob, axis=1, keepdims=True)
            ds = (prob * (dprob - delta)).astype(BF16)
            datt[mrow, at] = (join_heads(jnp.dot(ds, kv[m, :, at], preferred_element_type=F32)) * head_scale).astype(BF16)
            kv[m, :, at] = tn(ds, q2).astype(BF16)
            kv[m, :, vat] = tn(low, o2).astype(BF16)
            return 0

        for part in range(2):
            lax.fori_loop(part * pairs // 2, (part + 1) * pairs // 2, attend_back, 0)
            for f, *a in pumps[2 * m + part]:
                f(*a)
    dq, dkv = datt, kv
    for m in range(micro):

        def piece(i, _):
            at = pl.ds(pl.multiple_of(i * 256, 256), 256)
            got = nt(dkv[m], wqkv[at, width : 3 * width])
            tpart[:, :, m, :, at] = got.reshape(YS, XS, nrow, 256).astype(BF16)
            return 0

        lax.fori_loop(0, width // 256, piece, 0)
    t0()
    st2(U1)

    def gkv(i, _):
        at = pl.ds(pl.multiple_of(i * 384, 128), 384)
        to = pl.ds(pl.multiple_of(width + i * 384, 128), 384)
        total = tn(tout[:, :, 0].reshape(length, width), dkv[0, :, at])
        for m in range(1, micro):
            total = total + tn(tout[:, :, m].reshape(length, width), dkv[m, :, at])
        wqkv[:, to] = total.astype(BF16)
        return 0

    lax.fori_loop(0, 2 * width // 384, gkv, 0)
    cp = put(2, wqkv.at[:, pl.ds(width, 2 * width)], gs[3].at[:, pl.ds(width, 2 * width)])
    st2(OUT)
    cp.wait()
    post(KV)

    def dsrc(at):
        base[:, at] = base[:, at] + nt(dq[...], wqkv[at, 0:width])

    chunks(width, 256, dsrc)

    def gq(at):
        wqkv[:, at] = tn(tok[...].reshape(count, width), dq[:, at]).astype(BF16)

    chunks(width, 384, gq)
    cp = put(3, wqkv.at[:, pl.ds(0, width)], gs[3].at[:, pl.ds(0, width)])
    dv = sum(jnp.sum(dkv[m, :, width:].astype(F32), axis=0, keepdims=True) for m in range(micro))
    vec(0, jnp.concatenate([jnp.sum(dq[...].astype(F32), axis=0, keepdims=True), dv], axis=1))
    vec(4, jnp.sum(dpre[...].astype(F32), axis=0, keepdims=True))
    for r in range(3):
        vec(5 + r, sums[r : r + 1])
    cp.wait()
    post(QQ)
    st0(KV)
    cp = put(4, vscr, gs[4].reshape(vscr.shape))
    t1()
    cp.wait()
    post(VEC)
    st0(QQ)
    st0(VEC)
    for w in (D0, D1, U0, U1):
        st3(w)
    st1(KV)
    st1(QQ)
    st1(VEC)
    t2()
    st3(OUT)
    for w in (KV, QQ, VEC):
        st2(w)
    for w in (KV, QQ, VEC):
        st3(w)
    done()
    run("end")


def mega(small, shards, tok, cot, starts):
    D, V, ANY = pltpu.SemaphoreType.DMA, pltpu.VMEM, pl.ANY
    micro, nrow, width = tok.shape
    count, length, ff = micro * nrow, nrow * YS * XS, shards[2].shape[1]
    pairs = micro * width // LANE
    S = jax.ShapeDtypeStruct
    widths = tuple(v.shape[1] for v in small)
    total = ZS * CS * YS * XS
    vshape = (8, 256)
    order = (3, 2, 1, 0)
    garr = [(shards[i].shape, BF16) for i in order] + [(vshape, F32)]
    pieces = ((0, 0, width // 3), (0, width // 3, width - width // 3), (1, 0, ff // 2), (1, ff // 2, ff // 2), (2, 0, width), (3, width, 2 * width), (3, 0, width), (4, 0, 256))
    outs = [S((total * vshape[0], vshape[1]), F32)] + [S((total * s.shape[0], s.shape[1]), BF16) for s in shards]
    outs += [S((total * b[0], b[1]), t) for b, t in garr]
    res = [S((count, width), BF16)] + [S(b, F32) for b, _ in garr] + [S((micro, nrow, width), F32)]
    scr = [
        V(vshape, F32), V((YS, XS) + tok.shape, BF16), V((pairs, 2 * nrow, length), BF16), V((count, width), BF16),
        V((micro, length, 2 * width), BF16), V((count, width), BF16), V((count, width), F32), V((count, LANE), F32),
        V((count, width), BF16), V((count, ff), BF16), V((count, ff), BF16), V((count, width), F32), V((8, ff), F32), V((8, width), F32),
    ]
    scr += [V((total * s.shape[0], s.shape[1]), BF16) for s in shards]
    scr += [V((total,) + vshape, F32), V((micro, nrow, length), F32), V((count, width), BF16), V((2, 512, width), BF16)]
    both = [((garr[a][0][0], m), garr[a][1]) for a, _, m in pieces]
    scr += [V((ZS, YS, XS) + b, t) for b, t in both] * 2
    scr += [V((ZS, 2, b[0], b[1] // 2), t) for b, t in both] * 2
    scr += [V(((ZS - 1, 2) if w in RMIDS else (ZS,)) + (b[0], b[1] // 2), t) for w, (b, t) in enumerate(both)] * 2
    scr += [V((2, b[0], b[1] // 2) if w in RMIDS else (ZS - 1,) + b, t) for w, (b, t) in enumerate(both)]
    th = (micro, nrow, width // 2)
    scr += [V((2,) + th, BF16)] * 2 + [V(th, BF16)] * 2 + [V((count, width), F32)]
    n, q = 5, len(pieces)
    scr += [D((n,)), D((n,)), D((2,))]
    scr += [D((n + 1,)), D((n, 4)), D((n, 3))] + [D((n, 4))] * 8 + [D((n, 4, 4))] * 2 + [D((4,))] * 2
    scr += [D((1,))] * 2 + [D((n, 4)), D((n, 3))] * 2
    scr += [D((q, 16)), D((q, 12)), D((q, 12)), D((4,)), D((4,)), D((q, 16)), D((q, 16))]
    spec = lambda s: pl.BlockSpec(memory_space=s)
    got = pl.pallas_call(
        functools.partial(mega_body, widths, pieces),
        out_shape=outs + res,
        in_specs=[spec(V)] * (len(small) + 6) + [spec(pltpu.SMEM)],
        out_specs=[spec(ANY)] * 10 + [spec(V)] * len(res),
        scratch_shapes=scr,
        compiler_params=pltpu.CompilerParams(collective_id=0, has_side_effects=True, vmem_limit_bytes=67043328),
        name="layer",
    )(*small, *shards, tok, cot, starts)
    return got[10:]


def finish_body(widths, *refs):
    n = 6
    ins, vec, outs, small = refs[:n], refs[n], refs[n + 1 : 2 * n + 1], refs[2 * n + 1 :]
    for a, b in zip(ins, outs):
        b[...] = a[...]
    for r, o in enumerate(small):
        o[...] = vec[r : r + 1, 0 : widths[r]]


def finish(arrays, vec, widths):
    S = jax.ShapeDtypeStruct
    outs = [S(a.shape, a.dtype) for a in arrays] + [S((1, w), F32) for w in widths]
    spec = pl.BlockSpec(memory_space=pltpu.VMEM)
    return pl.pallas_call(
        functools.partial(finish_body, widths), out_shape=outs,
        in_specs=[spec] * (len(arrays) + 1), out_specs=[spec] * len(outs), name="finish",
    )(*arrays, vec)


def fits(mesh):
    return mesh.shape["dp"] == ZS * CS and mesh.shape["seq"] == YS * XS


def fast_device(
    tokens, piece_starts, qkv_weight, qv_bias, out_weight, out_bias, norm1_gain, norm1_bias,
    up_weight, up_bias, down_weight, down_bias, norm2_gain, norm2_bias, grad_out,
):
    micro, _, nrow, width = tokens.shape
    small = (qv_bias, out_bias, norm1_gain, norm1_bias, up_bias, down_bias, norm2_gain, norm2_bias)
    widths = tuple(v.shape[0] for v in small)
    got = mega(
        tuple(v.reshape(1, -1) for v in small), (qkv_weight, out_weight, up_weight, down_weight),
        tokens[:, 0], grad_out.reshape(micro * nrow, width), piece_starts[:, 0],
    )
    lout, down, up, out, qkv, vec, tgrad = got
    done = finish((lout, tgrad, qkv, out, up, down), vec, widths)
    lout, tgrad, qkv, out, up, down = done[:6]
    v = [a.reshape(-1) for a in done[6:]]
    return (
        lout.reshape(tokens.shape), tgrad.reshape(tokens.shape),
        qkv, v[0], out, v[1], v[2], v[3], up, v[4], down, v[5], v[6], v[7],
    )


def solution(mesh):
    return jax.shard_map(
        fast_device if fits(mesh) else on_device,
        mesh=mesh,
        in_specs=(
            P(None, "dp", "seq", None),
            P(None, "dp", None),
            P(("dp", "seq"), None),
            P(("dp", "seq")),
            P(("dp", "seq"), None),
            P(("dp", "seq")),
            P(("dp", "seq")),
            P(("dp", "seq")),
            P(("dp", "seq"), None),
            P(("dp", "seq")),
            P(("dp", "seq"), None),
            P(("dp", "seq")),
            P(("dp", "seq")),
            P(("dp", "seq")),
            P(None, "dp", "seq", None),
        ),
        out_specs=(
            P(None, "dp", "seq", None),
            P(None, "dp", "seq", None),
            P(("dp", "seq"), None),
            P(("dp", "seq")),
            P(("dp", "seq"), None),
            P(("dp", "seq")),
            P(("dp", "seq")),
            P(("dp", "seq")),
            P(("dp", "seq"), None),
            P(("dp", "seq")),
            P(("dp", "seq"), None),
            P(("dp", "seq")),
            P(("dp", "seq")),
            P(("dp", "seq")),
        ),
        check_vma=False,
    )
```

```python
import functools
import math

import jax
import jax.numpy as jnp
from jax import lax
from jax.experimental import pallas as pl
from jax.experimental.pallas import tpu as pltpu
from jax.sharding import PartitionSpec as P

HEADS = 12
PIC = 256


NEG = -1e30
EPS = 1e-05


def owners(positions, starts):
    inside = (positions[:, None] >= starts[None, :]) & (positions[:, None] < starts[None, :] + PIC)
    return jnp.max(jnp.where(inside, starts[None, :], -1), axis=1)


def visible_mask(query_pos, query_owner, key_pos, key_owner):
    later = key_pos[None, :] <= query_pos[:, None]
    shared = (key_owner[None, :] == query_owner[:, None]) & (query_owner[:, None] >= 0)
    return later | shared


def normalize(values):
    centre = values - jnp.mean(values, axis=-1, keepdims=True)
    inverse = lax.rsqrt(jnp.mean(centre * centre, axis=-1, keepdims=True) + EPS)
    return (centre * inverse, inverse)


def norm_back(upstream, normed, inverse, gain):
    scaled = upstream * gain
    return inverse * (
        scaled
        - jnp.mean(scaled, axis=-1, keepdims=True)
        - normed * jnp.mean(scaled * normed, axis=-1, keepdims=True)
    )


def matmul(left, right):
    return jnp.dot(left, right, preferred_element_type=jnp.float32)


def left_trans(left, right):
    return lax.dot_general(
        left, right, (((0,), (0,)), ((), ())), preferred_element_type=jnp.float32
    )


def right_trans(left, right):
    return lax.dot_general(
        left, right, (((1,), (1,)), ((), ())), preferred_element_type=jnp.float32
    )


def key_blocks(count):
    size = math.gcd(count, 1024)
    return (size, count // size)


def gather_forward(shards):
    return (
        lax.all_gather(shards[0], ("dp", "seq"), axis=0, tiled=True),
        lax.all_gather(shards[1], ("dp", "seq"), axis=0, tiled=True),
        lax.all_gather(shards[2], ("dp", "seq"), axis=0, tiled=True),
        lax.all_gather(shards[3], ("dp", "seq"), axis=0, tiled=True),
        lax.all_gather(shards[4], ("dp", "seq"), axis=0, tiled=True),
        lax.all_gather(shards[5], ("dp", "seq"), axis=0, tiled=True),
        lax.all_gather(shards[6], ("dp", "seq"), axis=0, tiled=True),
        lax.all_gather(shards[7], ("dp", "seq"), axis=0, tiled=True),
        lax.all_gather(shards[8], ("dp", "seq"), axis=0, tiled=True),
        lax.all_gather(shards[9], ("dp", "seq"), axis=0, tiled=True),
        lax.all_gather(shards[10], ("dp", "seq"), axis=0, tiled=True),
        lax.all_gather(shards[11], ("dp", "seq"), axis=0, tiled=True),
    )


def gather_backward(shards):
    return (
        lax.all_gather(shards[0], ("dp", "seq"), axis=0, tiled=True),
        lax.all_gather(shards[1], ("dp", "seq"), axis=0, tiled=True),
        lax.all_gather(shards[2], ("dp", "seq"), axis=0, tiled=True),
        lax.all_gather(shards[3], ("dp", "seq"), axis=0, tiled=True),
        lax.all_gather(shards[4], ("dp", "seq"), axis=0, tiled=True),
        lax.all_gather(shards[5], ("dp", "seq"), axis=0, tiled=True),
        lax.all_gather(shards[6], ("dp", "seq"), axis=0, tiled=True),
        lax.all_gather(shards[7], ("dp", "seq"), axis=0, tiled=True),
        lax.all_gather(shards[8], ("dp", "seq"), axis=0, tiled=True),
        lax.all_gather(shards[9], ("dp", "seq"), axis=0, tiled=True),
        lax.all_gather(shards[10], ("dp", "seq"), axis=0, tiled=True),
        lax.all_gather(shards[11], ("dp", "seq"), axis=0, tiled=True),
    )


def column_sum(values):
    return jnp.sum(values.astype(jnp.float32), axis=0)


def on_device(
    tokens,
    piece_starts,
    qkv_weight,
    qv_bias,
    out_weight,
    out_bias,
    norm1_gain,
    norm1_bias,
    up_weight,
    up_bias,
    down_weight,
    down_bias,
    norm2_gain,
    norm2_bias,
    grad_out,
):
    shards = (
        qkv_weight,
        qv_bias,
        out_weight,
        out_bias,
        norm1_gain,
        norm1_bias,
        up_weight,
        up_bias,
        down_weight,
        down_bias,
        norm2_gain,
        norm2_bias,
    )
    micro_count = tokens.shape[0]
    rows = tokens.shape[2]
    width = tokens.shape[3]
    head_size = width // HEADS
    scale = 1.0 / math.sqrt(head_size)
    length = rows * lax.axis_size("seq")
    query_pos = lax.axis_index("seq") * rows + jnp.arange(rows, dtype=jnp.int32)
    totals = None
    outputs = []
    input_grads = []
    for micro in range(micro_count):
        params = gather_forward(shards)
        (
            full_qkv,
            full_qvb,
            full_out,
            full_outb,
            full_g1,
            full_b1,
            full_up,
            full_upb,
            full_down,
            full_downb,
            full_g2,
            full_b2,
        ) = params
        starts = piece_starts[micro, 0]
        query_owner = owners(query_pos, starts)
        source = tokens[micro, 0]
        joined = matmul(source, full_qkv)
        queries = (joined[:, :width] + full_qvb[:width].astype(jnp.float32)).astype(jnp.bfloat16)
        keys = joined[:, width : 2 * width].astype(jnp.bfloat16)
        values = (joined[:, 2 * width :] + full_qvb[width:].astype(jnp.float32)).astype(
            jnp.bfloat16
        )
        query_heads = queries.reshape(rows, HEADS, head_size)

        def block_scores(key_block, key_pos):
            scores = (
                jnp.einsum(
                    "qhd,khd->hqk", query_heads, key_block, preferred_element_type=jnp.float32
                )
                * scale
            )
            allowed = visible_mask(query_pos, query_owner, key_pos, owners(key_pos, starts))
            return jnp.where(allowed[None], scores, NEG)

        initial = (
            jnp.full((HEADS, rows), NEG, jnp.float32),
            jnp.zeros((HEADS, rows), jnp.float32),
            jnp.zeros((HEADS, rows, head_size), jnp.float32),
        )
        key_piece = lax.all_gather(keys, "seq", axis=0, tiled=True)
        value_piece = lax.all_gather(values, "seq", axis=0, tiled=True)
        size, count = key_blocks(key_piece.shape[0])

        def one(block, carry):
            run_max, total, accum = carry
            key_block = lax.dynamic_slice_in_dim(key_piece, block * size, size, 0).reshape(
                size, HEADS, head_size
            )
            value_block = lax.dynamic_slice_in_dim(value_piece, block * size, size, 0).reshape(
                size, HEADS, head_size
            )
            key_pos = block * size + jnp.arange(size, dtype=jnp.int32)
            scores = block_scores(key_block, key_pos)
            new_max = jnp.maximum(run_max, jnp.max(scores, axis=-1))
            factor = jnp.exp(run_max - new_max)
            weights = jnp.exp(scores - new_max[:, :, None])
            total = total * factor + jnp.sum(weights, axis=-1)
            accum = accum * factor[:, :, None] + jnp.einsum(
                "hqk,khd->hqd",
                weights.astype(jnp.bfloat16),
                value_block,
                preferred_element_type=jnp.float32,
            )
            return (new_max, total, accum)

        run_max, total, accum = lax.fori_loop(0, count, one, initial)
        lse = run_max + jnp.log(total)
        exact = (accum / total[:, :, None]).transpose(1, 0, 2)
        attended = exact.reshape(rows, width).astype(jnp.bfloat16)
        resid1 = (
            source.astype(jnp.float32) + matmul(attended, full_out) + full_outb.astype(jnp.float32)
        )
        normed1, inverse1 = normalize(resid1)
        gain1 = full_g1.astype(jnp.float32)
        mixed1 = normed1 * gain1 + full_b1.astype(jnp.float32)
        inner = mixed1.astype(jnp.bfloat16)
        pre = matmul(inner, full_up) + full_upb.astype(jnp.float32)
        act = jax.nn.gelu(pre, approximate=False).astype(jnp.bfloat16)
        resid2 = mixed1 + matmul(act, full_down) + full_downb.astype(jnp.float32)
        normed2, inverse2 = normalize(resid2)
        gain2 = full_g2.astype(jnp.float32)
        outputs.append((normed2 * gain2 + full_b2.astype(jnp.float32)).astype(jnp.bfloat16))
        back = gather_backward(shards)
        back_qkv = back[0]
        back_out = back[2]
        back_up = back[6]
        back_down = back[8]
        cotan = grad_out[micro, 0].astype(jnp.float32)
        d_resid2 = norm_back(cotan, normed2, inverse2, gain2)
        grad_g2 = jnp.sum(cotan * normed2, axis=0)
        grad_b2 = jnp.sum(cotan, axis=0)
        d_branch2 = d_resid2.astype(jnp.bfloat16)
        grad_downb = column_sum(d_branch2)
        grad_down = left_trans(act, d_branch2)
        d_act = right_trans(d_branch2, back_down)
        gelu_value, gelu_back = jax.vjp(lambda value: jax.nn.gelu(value, approximate=False), pre)
        d_pre = gelu_back(d_act)[0].astype(jnp.bfloat16)
        grad_upb = column_sum(d_pre)
        grad_up = left_trans(inner, d_pre)
        d_mixed1 = d_resid2 + right_trans(d_pre, back_up)
        d_resid1 = norm_back(d_mixed1, normed1, inverse1, gain1)
        grad_g1 = jnp.sum(d_mixed1 * normed1, axis=0)
        grad_b1 = jnp.sum(d_mixed1, axis=0)
        d_branch1 = d_resid1.astype(jnp.bfloat16)
        grad_outb = column_sum(d_branch1)
        grad_out_w = left_trans(attended, d_branch1)
        d_attended = right_trans(d_branch1, back_out).astype(jnp.bfloat16)
        grad_heads = d_attended.reshape(rows, HEADS, head_size)
        delta = jnp.sum(grad_heads.astype(jnp.float32) * exact, axis=-1).T
        initial_back = (
            jnp.zeros((rows, HEADS, head_size), jnp.float32),
            jnp.zeros((length, width), jnp.float32),
            jnp.zeros((length, width), jnp.float32),
        )
        fold_key_piece = lax.all_gather(keys, "seq", axis=0, tiled=True)
        fold_value_piece = lax.all_gather(values, "seq", axis=0, tiled=True)
        fold_size, fold_count = key_blocks(fold_key_piece.shape[0])

        def fold_one(block, carry):
            query_grad, key_grads, value_grads = carry
            offset = block * fold_size
            key_block = lax.dynamic_slice_in_dim(fold_key_piece, offset, fold_size, 0).reshape(
                fold_size, HEADS, head_size
            )
            value_block = lax.dynamic_slice_in_dim(fold_value_piece, offset, fold_size, 0).reshape(
                fold_size, HEADS, head_size
            )
            key_pos = offset + jnp.arange(fold_size, dtype=jnp.int32)
            probs = jnp.exp(block_scores(key_block, key_pos) - lse[:, :, None])
            d_probs = jnp.einsum(
                "qhd,khd->hqk", grad_heads, value_block, preferred_element_type=jnp.float32
            )
            d_scores = (probs * (d_probs - delta[:, :, None])).astype(jnp.bfloat16)
            query_grad = (
                query_grad
                + jnp.einsum(
                    "hqk,khd->qhd", d_scores, key_block, preferred_element_type=jnp.float32
                )
                * scale
            )
            key_part = (
                jnp.einsum(
                    "hqk,qhd->khd", d_scores, query_heads, preferred_element_type=jnp.float32
                ).reshape(fold_size, width)
                * scale
            )
            value_part = jnp.einsum(
                "hqk,qhd->khd",
                probs.astype(jnp.bfloat16),
                grad_heads,
                preferred_element_type=jnp.float32,
            ).reshape(fold_size, width)
            key_grads = lax.dynamic_update_slice_in_dim(
                key_grads,
                lax.dynamic_slice_in_dim(key_grads, offset, fold_size, 0) + key_part,
                offset,
                0,
            )
            value_grads = lax.dynamic_update_slice_in_dim(
                value_grads,
                lax.dynamic_slice_in_dim(value_grads, offset, fold_size, 0) + value_part,
                offset,
                0,
            )
            return (query_grad, key_grads, value_grads)

        query_grad, key_grads, value_grads = lax.fori_loop(0, fold_count, fold_one, initial_back)
        key_grad, value_grad = (
            lax.psum_scatter(
                key_grads.astype(jnp.bfloat16), "seq", scatter_dimension=0, tiled=True
            ).astype(jnp.float32),
            lax.psum_scatter(
                value_grads.astype(jnp.bfloat16), "seq", scatter_dimension=0, tiled=True
            ).astype(jnp.float32),
        )
        query_share = query_grad.reshape(rows, width)
        d_queries = query_share.astype(jnp.bfloat16)
        d_keys = key_grad.astype(jnp.bfloat16)
        d_values = value_grad.astype(jnp.bfloat16)
        d_joined = jnp.concatenate([d_queries, d_keys, d_values], axis=1)
        grad_qvb = jnp.concatenate([column_sum(d_queries), column_sum(d_values)], axis=0)
        grad_qkv = left_trans(source, d_joined)
        input_grads.append(d_resid1 + right_trans(d_joined, back_qkv))
        terms = (
            grad_qkv,
            grad_qvb,
            grad_out_w,
            grad_outb,
            grad_g1,
            grad_b1,
            grad_up,
            grad_upb,
            grad_down,
            grad_downb,
            grad_g2,
            grad_b2,
        )
        if totals is None:
            totals = terms
        else:
            totals = tuple((first + second for first, second in zip(totals, terms)))
    shares = lax.psum_scatter(totals, ("dp", "seq"), scatter_dimension=0, tiled=True)
    layer_out = jnp.stack(outputs)[:, None]
    tokens_grad = jnp.stack(input_grads)[:, None]
    return (
        layer_out,
        tokens_grad,
        shares[0],
        shares[1],
        shares[2],
        shares[3],
        shares[4],
        shares[5],
        shares[6],
        shares[7],
        shares[8],
        shares[9],
        shares[10],
        shares[11],
    )


MESH = pl.DeviceIdType.MESH
ZS, CS, YS, XS = 4, 2, 2, 2
MIDS = (2,)
RMIDS = (0, 1, 2)
def place():
    dp = lax.axis_index("dp"); seq = lax.axis_index("seq")
    return dp // CS, dp % CS, seq // XS, seq % XS
def dev(z, c, y, x):
    return (z * CS + c, y * XS + x)
def greet(z, c, y, x):
    barrier = pltpu.get_barrier_semaphore()
    partners = [dev((z + k) % ZS, c, y, x) for k in (1, 2, 3)]
    partners += [dev(z, 1 - c, y, x), dev(z, c, 1 - y, x), dev(z, c, y, 1 - x)]
    for p in partners:
        pl.semaphore_signal(barrier, inc=1, device_id=p, device_id_type=MESH)
    pl.semaphore_wait(barrier, len(partners))
def block(ref, r, z, c, y, x, *cols):
    at = pl.multiple_of((((z * CS + c) * YS + y) * XS + x) * r, 8)
    return ref.at[(pl.ds(at, r),) + cols]


def gather_tasks(ins, tok, outs, tout, sems):
    n = len(ins)
    (loc, zs, zr, xs, xr, ys, yr, as_, ar, bs, br, cs, cr, ts, tr, es, er, us, ur, vs, vr) = sems
    z, c, y, x = place()
    X, Y = 1 - x, 1 - y
    xn, yn, cn = dev(z, c, y, X), dev(z, c, Y, x), dev(z, 1 - c, y, x)

    def rc(src, dst, s, r, d):
        return pltpu.make_async_remote_copy(src_ref=src, dst_ref=dst, send_sem=s, recv_sem=r, device_id=d, device_id_type=MESH)

    sent, local, maybe = [], [], []

    def go(cp):
        cp.start()
        sent.append(cp)

    hh = tok.shape[-1] // 2

    def far(k):
        return (z == 0) & (k == 3) | (z == ZS - 1) & (k == 1)

    def zcast(at, s, r):
        for k in (1, 2, 3):
            cp = rc(at(z)[0], at(z)[1], s.at[k - 1], r.at[k - 1], dev((z + k) % ZS, c, y, x))
            if k == 2:
                go(cp)
                continue
            there = jnp.logical_not(far(k))
            pl.when(there)(cp.start)
            maybe.append((there, cp))

    def zpass(at, s, r):
        inner = (z == 1) | (z == 2)
        b = at(jnp.where(z == 2, 0, ZS - 1))[1]
        cp = rc(b, b, s.at[3], r.at[jnp.where(z == 2, 2, 0)], dev(jnp.where(z == 2, ZS - 1, 0), c, y, x))
        pl.when(inner)(cp.start)
        maybe.append((inner, cp))

    def own_at(w):
        return lambda q: (ins[w] if q is z else None, block(outs[w], ins[w].shape[0], q, c, y, x))

    def a_at(w):
        h = ins[w].shape[-1] // 2
        return lambda q: (block(outs[w], ins[w].shape[0], q, c, y, X, pl.ds(0, h)),) * 2

    def b_at(w):
        h = ins[w].shape[-1] // 2
        return lambda q: (block(outs[w], ins[w].shape[0], q, c, Y, x, pl.ds(h, h)),) * 2

    def begin():
        greet(z, c, y, x)
        for w in range(n + 1):
            pair = (ins[w], block(outs[w], ins[w].shape[0], z, c, y, x)) if w < n else (tok, tout.at[y, x])
            cp = pltpu.make_async_copy(*pair, loc.at[w])
            cp.start()
            local.append(cp)
        for w in range(n):
            o = block(outs[w], ins[w].shape[0], z, c, y, x)
            go(rc(ins[w], o, xs.at[w, 0], xr.at[w, 0], xn))
            go(rc(ins[w], o, ys.at[w, 0], yr.at[w, 0], yn))
            go(rc(ins[w], o, cs.at[w, 0, 0], cr.at[w, 0, 0], cn))
            cast(w)
            if w == 1:
                to = tout.at[y, x]
                go(rc(tok, to, ts.at[0], tr.at[0], xn))
                go(rc(tok, to, ts.at[1], tr.at[1], yn))

    def cast(w):
        zcast(own_at(w), zs.at[w], zr.at[w])

    def line(w, k):
        q = (z + ZS - k) % ZS
        h = ins[w].shape[-1] // 2
        r = ins[w].shape[0]
        o = block(outs[w], r, q, c, y, x)
        rc(o, o, zs.at[w, k - 1], zr.at[w, k - 1], xn).wait_recv()
        if k == 2:
            zpass(own_at(w), zs.at[w], zr.at[w])
        a, b = block(outs[w], r, q, c, y, x, pl.ds(0, h)), block(outs[w], r, q, c, y, x, pl.ds(h, h))
        go(rc(b if w in MIDS else o, b if w in MIDS else o, xs.at[w, k], xr.at[w, k], xn))
        go(rc(a if w in MIDS else o, a if w in MIDS else o, ys.at[w, k], yr.at[w, k], yn))
        go(rc(o, o, cs.at[w, k, 0], cr.at[w, k, 0], cn))

    def sides(w, k):
        if w not in MIDS:
            return
        q = (z + ZS - k) % ZS
        a, b = a_at(w)(q)[0], b_at(w)(q)[0]
        rc(a, a, us.at[w, k - 1], ur.at[w, k - 1], xn).wait_recv()
        if k == 2:
            zpass(a_at(w), us.at[w], ur.at[w])
        go(rc(a, a, as_.at[w, k], ar.at[w, k], yn))
        rc(b, b, vs.at[w, k - 1], vr.at[w, k - 1], xn).wait_recv()
        if k == 2:
            zpass(b_at(w), vs.at[w], vr.at[w])
        go(rc(b, b, bs.at[w, k], br.at[w, k], xn))

    def pairs(w, k):
        q = (z + ZS - k) % ZS
        h = ins[w].shape[-1] // 2
        r = ins[w].shape[0]
        bx, by = block(outs[w], r, q, c, y, X), block(outs[w], r, q, c, Y, x)
        b, a = block(outs[w], r, q, c, y, X, pl.ds(h, h)), block(outs[w], r, q, c, Y, x, pl.ds(0, h))
        got = (b, a) if w in MIDS else (bx, by)
        rc(got[0], got[0], xs.at[w, k], xr.at[w, k], xn).wait_recv()
        if w not in MIDS:
            near = a_at(w)(q)[0]
            go(rc(near, near, as_.at[w, k], ar.at[w, k], yn))
        go(rc(bx, bx, cs.at[w, k, 1], cr.at[w, k, 1], cn))
        rc(got[1], got[1], ys.at[w, k], yr.at[w, k], yn).wait_recv()
        if w not in MIDS:
            near = b_at(w)(q)[0]
            go(rc(near, near, bs.at[w, k], br.at[w, k], xn))
        go(rc(by, by, cs.at[w, k, 2], cr.at[w, k, 2], cn))

    def relay(w):
        bx, by = block(outs[w], ins[w].shape[0], z, c, y, X), block(outs[w], ins[w].shape[0], z, c, Y, x)
        rc(bx, bx, xs.at[w, 0], xr.at[w, 0], xn).wait_recv()
        a = a_at(w)(z)[0]
        go(rc(a, a, as_.at[w, 0], ar.at[w, 0], yn))
        if w in MIDS:
            zcast(a_at(w), us.at[w], ur.at[w])
        go(rc(bx, bx, cs.at[w, 0, 1], cr.at[w, 0, 1], cn))
        rc(by, by, ys.at[w, 0], yr.at[w, 0], yn).wait_recv()
        b = b_at(w)(z)[0]
        go(rc(b, b, bs.at[w, 0], br.at[w, 0], xn))
        if w in MIDS:
            zcast(b_at(w), vs.at[w], vr.at[w])
        go(rc(by, by, cs.at[w, 0, 2], cr.at[w, 0, 2], cn))

    def corner(w, k):
        h = ins[w].shape[-1] // 2
        q = (z + ZS - k) % ZS
        d = block(outs[w], ins[w].shape[0], q, c, Y, X)
        a = block(outs[w], ins[w].shape[0], q, c, Y, X, pl.ds(0, h))
        b = block(outs[w], ins[w].shape[0], q, c, Y, X, pl.ds(h, h))
        rc(a, a, as_.at[w, k], ar.at[w, k], yn).wait_recv()
        rc(b, b, bs.at[w, k], br.at[w, k], xn).wait_recv()
        go(rc(d, d, cs.at[w, k, 3], cr.at[w, k, 3], cn))

    def arrive(w, k):
        q = (z + ZS - k) % ZS
        for j, (yy, xx) in enumerate(((y, x), (y, X), (Y, x), (Y, X))):
            o = block(outs[w], ins[w].shape[0], q, 1 - c, yy, xx)
            rc(o, o, cs.at[w, k, j], cr.at[w, k, j], cn).wait_recv()

    def own(w):
        local[w].wait()

    def tok_relay():
        bx, by = tout.at[y, X], tout.at[Y, x]
        rc(bx, bx, ts.at[0], tr.at[0], xn).wait_recv()
        a = tout.at[y, X, :, :, pl.ds(0, hh)]
        go(rc(a, a, ts.at[2], tr.at[2], yn))
        rc(by, by, ts.at[1], tr.at[1], yn).wait_recv()
        b = tout.at[Y, x, :, :, pl.ds(hh, hh)]
        go(rc(b, b, ts.at[3], tr.at[3], xn))

    def tok_corner():
        a = tout.at[Y, X, :, :, pl.ds(0, hh)]
        b = tout.at[Y, X, :, :, pl.ds(hh, hh)]
        rc(a, a, ts.at[2], tr.at[2], yn).wait_recv()
        rc(b, b, ts.at[3], tr.at[3], xn).wait_recv()
        local[n].wait()

    def finish():
        for cp in sent:
            cp.wait_send()
        for there, cp in maybe:
            pl.when(there)(cp.wait_send)

    P = functools.partial
    tasks = {"start": [begin], "end": [finish]}
    K = range(ZS)

    ks = (2, 1, 3)

    def mid(w): return [P(f, w, k) for k in ks for f in (line, sides)]
    def meet(w): return [P(pairs, w, k) for k in ks]
    def ends(w): return [P(corner, w, k) for k in (0,) + ks]
    def last(w): return [P(arrive, w, k) for k in (0,) + ks] + [P(own, w)]

    tasks[0] = [P(relay, 0), P(relay, 1), P(relay, 2), tok_relay, P(relay, 3), P(relay, 4)] + mid(0) + mid(1) + mid(2)
    m3, m4, e3 = mid(3), mid(4), meet(3)
    tasks[1] = m3 + meet(0) + meet(1) + m4[:4] + meet(2) + ends(0) + ends(1) + m4[4:] + last(0) + last(1)
    tasks[(2, 0)] = [tok_corner] + e3[:1]
    tasks[(2, 1)] = e3[1:] + ends(2)
    tasks[(2, 2)] = meet(4)[:1] + last(2)
    tasks[(3, 0)] = meet(4)[1:2] + ends(3)[:2]
    tasks[(3, 1)] = meet(4)[2:]
    tasks[(3, 2)] = ends(3)[2:]
    e4 = ends(4)
    tasks[(3, 3)] = last(3) + e4[:1]
    for part in range(3):
        tasks[(4, part)] = [e4[part + 1]]
    tasks[4] = last(4)
    return tasks


F32, BF16 = jnp.float32, jnp.bfloat16
LANE = 128


def nt(a, b):
    return lax.dot_general(a, b, (((1,), (1,)), ((), ())), preferred_element_type=F32)


def tn(a, b):
    return lax.dot_general(a, b, (((0,), (0,)), ((), ())), preferred_element_type=F32)


def chunks(total, size, body):
    def one(i, _):
        body(pl.ds(pl.multiple_of(i * size, size), size))
        return 0

    lax.fori_loop(0, total // size, one, 0)


def spread(width, per, owners_count):
    n = lax.broadcasted_iota(jnp.int32, (1, width), 1)
    block = jnp.floor((n.astype(F32) + 0.5) / per).astype(jnp.int32)
    pick = lax.broadcasted_iota(jnp.int32, (LANE, width), 0) == n - block * per
    mine = lax.broadcasted_iota(jnp.int32, (owners_count, width), 0) == block
    return pick.astype(F32), mine.astype(F32)


def split_heads(v):
    low = lax.broadcasted_iota(jnp.int32, v.shape, 1) < v.shape[1] // 2
    return jnp.concatenate([jnp.where(low, v, 0.0), jnp.where(low, 0.0, v)], axis=0).astype(BF16)


def join_heads(v):
    half = v.shape[0] // 2
    low = lax.broadcasted_iota(jnp.int32, (half, v.shape[1]), 1) < v.shape[1] // 2
    return jnp.where(low, v[:half], v[half:])


def scatter_tasks(gs, pieces, tparts, outs, tout, hold, sems):
    n = len(pieces)
    hs, rbs, ras, rys, r2as, r2bs, rzs = (hold[i * n : (i + 1) * n] for i in range(7))
    tx, ty, t2a, t2b, base = hold[7 * n :]
    loc, ss, sr, tss, tsr, cs, cr = sems
    z, c, y, x = place()
    X, Y = 1 - x, 1 - y
    xn, yn, cn = dev(z, c, y, X), dev(z, c, Y, x), dev(z, 1 - c, y, x)

    def rc(src, dst, s, r, d):
        return pltpu.make_async_remote_copy(src_ref=src, dst_ref=dst, send_sem=s, recv_sem=r, device_id=d, device_id_type=MESH)

    sent = []

    def go(cp):
        cp.start()
        sent.append(cp)

    A = [pl.ds(0, h.shape[-1] // 2) for h in hs]
    B = [pl.ds(h.shape[-1] // 2, h.shape[-1] // 2) for h in hs]
    hh = tparts.shape[-1] // 2
    TA, TB = pl.ds(0, hh), pl.ds(hh, hh)

    spots = [(i, yy, xx) for i in range(ZS) for yy in range(YS) for xx in range(XS)]

    def load(w, k):
        i, yy, xx = spots[k]
        return pltpu.make_async_copy(block(gs[pieces[w][0]], hs[w].shape[3], i, c, yy, xx, pl.ds(*pieces[w][1:])), hs[w].at[i, yy, xx], loc.at[w, k])

    def swap(w, k):
        i, yy, xx = spots[k]
        return rc(block(gs[pieces[w][0]], hs[w].shape[3], i, 1 - c, yy, xx, pl.ds(*pieces[w][1:])), rbs[w].at[i, yy, xx], cs.at[w, k], cr.at[w, k], cn)

    def s1a(w): return rc(hs[w].at[:, :, X, :, A[w]], ras[w], ss.at[w, 1], sr.at[w, 1], xn)
    def s1b(w): return rc(hs[w].at[:, Y, :, :, B[w]], rys[w], ss.at[w, 2], sr.at[w, 2], yn)
    def s2a(w): return rc(hs[w].at[:, Y, x, :, A[w]], r2as[w], ss.at[w, 3], sr.at[w, 3], yn)
    def s2b(w): return rc(hs[w].at[:, y, X, :, B[w]], r2bs[w], ss.at[w, 4], sr.at[w, 4], xn)
    def s3(w, k): return rc(hs[w].at[(z + k) % ZS, y, x], rzs[w].at[k - 1], ss.at[w, 4 + k], sr.at[w, 4 + k], dev((z + k) % ZS, c, y, x))

    def m1a(w): return rc(hs[w].at[:, Y, :, :, A[w]], ras[w], ss.at[w, 1], sr.at[w, 1], yn)
    def m1b(w): return rc(hs[w].at[:, :, X, :, B[w]], rys[w], ss.at[w, 2], sr.at[w, 2], xn)

    def m2a(w, k):
        q = (z + k) % ZS
        return rc(hs[w].at[q, y, :, :, A[w]], r2as[w].at[k - 1], ss.at[w, 2 + k], sr.at[w, 2 + k], dev(q, c, y, x))

    def m2b(w, k):
        q = (z + k) % ZS
        return rc(hs[w].at[q, :, x, :, B[w]], r2bs[w].at[k - 1], ss.at[w, 5 + k], sr.at[w, 5 + k], dev(q, c, y, x))

    def m3a(w): return rc(hs[w].at[z, y, X, :, A[w]], rzs[w].at[0], ss.at[w, 9], sr.at[w, 9], xn)
    def m3b(w): return rc(hs[w].at[z, Y, x, :, B[w]], rzs[w].at[1], ss.at[w, 10], sr.at[w, 10], yn)

    def post(w):
        for k in range(len(spots)):
            load(w, k).start()
            go(swap(w, k))

    def plus(a, b, t):
        return (a.astype(F32) + b.astype(F32)).astype(t)

    def st0(w):
        for k in range(len(spots)):
            load(w, k).wait()
            swap(w, k).wait_recv()

        def one(i, _):
            for yy in range(YS):
                for xx in range(XS):
                    hs[w][i, yy, xx] = plus(hs[w][i, yy, xx], rbs[w][i, yy, xx], hs[w].dtype)
            return 0

        lax.fori_loop(0, ZS, one, 0)
        go(m1a(w) if w in RMIDS else s1a(w))
        go(m1b(w) if w in RMIDS else s1b(w))

    def mid1(w):
        m1a(w).wait_recv()
        m1b(w).wait_recv()

        def one(i, _):
            for j in range(2):
                hs[w][i, y, j, :, A[w]] = plus(hs[w][i, y, j, :, A[w]], ras[w][i, j], hs[w].dtype)
                hs[w][i, j, x, :, B[w]] = plus(hs[w][i, j, x, :, B[w]], rys[w][i, j], hs[w].dtype)
            return 0

        lax.fori_loop(0, ZS, one, 0)
        for k in (2, 1, 3):
            go(m2a(w, k))
            go(m2b(w, k))

    def mid2(w):
        for k in (1, 2, 3):
            m2a(w, k).wait_recv()
            m2b(w, k).wait_recv()
        for j in range(2):
            a, b = hs[w][z, y, j, :, A[w]].astype(F32), hs[w][z, j, x, :, B[w]].astype(F32)
            for k in range(ZS - 1):
                a = a + r2as[w][k, j].astype(F32)
                b = b + r2bs[w][k, j].astype(F32)
            hs[w][z, y, j, :, A[w]] = a.astype(hs[w].dtype)
            hs[w][z, j, x, :, B[w]] = b.astype(hs[w].dtype)
        go(m3a(w))
        go(m3b(w))

    def mid3(w):
        m3a(w).wait_recv()
        m3b(w).wait_recv()
        arr, col, size = pieces[w]
        for i, cols in enumerate((A[w], B[w])):
            own = hs[w][z, y, x, :, cols].astype(F32) + rzs[w][i].astype(F32)
            outs[arr][:, pl.ds(col + i * (size // 2), size // 2)] = own

    def st1(w):
        if w in RMIDS:
            return mid1(w)
        s1a(w).wait_recv()
        s1b(w).wait_recv()

        def one(i, _):
            for j in range(2):
                hs[w][i, j, x, :, A[w]] = plus(hs[w][i, j, x, :, A[w]], ras[w][i, j], hs[w].dtype)
                hs[w][i, y, j, :, B[w]] = plus(hs[w][i, y, j, :, B[w]], rys[w][i, j], hs[w].dtype)
            return 0

        lax.fori_loop(0, ZS, one, 0)
        go(s2a(w))
        go(s2b(w))

    def st2(w):
        if w in RMIDS:
            return mid2(w)
        s2a(w).wait_recv()
        s2b(w).wait_recv()

        def one(i, _):
            hs[w][i, y, x, :, A[w]] = plus(hs[w][i, y, x, :, A[w]], r2as[w][i], hs[w].dtype)
            hs[w][i, y, x, :, B[w]] = plus(hs[w][i, y, x, :, B[w]], r2bs[w][i], hs[w].dtype)
            return 0

        lax.fori_loop(0, ZS, one, 0)
        for k in (1, 2, 3):
            go(s3(w, k))

    def st3(w):
        if w in RMIDS:
            return mid3(w)
        total = hs[w][z, y, x].astype(F32)
        for k in (1, 2, 3):
            s3(w, k).wait_recv()
            total = total + rzs[w][k - 1].astype(F32)
        outs[pieces[w][0]][:, pl.ds(*pieces[w][1:])] = total

    def t0():
        go(rc(tparts.at[:, X, :, :, TA], tx, tss.at[0], tsr.at[0], xn))
        go(rc(tparts.at[Y, :, :, :, TB], ty, tss.at[1], tsr.at[1], yn))

    def t1():
        rc(tx, tx, tss.at[0], tsr.at[0], xn).wait_recv()
        rc(ty, ty, tss.at[1], tsr.at[1], yn).wait_recv()
        tparts[Y, x, :, :, TA] = plus(tparts[Y, x, :, :, TA], tx[Y], BF16)
        tparts[y, X, :, :, TB] = plus(tparts[y, X, :, :, TB], ty[X], BF16)
        go(rc(tparts.at[Y, x, :, :, TA], t2a, tss.at[2], tsr.at[2], yn))
        go(rc(tparts.at[y, X, :, :, TB], t2b, tss.at[3], tsr.at[3], xn))

    def t2():
        rc(t2a, t2a, tss.at[2], tsr.at[2], yn).wait_recv()
        rc(t2b, t2b, tss.at[3], tsr.at[3], xn).wait_recv()
        own = base[...].reshape(tout.shape) + tparts[y, x].astype(F32)
        low = jnp.concatenate([tx[y].astype(F32) + t2a[...].astype(F32), ty[x].astype(F32) + t2b[...].astype(F32)], axis=2)
        tout[...] = own + low

    def done():
        for cp in sent:
            cp.wait_send()

    return post, (st0, st1, st2, st3), (t0, t1, t2), done


def mega_body(widths, pieces, *refs):
    nv = len(widths)
    small = refs[:nv]
    (sqkv, sout, sup, sdown, tok, cot, starts) = refs[nv : nv + 7]
    k = nv + 7
    gweights = refs[k : k + 5]
    gs = refs[k + 5 : k + 10]
    lout = refs[k + 10]
    shares, tgrad = refs[k + 11 : k + 16], refs[k + 16]
    k += 17
    (svec, tout, probs, qs, kv, att, normed1, inv1, inner, act, dpre, dres2, rows, sums) = refs[k : k + 14]
    k += 14
    (wqkv, wout, wup, wdown, vecs, bias, datt, dstage) = refs[k : k + 8]
    k += 8
    np_ = len(pieces)
    hold = refs[k : k + 7 * np_ + 5]
    base = hold[-1]
    k += 7 * np_ + 5
    wsem, psem, dsem = refs[k : k + 3]
    comm = refs[k + 3 : k + 24]
    sems = refs[k + 24 :]
    gvec, gqkv, gout, gup, gdown = gweights
    mixed, gp, vscr = base, dpre, vecs
    spare = tok.shape[0] * tok.shape[1] * YS * XS
    tpart = wdown.at[pl.ds(0, spare)].reshape((YS, XS) + tok.shape)
    svec[...] = jnp.zeros(svec.shape, F32)
    for r, v in enumerate(small):
        svec[r : r + 1, 0 : widths[r]] = v[...].astype(F32)
    micro, nrow, width = tok.shape
    count = micro * nrow
    length = nrow * YS * XS
    ff = sup.shape[1]
    ins = (svec, sqkv, sout, sup, sdown)
    outs = (gvec, gqkv, gout, gup, gdown)
    tasks = gather_tasks(ins, tok, outs, tout, comm)
    run = lambda name: [f() for f in tasks[name]]
    run("start")
    lin = [(gvec, vecs), (gqkv, wqkv), (gout, wout), (gup, wup), (gdown, wdown)]

    def fetch(w):
        src, dst = lin[w]
        cp = pltpu.make_async_copy(src.reshape(dst.shape) if w == 0 else src, dst, wsem.at[w])
        cp.start()
        return cp

    seq = lax.axis_index("seq")
    qpos = seq * nrow + lax.broadcasted_iota(jnp.int32, (nrow, length), 0)
    kpos = lax.broadcasted_iota(jnp.int32, (nrow, length), 1)
    for m in range(micro):
        ok = kpos <= qpos
        for j in range(starts.shape[1]):
            s = starts[m, j]
            both = (qpos >= s) & (qpos < s + PIC) & (kpos >= s) & (kpos < s + PIC)
            ok = ok | both
        bias[m] = jnp.where(ok, 0.0, NEG)
    run(0)
    run(1)
    first = [fetch(0), fetch(1)]
    for cp in first:
        cp.wait()
    nown = vecs.shape[0]
    made = {}
    for r, n in enumerate(widths):
        if n not in made:
            made[n] = spread(n * nown, n, nown)
        pick, mine = made[n]
        got = jnp.dot(vecs[:, r, 0:LANE], pick, preferred_element_type=F32)
        rows[r : r + 1, 0 : n * nown] = jnp.sum(got * mine, axis=0, keepdims=True)
    src = tok[...].reshape(count, width)
    head_scale = 1.0 / math.sqrt(width // HEADS)

    def make_q(at):
        qs[:, at] = (jnp.dot(tok[...].reshape(count, width), wqkv[:, at], preferred_element_type=F32) + rows[0:1, at]).astype(BF16)

    chunks(width, 384, make_q)
    run((2, 0))
    for m in range(micro):
        whole = tout[:, :, m].reshape(length, width)

        def make_k(i, _):
            at = pl.ds(pl.multiple_of(width + i * 384, 128), 384)
            to = pl.ds(pl.multiple_of(i * 384, 128), 384)
            kv[m, :, to] = jnp.dot(whole, wqkv[:, at], preferred_element_type=F32).astype(BF16)
            return 0

        def make_v(i, _):
            at = pl.ds(pl.multiple_of(2 * width + i * 384, 128), 384)
            to = pl.ds(pl.multiple_of(width + i * 384, 128), 384)
            kv[m, :, to] = (jnp.dot(whole, wqkv[:, at], preferred_element_type=F32) + rows[0:1, to]).astype(BF16)
            return 0

        lax.fori_loop(0, width // 384, make_k, 0)
        lax.fori_loop(0, width // 384, make_v, 0)
        run((2, 1 + m))
    pairs = width // LANE
    for m in range(micro):
        both = jnp.concatenate([bias[m], bias[m]], axis=0)

        def attend(p, _):
            at = pl.ds(pl.multiple_of(p * LANE, LANE), LANE)
            vat = pl.ds(pl.multiple_of(width + p * LANE, LANE), LANE)
            q2 = split_heads(qs[m * nrow : (m + 1) * nrow, at].astype(F32) * head_scale)
            score = nt(q2, kv[m, :, at]) + jnp.concatenate([bias[m], bias[m]], axis=0)
            expo = jnp.exp(score - jnp.max(score, axis=1, keepdims=True))
            low = (expo * (1.0 / jnp.sum(expo, axis=1, keepdims=True))).astype(BF16)
            probs[m * pairs + p] = low
            o = join_heads(jnp.dot(low, kv[m, :, vat], preferred_element_type=F32))
            att[m * nrow : (m + 1) * nrow, at] = o.astype(BF16)
            return 0

        for part in range(2):
            lax.fori_loop(part * pairs // 2, (part + 1) * pairs // 2, attend, 0)
            run((3, 2 * m + part))
    cp = [fetch(2), fetch(3)]
    cp[0].wait()

    def project(at):
        normed1[:, at] = tok[:, :, at].reshape(count, 384).astype(F32) + jnp.dot(att[...], wout[:, at], preferred_element_type=F32) + rows[1:2, at]

    chunks(width, 384, project)
    res = normed1[...]
    centre = res - jnp.mean(res, axis=1, keepdims=True)
    inverse = lax.rsqrt(jnp.mean(centre * centre, axis=1, keepdims=True) + EPS)
    norm = centre * inverse
    normed1[...] = norm
    inv1[...] = jnp.broadcast_to(inverse, inv1.shape)
    mix = norm * rows[2:3, 0:width] + rows[3:4, 0:width]
    mixed[...] = mix
    inner[...] = mix.astype(BF16)
    cp[1].wait()

    def feed(at):
        pre = jnp.dot(inner[...], wup[:, at], preferred_element_type=F32) + rows[4:5, at]
        cdf = 0.5 * (1.0 + lax.erf(pre * math.sqrt(0.5)))
        act[:, at] = (pre * cdf).astype(BF16)
        gp[:, at] = (cdf + pre * jnp.exp(-0.5 * pre * pre) * (1.0 / math.sqrt(2.0 * math.pi))).astype(BF16)

    for part in range(3):
        lax.fori_loop(2 * part, 2 * part + 2, lambda i, _: (feed(pl.ds(pl.multiple_of(i * (ff // 6), 128), ff // 6)), 0)[1], 0)
        run((4, part))
    run(4)
    last = fetch(4)
    last.wait()

    def out2(at):
        dres2[:, at] = mixed[:, at] + jnp.dot(act[...], wdown[:, at], preferred_element_type=F32) + rows[5:6, at]

    chunks(width, 256, out2)
    res = dres2[...]
    centre = res - jnp.mean(res, axis=1, keepdims=True)
    inverse = lax.rsqrt(jnp.mean(centre * centre, axis=1, keepdims=True) + EPS)
    norm = centre * inverse
    gain = rows[6:7, 0:width]
    lout[...] = (norm * gain + rows[7:8, 0:width]).astype(BF16)
    up = cot[...].astype(F32)
    scaled = up * gain
    dres = inverse * (scaled - jnp.mean(scaled, axis=1, keepdims=True) - norm * jnp.mean(scaled * norm, axis=1, keepdims=True))
    dres2[...] = dres
    sums[0:1] = jnp.sum(dres.astype(BF16).astype(F32), axis=0, keepdims=True)
    sums[1:2] = jnp.sum(up * norm, axis=0, keepdims=True)
    sums[2:3] = jnp.sum(up, axis=0, keepdims=True)
    pairs = width // LANE
    vscr[...] = jnp.zeros(vscr.shape, F32)

    def vec(r, value):
        n = widths[r]
        pick, mine = made[n]
        vscr[:, r, 0:LANE] = lax.dot_general(value * mine, pick, (((1,), (1,)), ((), ())), precision=lax.Precision.HIGHEST, preferred_element_type=F32)

    post, (st0, st1, st2, st3), (t0, t1, t2), done = scatter_tasks(gs, pieces, tpart, shares, tgrad, hold, sems)
    D0, D1, U0, U1, OUT, KV, QQ, VEC = range(8)
    step = dstage.shape[1]

    def gdown_cols(col, size):
        cols = pl.ds(col, size)

        def send(slot, at):
            return pltpu.make_async_copy(dstage.at[slot, :, pl.ds(0, size)], gs[0].at[at, cols], dsem.at[slot])

        def one(i, _):
            slot = lax.rem(i, 2)

            @pl.when(i >= 2)
            def _():
                send(slot, pl.ds(0, step)).wait()

            at = pl.ds(pl.multiple_of(i * step, step), step)
            dstage[slot, :, 0:size] = tn(act[:, at], dres2[:, cols].astype(BF16)).astype(BF16)
            send(slot, at).start()
            return 0

        lax.fori_loop(0, ff // step, one, 0)
        send(0, pl.ds(0, step)).wait()
        send(1, pl.ds(0, step)).wait()

    gdown_cols(*pieces[D0][1:])
    post(D0)
    gdown_cols(*pieces[D1][1:])
    post(D1)

    def put(i, src, dst):
        cp = pltpu.make_async_copy(src, dst, psem.at[i])
        cp.start()
        return cp

    def feed_back(at):
        d = nt(dres2[...].astype(BF16), wdown[at, :])
        dpre[:, at] = (d * dpre[:, at].astype(F32)).astype(BF16)

    st0(D0)
    chunks(ff, 512, feed_back)
    st0(D1)

    def dmix(at):
        base[:, at] = dres2[:, at] + nt(dpre[...], wup[at, :])

    chunks(width, 256, dmix)
    st1(D0)

    def gup_part(at):
        wup[:, at] = tn(inner[...], dpre[:, at]).astype(BF16)

    chunks(ff, 512, gup_part)
    cp = put(0, wup, gs[1])
    dm, normed = base[...], normed1[...]
    vec(2, jnp.sum(dm * normed, axis=0, keepdims=True))
    vec(3, jnp.sum(dm, axis=0, keepdims=True))
    scaled = dm * rows[2:3, 0:width]
    d1 = inv1[:, 0:1] * (scaled - jnp.mean(scaled, axis=1, keepdims=True) - normed * jnp.mean(scaled * normed, axis=1, keepdims=True))
    base[...] = d1
    vec(1, jnp.sum(d1.astype(BF16).astype(F32), axis=0, keepdims=True))
    cp.wait()
    post(U0)
    post(U1)

    def back_out(at):
        datt[:, at] = nt(base[...].astype(BF16), wout[at, :]).astype(BF16)

    chunks(width, 384, back_out)

    def gout_part(at):
        wout[:, at] = tn(att[...], base[:, at].astype(BF16)).astype(BF16)

    chunks(width, 384, gout_part)
    cp = put(1, wout, gs[2])
    pumps = [[(cp.wait,), (post, OUT), (st0, U0)], [(st0, U1), (st1, D1)], [(st0, OUT)], [(st1, U0)]]
    for m in range(micro):
        mrow = slice(m * nrow, (m + 1) * nrow)

        def attend_back(p, _):
            at = pl.ds(pl.multiple_of(p * LANE, LANE), LANE)
            vat = pl.ds(pl.multiple_of(width + p * LANE, LANE), LANE)
            q2 = split_heads(qs[mrow, at].astype(F32) * head_scale)
            o2 = split_heads(datt[mrow, at].astype(F32))
            low = probs[m * pairs + p]
            prob = low.astype(F32)
            dprob = nt(o2, kv[m, :, vat])
            delta = jnp.sum(prob * dprob, axis=1, keepdims=True)
            ds = (prob * (dprob - delta)).astype(BF16)
            datt[mrow, at] = (join_heads(jnp.dot(ds, kv[m, :, at], preferred_element_type=F32)) * head_scale).astype(BF16)
            kv[m, :, at] = tn(ds, q2).astype(BF16)
            kv[m, :, vat] = tn(low, o2).astype(BF16)
            return 0

        for part in range(2):
            lax.fori_loop(part * pairs // 2, (part + 1) * pairs // 2, attend_back, 0)
            for f, *a in pumps[2 * m + part]:
                f(*a)
    dq, dkv = datt, kv
    for m in range(micro):

        def piece(i, _):
            at = pl.ds(pl.multiple_of(i * 256, 256), 256)
            got = nt(dkv[m], wqkv[at, width : 3 * width])
            tpart[:, :, m, :, at] = got.reshape(YS, XS, nrow, 256).astype(BF16)
            return 0

        lax.fori_loop(0, width // 256, piece, 0)
    t0()

    def gkv(i, _):
        at = pl.ds(pl.multiple_of(i * 384, 128), 384)
        to = pl.ds(pl.multiple_of(width + i * 384, 128), 384)
        total = tn(tout[:, :, 0].reshape(length, width), dkv[0, :, at])
        for m in range(1, micro):
            total = total + tn(tout[:, :, m].reshape(length, width), dkv[m, :, at])
        wqkv[:, to] = total.astype(BF16)
        return 0

    lax.fori_loop(0, 2 * width // 384, gkv, 0)
    cp = put(2, wqkv.at[:, pl.ds(width, 2 * width)], gs[3].at[:, pl.ds(width, 2 * width)])
    cp.wait()
    post(KV)
    st1(U1)

    def dsrc(at):
        base[:, at] = base[:, at] + nt(dq[...], wqkv[at, 0:width])

    chunks(width, 256, dsrc)

    def gq(at):
        wqkv[:, at] = tn(tok[...].reshape(count, width), dq[:, at]).astype(BF16)

    chunks(width, 384, gq)
    cp = put(3, wqkv.at[:, pl.ds(0, width)], gs[3].at[:, pl.ds(0, width)])
    dv = sum(jnp.sum(dkv[m, :, width:].astype(F32), axis=0, keepdims=True) for m in range(micro))
    vec(0, jnp.concatenate([jnp.sum(dq[...].astype(F32), axis=0, keepdims=True), dv], axis=1))
    vec(4, jnp.sum(dpre[...].astype(F32), axis=0, keepdims=True))
    for r in range(3):
        vec(5 + r, sums[r : r + 1])
    cp.wait()
    post(QQ)
    st0(KV)
    cp = put(4, vscr, gs[4].reshape(vscr.shape))
    st1(OUT)
    cp.wait()
    post(VEC)
    st0(QQ)
    st0(VEC)
    st2(D0)
    st2(U0)
    t1()
    st2(D1)
    st2(U1)
    st2(OUT)
    for w in (KV, QQ, VEC):
        st1(w)
    for w in (D0, U0, D1, U1, OUT):
        st3(w)
    for w in (KV, QQ, VEC):
        st2(w)
    t2()
    for w in (KV, QQ, VEC):
        st3(w)
    done()
    run("end")


def mega(small, shards, tok, cot, starts):
    D, V, ANY = pltpu.SemaphoreType.DMA, pltpu.VMEM, pl.ANY
    micro, nrow, width = tok.shape
    count, length, ff = micro * nrow, nrow * YS * XS, shards[2].shape[1]
    pairs = micro * width // LANE
    S = jax.ShapeDtypeStruct
    widths = tuple(v.shape[1] for v in small)
    total = ZS * CS * YS * XS
    vshape = (8, 256)
    order = (3, 2, 1, 0)
    garr = [(shards[i].shape, BF16) for i in order] + [(vshape, F32)]
    pieces = ((0, 0, width // 3), (0, width // 3, width - width // 3), (1, 0, ff // 2), (1, ff // 2, ff // 2), (2, 0, width), (3, width, 2 * width), (3, 0, width), (4, 0, 256))
    outs = [S((total * vshape[0], vshape[1]), F32)] + [S((total * s.shape[0], s.shape[1]), BF16) for s in shards]
    outs += [S((total * b[0], b[1]), t) for b, t in garr]
    res = [S((count, width), BF16)] + [S(b, F32) for b, _ in garr] + [S((micro, nrow, width), F32)]
    scr = [
        V(vshape, F32), V((YS, XS) + tok.shape, BF16), V((pairs, 2 * nrow, length), BF16), V((count, width), BF16),
        V((micro, length, 2 * width), BF16), V((count, width), BF16), V((count, width), F32), V((count, LANE), F32),
        V((count, width), BF16), V((count, ff), BF16), V((count, ff), BF16), V((count, width), F32), V((8, ff), F32), V((8, width), F32),
    ]
    scr += [V((total * s.shape[0], s.shape[1]), BF16) for s in shards]
    scr += [V((total,) + vshape, F32), V((micro, nrow, length), F32), V((count, width), BF16), V((2, 512, width), BF16)]
    both = [((garr[a][0][0], m), garr[a][1]) for a, _, m in pieces]
    scr += [V((ZS, YS, XS) + b, t) for b, t in both] * 2
    scr += [V((ZS, 2, b[0], b[1] // 2), t) for b, t in both] * 2
    scr += [V(((ZS - 1, 2) if w in RMIDS else (ZS,)) + (b[0], b[1] // 2), t) for w, (b, t) in enumerate(both)] * 2
    scr += [V((2, b[0], b[1] // 2) if w in RMIDS else (ZS - 1,) + b, t) for w, (b, t) in enumerate(both)]
    th = (micro, nrow, width // 2)
    scr += [V((2,) + th, BF16)] * 2 + [V(th, BF16)] * 2 + [V((count, width), F32)]
    n, q = 5, len(pieces)
    scr += [D((n,)), D((n,)), D((2,))]
    scr += [D((n + 1,)), D((n, 4)), D((n, 3))] + [D((n, 4))] * 8 + [D((n, 4, 4))] * 2 + [D((4,))] * 2
    scr += [D((1,))] * 2 + [D((n, 4)), D((n, 3))] * 2
    scr += [D((q, 16)), D((q, 12)), D((q, 12)), D((4,)), D((4,)), D((q, 16)), D((q, 16))]
    spec = lambda s: pl.BlockSpec(memory_space=s)
    got = pl.pallas_call(
        functools.partial(mega_body, widths, pieces),
        out_shape=outs + res,
        in_specs=[spec(V)] * (len(small) + 6) + [spec(pltpu.SMEM)],
        out_specs=[spec(ANY)] * 10 + [spec(V)] * len(res),
        scratch_shapes=scr,
        compiler_params=pltpu.CompilerParams(collective_id=0, has_side_effects=True, vmem_limit_bytes=67043328),
        name="layer",
    )(*small, *shards, tok, cot, starts)
    return got[10:]


def finish_body(widths, *refs):
    n = 6
    ins, vec, outs, small = refs[:n], refs[n], refs[n + 1 : 2 * n + 1], refs[2 * n + 1 :]
    for a, b in zip(ins, outs):
        b[...] = a[...]
    for r, o in enumerate(small):
        o[...] = vec[r : r + 1, 0 : widths[r]]


def finish(arrays, vec, widths):
    S = jax.ShapeDtypeStruct
    outs = [S(a.shape, a.dtype) for a in arrays] + [S((1, w), F32) for w in widths]
    spec = pl.BlockSpec(memory_space=pltpu.VMEM)
    return pl.pallas_call(
        functools.partial(finish_body, widths), out_shape=outs,
        in_specs=[spec] * (len(arrays) + 1), out_specs=[spec] * len(outs), name="finish",
    )(*arrays, vec)


def fits(mesh):
    return mesh.shape["dp"] == ZS * CS and mesh.shape["seq"] == YS * XS


def fast_device(
    tokens, piece_starts, qkv_weight, qv_bias, out_weight, out_bias, norm1_gain, norm1_bias,
    up_weight, up_bias, down_weight, down_bias, norm2_gain, norm2_bias, grad_out,
):
    micro, _, nrow, width = tokens.shape
    small = (qv_bias, out_bias, norm1_gain, norm1_bias, up_bias, down_bias, norm2_gain, norm2_bias)
    widths = tuple(v.shape[0] for v in small)
    got = mega(
        tuple(v.reshape(1, -1) for v in small), (qkv_weight, out_weight, up_weight, down_weight),
        tokens[:, 0], grad_out.reshape(micro * nrow, width), piece_starts[:, 0],
    )
    lout, down, up, out, qkv, vec, tgrad = got
    done = finish((lout, tgrad, qkv, out, up, down), vec, widths)
    lout, tgrad, qkv, out, up, down = done[:6]
    v = [a.reshape(-1) for a in done[6:]]
    return (
        lout.reshape(tokens.shape), tgrad.reshape(tokens.shape),
        qkv, v[0], out, v[1], v[2], v[3], up, v[4], down, v[5], v[6], v[7],
    )


def solution(mesh):
    return jax.shard_map(
        fast_device if fits(mesh) else on_device,
        mesh=mesh,
        in_specs=(
            P(None, "dp", "seq", None),
            P(None, "dp", None),
            P(("dp", "seq"), None),
            P(("dp", "seq")),
            P(("dp", "seq"), None),
            P(("dp", "seq")),
            P(("dp", "seq")),
            P(("dp", "seq")),
            P(("dp", "seq"), None),
            P(("dp", "seq")),
            P(("dp", "seq"), None),
            P(("dp", "seq")),
            P(("dp", "seq")),
            P(("dp", "seq")),
            P(None, "dp", "seq", None),
        ),
        out_specs=(
            P(None, "dp", "seq", None),
            P(None, "dp", "seq", None),
            P(("dp", "seq"), None),
            P(("dp", "seq")),
            P(("dp", "seq"), None),
            P(("dp", "seq")),
            P(("dp", "seq")),
            P(("dp", "seq")),
            P(("dp", "seq"), None),
            P(("dp", "seq")),
            P(("dp", "seq"), None),
            P(("dp", "seq")),
            P(("dp", "seq")),
            P(("dp", "seq")),
        ),
        check_vma=False,
    )
```
